256 devices in a mesh: rows: 128 (over z_hi, x, y, core), spec: 2 (over z_lo).
Axes of the slice: x: 4, y: 4, z: 8 (z_hi: 4, z_lo: 2; z = z_hi * 2 + z_lo), core: 2. Of those that a mesh axis runs over, the one named last changes fastest.
Arguments:
- field: float32 [36, 30, 65536], P('spec', None, 'rows'), may hold values from 0.1 to 4
- group_speed: float32 [30], replicated, may hold values from 0.3 to 1
- face_angle: float32 [131072], P('rows'), may hold values from -3.140625 to 3.140625
- face_speed: float32 [131072], P('rows'), may hold values from 0.04 to 0.2
- face_cells: int32 [2, 131072], P(None, 'rows'), may hold values from 0 to 1023, as said below
- face_live: int32 [128], P('rows'), may hold values from 1 to 8, as said below
- halo_blocks: int32 [128, 2, 2], P('rows'), may hold values from 0 to 3
- cell_level: int32 [65536], P('rows'), may hold values from 0 to 2
- polar_mask: int32 [65536], P('rows'), may hold values 0 or 1
- turn_rate: float32 [65536], P('rows'), may hold values from -0.45 to 0.45
Outputs:
- advanced: float32 [36, 30, 65536], P('spec', None, 'rows')
The draws below stay inside these ranges and needn't reach their ends.
Inputs may be any that keep to these rules, and one draw needn't show every extreme that they name: `face_cells`: row 0 is a face's lower cell, a position among its row block's own 512 cells; row 1 its upper cell, a position among the own cells followed by 2 halo blocks from the block before and 2 from the block after (128 cells each). Only the first face_live[r] of row block r's 8 face blocks carry faces; some row block has all 8 live.
All inputs are finite; a program needn't handle non-finite values. No bound on the sum of `polar_mask` on one device may be relied on, other than what follows from the above.
Results may differ from the reference program's by a relative error of at most 0.0003.
Values sent between devices are 32-bit elements; how exact they have to be, the bound alone decides.
A program may use at most 64 MiB of HBM per device.

```python
import math
import jax
import jax.numpy as jnp
from jax import lax

NDIR = 36
NFREQ = 30
CELL_DEV = 512
HBO = 2
ITERS = 3
FBLK = 8
CELLS = 65536
FACES = 131072
N_ROWS = 128


def draw_face_cells(key, part):
    base = jax.random.fold_in(key, 11)
    key_low, key_own, key_halo, key_pick = jax.random.split(base, 4)
    faces = N_ROWS * FBLK * 128
    lower = jax.random.randint(key_low, (faces,), 0, CELL_DEV)
    own_upper = jax.random.randint(key_own, (faces,), 0, CELL_DEV)
    halo_upper = CELL_DEV + jax.random.randint(key_halo, (faces,), 0, 256 * HBO)
    picked = jax.random.randint(key_pick, (faces,), 0, 100) < 20
    upper = jnp.where(picked, halo_upper, own_upper)
    return jnp.stack([lower, upper]).astype(jnp.int32)


def draw_face_live(key, part):
    base = jax.random.fold_in(key, 23)
    key_first, key_second, key_full = jax.random.split(base, 3)
    first = jax.random.randint(key_first, (N_ROWS,), 0, FBLK + 1)
    second = jax.random.randint(key_second, (N_ROWS,), 0, FBLK + 1)
    live = jnp.maximum(1, first * second // FBLK)
    fullest = jax.random.randint(key_full, (), 0, N_ROWS)
    return live.at[fullest].set(FBLK).astype(jnp.int32)


def touch_ends(array, own_key, low, high):
    dims = array.shape
    spot = [jax.random.randint(jax.random.fold_in(own_key, axis), (), 0, dims[axis]) for axis in range(len(dims))]
    array = array.at[tuple(spot)].set(low)
    longest = dims.index(max(dims))
    spot[longest] = (spot[longest] + 1) % dims[longest]
    return array.at[tuple(spot)].set(high)


def block_levels(rng, shape, pieces, least, largest):
    def one(axis_at, parts):
        heights = jax.random.uniform(jax.random.fold_in(jax.random.fold_in(rng, 6), axis_at), (parts,), jnp.float32, least / len(pieces), largest / len(pieces))
        return jnp.repeat(jnp.exp(heights), shape[axis_at] // parts).reshape((-1,) + (1,) * (len(shape) - axis_at - 1))

    loudness = one(*pieces[0])
    for cut in pieces[1:]:
        loudness = loudness * one(*cut)
    return loudness


def setup_inputs(seed: int = 0) -> dict:
    arg_keys = jax.random.split(jax.random.key(seed), 11)
    field = jnp.clip(jnp.exp(math.log(4.0) - 3.6888794 * jax.random.uniform(arg_keys[0], (NDIR, NFREQ, CELLS), jnp.float32) ** block_levels(arg_keys[0], (NDIR, NFREQ, CELLS), ((0, 2), (2, 128)), -0.2, 0.2)), 0.1, 4.0)
    group_speed = jnp.clip(jnp.exp(jax.random.uniform(arg_keys[1], (NFREQ,), jnp.float32, math.log(0.3), math.log(1.0))), 0.3, 1.0)
    face_angle = jnp.clip(jax.random.uniform(arg_keys[2], (FACES,), jnp.float32, -3.140625, 3.140625), -3.140625, 3.140625)
    face_speed = jnp.clip(jnp.exp(math.log(0.2) - 1.609438 * jax.random.uniform(arg_keys[3], (FACES,), jnp.float32) ** block_levels(arg_keys[3], (FACES,), ((0, 128),), -0.2, 0.2)), 0.04, 0.2)
    face_cells = draw_face_cells(jax.random.fold_in(arg_keys[10], 71), 0)
    face_live = draw_face_live(jax.random.fold_in(arg_keys[10], 71), 0)
    halo_blocks = touch_ends(jax.random.randint(arg_keys[6], (N_ROWS, 2, HBO), 0, CELL_DEV // 128), jax.random.fold_in(arg_keys[6], 1), 0, (CELL_DEV // 128) - 1).astype(jnp.int32)
    cell_level = touch_ends(jax.random.randint(arg_keys[7], (CELLS,), 0, 3), jax.random.fold_in(arg_keys[7], 1), 0, 2).astype(jnp.int32)
    polar_mask = touch_ends((jax.random.randint(arg_keys[8], (CELLS,), 0, 3) < 1).astype(jnp.int32), jax.random.fold_in(arg_keys[8], 1), 0, 1)
    turn_rate = jnp.clip(jax.random.uniform(arg_keys[9], (CELLS,), jnp.float32, -0.45, 0.45) * block_levels(arg_keys[9], (CELLS,), ((0, 128),), -0.4, 0.0), -0.45, 0.45)
    return {"field": field, "group_speed": group_speed, "face_angle": face_angle, "face_speed": face_speed, "face_cells": face_cells, "face_live": face_live, "halo_blocks": halo_blocks, "cell_level": cell_level, "polar_mask": polar_mask, "turn_rate": turn_rate}


def face_flux_sum(total, ext, lower, upper, weight, theta, angle, group_speed):
    cosine = jnp.cos(theta[:, None] - angle[None, :]) * weight[None, :]
    velocity = group_speed[None, :, None] * cosine[:, None, :]
    low_vals = jnp.take(ext, lower, axis=2)
    up_vals = jnp.take(ext, upper, axis=2)
    flux = jnp.maximum(velocity, 0.0) * low_vals + jnp.minimum(velocity, 0.0) * up_vals
    total = total.at[:, :, lower].add(flux)
    return total.at[:, :, upper].add(-flux)


def pick_blocks(neighbour, table):
    ndir, nfreq, cdev = neighbour.shape
    view = neighbour.reshape(ndir, nfreq, cdev // 128, 128)
    return jnp.take(view, table, axis=2).reshape(ndir, nfreq, -1)


def reference(field, group_speed, face_angle, face_speed, face_cells, face_live, halo_blocks, cell_level, polar_mask, turn_rate):
    ndir, nfreq, cells = field.shape
    rows_n = N_ROWS
    cdev = cells // rows_n
    fdev = face_angle.shape[0] // rows_n
    theta = (jnp.arange(ndir, dtype=jnp.float32) + 0.5) * (2.0 * math.pi / NDIR)
    weight_turn = (polar_mask.astype(jnp.float32) * turn_rate)[None, None, :]
    current = field
    for step in range(ITERS):
        def one_row(r):
            own = lax.dynamic_slice_in_dim(current, r * cdev, cdev, 2)
            below = lax.dynamic_slice_in_dim(current, jnp.maximum(r - 1, 0) * cdev, cdev, 2) * (r > 0).astype(jnp.float32)
            above = lax.dynamic_slice_in_dim(current, jnp.minimum(r + 1, rows_n - 1) * cdev, cdev, 2) * (r < rows_n - 1).astype(jnp.float32)
            table = halo_blocks[r]
            ext = jnp.concatenate([own, pick_blocks(below, table[0]), pick_blocks(above, table[1])], axis=2)
            pair = lax.dynamic_slice_in_dim(face_cells, r * fdev, fdev, 1)
            angle = lax.dynamic_slice_in_dim(face_angle, r * fdev, fdev, 0)
            speed = lax.dynamic_slice_in_dim(face_speed, r * fdev, fdev, 0)
            live = (jnp.arange(fdev, dtype=jnp.int32) < face_live[r] * 128).astype(jnp.float32)
            total = jnp.zeros(ext.shape, jnp.float32)
            total = face_flux_sum(total, ext, pair[0], pair[1], speed * live, theta, angle, group_speed)
            level = lax.dynamic_slice_in_dim(cell_level, r * cdev, cdev, 0)
            return own - total[:, :, :cdev] * jnp.exp2(-level.astype(jnp.float32))[None, None, :]

        moved = lax.map(one_row, jnp.arange(rows_n, dtype=jnp.int32))
        moved = jnp.transpose(moved, (1, 2, 0, 3)).reshape(ndir, nfreq, cells)
        before = jnp.roll(moved, 1, axis=0)
        after = jnp.roll(moved, -1, axis=0)
        current = moved - jnp.maximum(weight_turn, 0.0) * (moved - before) - jnp.minimum(weight_turn, 0.0) * (after - moved)
    return current
```

```python
import functools
import math

import jax
import jax.numpy as jnp
from jax import lax
from jax.experimental import pallas as pl
from jax.experimental.pallas import tpu as pltpu
from jax.sharding import PartitionSpec as P

MESH = pl.DeviceIdType.MESH
NDIR = 36
ITERS = 3
LANES = 128
ROWS = 32
CHUNK = 3
BF16 = jnp.bfloat16
F32 = jnp.float32


def split(value):
    high = value.astype(BF16)
    return high, (value - high.astype(F32)).astype(BF16)


def kernel(
    field,
    speed_s,
    angle_h,
    weight_h,
    cells_h,
    live_s,
    table_h,
    level_h,
    mask_h,
    rate_h,
    out,
    cur,
    moved,
    sent,
    got,
    edge_sent,
    edge_got,
    ext_hi,
    ext_lo,
    flux_hi,
    flux_lo,
    own_hot,
    up_hot,
    back_hot,
    vel,
    scale,
    turn,
    angle,
    weight,
    cells,
    level,
    mask,
    rate,
    table_v,
    table_r,
    picks,
    load_sem,
    out_sem,
    small_sem,
    table_send,
    table_recv,
    send_sem,
    recv_sem,
    edge_send,
    edge_recv,
):
    dloc, nfreq, own = field.shape
    pairs = dloc // 2
    chunks = pairs // CHUNK
    hb = table_h.shape[2]
    faces = cells.shape[1]
    fblk = faces // LANES
    size = lax.axis_size("rows")
    row = lax.axis_index("rows")
    spec = lax.axis_index("spec")
    has = (row > 0, row < size - 1)
    peer = ({"rows": jnp.maximum(row - 1, 0)}, {"rows": jnp.minimum(row + 1, size - 1)})
    partner = {"spec": 1 - spec}

    def slot(d):
        return 2 * d if d < pairs else 2 * (dloc - 1 - d) + 1

    def direction(p):
        return p // 2 if p % 2 == 0 else dloc - 1 - p // 2

    small = [
        pltpu.make_async_copy(src, dst, small_sem.at[i])
        for i, (src, dst) in enumerate(
            (
                (table_h, table_v),
                (cells_h, cells),
                (angle_h, angle),
                (weight_h, weight),
                (level_h, level),
                (mask_h, mask),
                (rate_h, rate),
            )
        )
    ]
    for copy in small:
        copy.start()
    loads = [
        pltpu.make_async_copy(
            field.at[direction(p)], cur.at[p], load_sem.at[p]
        )
        for p in range(dloc)
    ]
    for copy in loads:
        copy.start()
    table_r[...] = jnp.zeros_like(table_r)

    barrier = pltpu.get_barrier_semaphore()
    pl.semaphore_signal(barrier, inc=1, device_id=partner, device_id_type=MESH)
    for side in (0, 1):

        @pl.when(has[side])
        def _():
            pl.semaphore_signal(barrier, inc=1, device_id=peer[side], device_id_type=MESH)

    pl.semaphore_wait(barrier, 1 + has[0].astype(jnp.int32) + has[1].astype(jnp.int32))

    small[0].wait()
    tables = [
        pltpu.make_async_remote_copy(
            src_ref=table_v,
            dst_ref=table_r.at[1 - side],
            send_sem=table_send.at[side],
            recv_sem=table_recv.at[1 - side],
            device_id=peer[side],
            device_id_type=MESH,
        )
        for side in (0, 1)
    ]
    for side in (0, 1):

        @pl.when(has[side])
        def _():
            tables[side].start()

    for copy in small[1:]:
        copy.wait()

    sub = lax.broadcasted_iota(jnp.int32, (LANES, LANES), 0)
    lane = lax.broadcasted_iota(jnp.int32, (LANES, LANES), 1)
    one = jnp.float32(1.0)
    zero = jnp.float32(0.0)

    def build(j, carry):
        at = pl.ds(pl.multiple_of(j * LANES, LANES), LANES)
        low = jnp.broadcast_to(cells[0:1, at], (LANES, LANES))
        upp = jnp.broadcast_to(cells[1:2, at], (LANES, LANES))
        for c in range(own // LANES):
            own_hot[c * LANES : (c + 1) * LANES, at] = jnp.where(
                low == sub + c * LANES, one, zero
            ).astype(BF16)
        for c in range(up_hot.shape[0] // LANES):
            up_hot[c * LANES : (c + 1) * LANES, at] = jnp.where(
                upp == sub + c * LANES, one, zero
            ).astype(BF16)
        low_t = low.T
        upp_t = upp.T
        for c in range(own // LANES):
            here = lane + c * LANES
            back_hot[at, c * LANES : (c + 1) * LANES] = (
                jnp.where(low_t == here, one, zero) - jnp.where(upp_t == here, one, zero)
            ).astype(BF16)
        return carry

    lax.fori_loop(0, fblk, build, 0)

    blocks = lax.broadcasted_iota(jnp.int32, (fblk, LANES), 0)
    slot_weight = jnp.where(blocks < live_s[0], weight[...], zero)
    along = jnp.cos(angle[...]) * slot_weight
    across = jnp.sin(angle[...]) * slot_weight
    sign = (1 - 2 * spec).astype(F32)
    along = along * sign
    across = across * sign
    for p in range(dloc):
        theta = (direction(p) + 0.5) * (2.0 * math.pi / NDIR)
        vel[p] = along * math.cos(theta) + across * math.sin(theta)

    freq = lax.broadcasted_iota(jnp.int32, (nfreq, LANES), 0)
    group = jnp.zeros((nfreq, LANES), F32)
    for f in range(nfreq):
        group = jnp.where(freq == f, speed_s[f], group)
    for c in range(own // LANES):
        lev = level[0:1, c * LANES : (c + 1) * LANES]
        area = jnp.exp2(-lev.astype(F32))
        scale[:, c * LANES : (c + 1) * LANES] = group * area
    bend = mask[...].astype(F32) * rate[...]
    turn[0:1, :] = jnp.maximum(bend, 0.0)
    turn[1:2, :] = jnp.minimum(bend, 0.0)

    for side in (0, 1):

        @pl.when(jnp.logical_not(has[side]))
        def _():
            def clear(i, carry):
                def inner(j, c):
                    got[i, side, j] = jnp.zeros(got.shape[3:], F32)
                    return c

                return lax.fori_loop(0, pairs, inner, carry)

            lax.fori_loop(0, ITERS, clear, 0)

    for side in (0, 1):

        @pl.when(has[side])
        def _():
            pltpu.make_async_remote_copy(
                src_ref=table_v,
                dst_ref=table_r.at[side],
                send_sem=table_send.at[side],
                recv_sem=table_recv.at[side],
                device_id=peer[side],
                device_id_type=MESH,
            ).wait_recv()

    for side in (0, 1):
        taken = table_r[side, 0]
        for k in range(hb):
            picks[side * hb + k] = jnp.broadcast_to(
                taken[1 - side : 2 - side, k : k + 1], (8, LANES)
            )

    def pick(value, side, k):
        wanted = jnp.broadcast_to(picks[side * hb + k, 0:1, :], (nfreq, LANES))
        chosen = value[:, 0:LANES]
        for c in range(1, own // LANES):
            chosen = jnp.where(wanted == c, value[:, c * LANES : (c + 1) * LANES], chosen)
        return chosen

    def halo_copy(step, side, pair):
        return pltpu.make_async_remote_copy(
            src_ref=sent.at[step, side, pair],
            dst_ref=got.at[step, 1 - side, pair],
            send_sem=send_sem.at[step, side, pair],
            recv_sem=recv_sem.at[step, 1 - side, pair],
            device_id=peer[side],
            device_id_type=MESH,
        )

    def halo_arrival(step, side, pair):
        return pltpu.make_async_remote_copy(
            src_ref=sent.at[step, side, pair],
            dst_ref=got.at[step, side, pair],
            send_sem=send_sem.at[step, side, pair],
            recv_sem=recv_sem.at[step, side, pair],
            device_id=peer[side],
            device_id_type=MESH,
        )

    def send_pair(step, pair):
        for side in (0, 1):
            for e in (0, 1):
                value = cur[2 * pair + e]
                for k in range(hb):
                    sent[step, side, pair, e, k] = pick(value, side, k)

            @pl.when(has[side])
            def _():
                halo_copy(step, side, pair).start()

    def split_own(p):
        rows = pl.ds(p * ROWS, nfreq)
        high, low = split(cur[p])
        ext_hi[rows, 0:own] = high
        ext_lo[rows, 0:own] = low

    for pair in range(pairs):
        for e in (0, 1):
            loads[2 * pair + e].wait()
        send_pair(0, pair)
    for p in range(dloc):
        split_own(p)

    def turn_slot(step, p):
        d = direction(p)
        here = moved[p]
        before = moved[slot(d - 1)] if d > 0 else edge_got[step, 1]
        after = moved[slot(d + 1)] if d < dloc - 1 else edge_got[step, 0]
        cur[p] = here - turn[0:1, :] * (here - before) - turn[1:2, :] * (after - here)
        split_own(p)

    def edge_copy(step):
        return pltpu.make_async_remote_copy(
            src_ref=edge_sent.at[step],
            dst_ref=edge_got.at[step],
            send_sem=edge_send.at[step],
            recv_sem=edge_recv.at[step],
            device_id=partner,
            device_id_type=MESH,
        )

    def store_pair(pair):
        return [
            pltpu.make_async_copy(
                cur.at[p], out.at[direction(p)], out_sem.at[p]
            )
            for p in (2 * pair, 2 * pair + 1)
        ]

    def finish_pair(step, pair):
        turn_slot(step, 2 * pair)
        turn_slot(step, 2 * pair + 1)

        @pl.when(step < ITERS - 1)
        def _():
            send_pair(step + 1, pair)

        @pl.when(step == ITERS - 1)
        def _():
            for copy in store_pair(pair):
                copy.start()

    def compute(step, chunk):
        span = 2 * CHUNK * ROWS
        rows = pl.ds(chunk * span, span)
        for i in range(CHUNK):
            pair = chunk * CHUNK + i
            for side in (0, 1):

                @pl.when(has[side])
                def _():
                    halo_arrival(step, side, pair).wait_recv()

            for side in (0, 1):
                for e in (0, 1):
                    for k in range(hb):
                        high, low = split(got[step, side, pair, e, k])
                        at = pl.ds(own + (side * hb + k) * LANES, LANES)
                        there = pl.ds((2 * pair + e) * ROWS, nfreq)
                        ext_hi[there, at] = high
                        ext_lo[there, at] = low
        width = 2 * LANES
        for n in range(faces // width):
            at = slice(n * width, (n + 1) * width)
            low = jnp.dot(
                ext_hi[rows, 0:own], own_hot[:, at], preferred_element_type=F32
            ) + jnp.dot(ext_lo[rows, 0:own], own_hot[:, at], preferred_element_type=F32)
            upp = jnp.dot(
                ext_hi[rows, :], up_hot[:, at], preferred_element_type=F32
            ) + jnp.dot(ext_lo[rows, :], up_hot[:, at], preferred_element_type=F32)
            for i in range(2 * CHUNK):
                p = chunk * 2 * CHUNK + i
                there = slice(i * ROWS, (i + 1) * ROWS)
                for h in range(2):
                    inner = slice(h * LANES, (h + 1) * LANES)
                    u = jnp.broadcast_to(
                        vel[p, 2 * n + h : 2 * n + h + 1, :], (ROWS, LANES)
                    )
                    flow = u * jnp.where(u > 0.0, low[there, inner], upp[there, inner])
                    high, rest = split(flow)
                    outer = slice(n * width + h * LANES, n * width + (h + 1) * LANES)
                    flux_hi[there, outer] = high
                    flux_lo[there, outer] = rest
        total = jnp.dot(flux_hi[...], back_hot[...], preferred_element_type=F32) + jnp.dot(
            flux_lo[...], back_hot[...], preferred_element_type=F32
        )
        for i in range(2 * CHUNK):
            p = chunk * 2 * CHUNK + i
            moved[p] = cur[p] - scale[...] * total[i * ROWS : i * ROWS + nfreq]

    def one_step(step, carry):
        compute(step, 0)
        edge_sent[step] = moved[0:2]
        edge_copy(step).start()
        finish_pair(step, 1)
        compute(step, 1)
        edge_copy(step).wait_recv()
        for pair in (0, 2, 3, 4):
            finish_pair(step, pair)
        compute(step, 2)
        for pair in (5, 6, 7, 8):
            finish_pair(step, pair)
        return carry

    lax.fori_loop(0, ITERS, one_step, 0)

    for side in (0, 1):

        @pl.when(has[side])
        def _():
            tables[side].wait_send()

    def drain(step, carry):
        edge_copy(step).wait_send()
        for side in (0, 1):

            @pl.when(has[side])
            def _():
                def inner(pair, c):
                    halo_copy(step, side, pair).wait_send()
                    return c

                lax.fori_loop(0, pairs, inner, 0)

        return carry

    lax.fori_loop(0, ITERS, drain, 0)
    for pair in range(pairs):
        for copy in store_pair(pair):
            copy.wait()


def on_device(
    field,
    group_speed,
    face_angle,
    face_speed,
    face_cells,
    face_live,
    halo_blocks,
    cell_level,
    polar_mask,
    turn_rate,
):
    dloc, nfreq, own = field.shape
    faces = face_angle.shape[0]
    fblk = faces // LANES
    hb = halo_blocks.shape[2]
    ext = own + 2 * hb * LANES
    pairs = dloc // 2
    any_spec = pl.BlockSpec(memory_space=pl.ANY)
    smem_spec = pl.BlockSpec(memory_space=pltpu.SMEM)
    halo = (ITERS, 2, pairs, 2, hb, nfreq, LANES)
    span = 2 * CHUNK * ROWS
    return pl.pallas_call(
        kernel,
        out_shape=jax.ShapeDtypeStruct(field.shape, field.dtype),
        in_specs=[
            any_spec,
            smem_spec,
            any_spec,
            any_spec,
            any_spec,
            smem_spec,
            any_spec,
            any_spec,
            any_spec,
            any_spec,
        ],
        out_specs=any_spec,
        scratch_shapes=[
            pltpu.VMEM((dloc, nfreq, own), F32),
            pltpu.VMEM((dloc, nfreq, own), F32),
            pltpu.VMEM(halo, F32),
            pltpu.VMEM(halo, F32),
            pltpu.VMEM((ITERS, 2, nfreq, own), F32),
            pltpu.VMEM((ITERS, 2, nfreq, own), F32),
            pltpu.VMEM((dloc * ROWS, ext), BF16),
            pltpu.VMEM((dloc * ROWS, ext), BF16),
            pltpu.VMEM((span, faces), BF16),
            pltpu.VMEM((span, faces), BF16),
            pltpu.VMEM((own, faces), BF16),
            pltpu.VMEM((ext, faces), BF16),
            pltpu.VMEM((faces, own), BF16),
            pltpu.VMEM((dloc, fblk, LANES), F32),
            pltpu.VMEM((nfreq, own), F32),
            pltpu.VMEM((2, own), F32),
            pltpu.VMEM((fblk, LANES), F32),
            pltpu.VMEM((fblk, LANES), F32),
            pltpu.VMEM((2, faces), jnp.int32),
            pltpu.VMEM((1, own), jnp.int32),
            pltpu.VMEM((1, own), jnp.int32),
            pltpu.VMEM((1, own), F32),
            pltpu.VMEM((1, 2, hb), jnp.int32),
            pltpu.VMEM((2, 1, 2, hb), jnp.int32),
            pltpu.VMEM((2 * hb, 8, LANES), jnp.int32),
            pltpu.SemaphoreType.DMA((dloc,)),
            pltpu.SemaphoreType.DMA((dloc,)),
            pltpu.SemaphoreType.DMA((7,)),
            pltpu.SemaphoreType.DMA((2,)),
            pltpu.SemaphoreType.DMA((2,)),
            pltpu.SemaphoreType.DMA((ITERS, 2, pairs)),
            pltpu.SemaphoreType.DMA((ITERS, 2, pairs)),
            pltpu.SemaphoreType.DMA((ITERS,)),
            pltpu.SemaphoreType.DMA((ITERS,)),
        ],
        compiler_params=pltpu.CompilerParams(
            collective_id=0, has_side_effects=True, vmem_limit_bytes=60 * 1024 * 1024
        ),
    )(
        field,
        group_speed,
        face_angle.reshape(fblk, LANES),
        face_speed.reshape(fblk, LANES),
        face_cells,
        face_live,
        halo_blocks,
        cell_level.reshape(1, own),
        polar_mask.reshape(1, own),
        turn_rate.reshape(1, own),
    )


def solution(mesh):
    return jax.shard_map(
        on_device,
        mesh=mesh,
        in_specs=(
            P("spec", None, "rows"),
            P(),
            P("rows"),
            P("rows"),
            P(None, "rows"),
            P("rows"),
            P("rows", None, None),
            P("rows"),
            P("rows"),
            P("rows"),
        ),
        out_specs=P("spec", None, "rows"),
        check_vma=False,
    )
```

```python
import functools
import math

import jax
import jax.numpy as jnp
from jax import lax
from jax.experimental import pallas as pl
from jax.experimental.pallas import tpu as pltpu
from jax.sharding import PartitionSpec as P

MESH = pl.DeviceIdType.MESH
NDIR = 36
ITERS = 3
LANES = 128
ROWS = 32
CHUNK = 3
BF16 = jnp.bfloat16
F32 = jnp.float32


def split(value):
    high = value.astype(BF16)
    return high, (value - high.astype(F32)).astype(BF16)


def kernel(
    field,
    speed_s,
    angle_h,
    weight_h,
    cells_h,
    live_s,
    table_h,
    level_h,
    mask_h,
    rate_h,
    out,
    cur,
    moved,
    sent,
    got,
    edge_sent,
    edge_got,
    ext,
    flux,
    own_hot,
    up_hot,
    back_hot,
    vel,
    scale,
    turn,
    angle,
    weight,
    cells,
    level,
    mask,
    rate,
    table_v,
    table_r,
    picks,
    full,
    load_sem,
    small_sem,
    table_send,
    table_recv,
    full_send,
    full_recv,
    send_sem,
    recv_sem,
    edge_send,
    edge_recv,
):
    dloc, nfreq, own = field.shape
    pairs = dloc // 2
    span = 2 * CHUNK * ROWS
    hb = table_h.shape[2]
    faces = cells.shape[1]
    fblk = faces // LANES
    size = lax.axis_size("rows")
    row = lax.axis_index("rows")
    spec = lax.axis_index("spec")
    has = (row > 0, row < size - 1)
    peer = ({"rows": jnp.maximum(row - 1, 0)}, {"rows": jnp.minimum(row + 1, size - 1)})
    partner = {"spec": 1 - spec}

    def slot(d):
        return 2 * d if d < pairs else 2 * (dloc - 1 - d) + 1

    def direction(p):
        return p // 2 if p % 2 == 0 else dloc - 1 - p // 2

    small = [
        pltpu.make_async_copy(src, dst, small_sem.at[i])
        for i, (src, dst) in enumerate(
            (
                (table_h, table_v),
                (cells_h, cells),
                (angle_h, angle),
                (weight_h, weight),
                (level_h, level),
                (mask_h, mask),
                (rate_h, rate),
            )
        )
    ]
    for copy in small:
        copy.start()
    loads = [
        pltpu.make_async_copy(
            field.at[direction(p)], cur.at[p], load_sem.at[p]
        )
        for p in range(dloc)
    ]
    for copy in loads:
        copy.start()
    table_r[...] = jnp.zeros_like(table_r)

    barrier = pltpu.get_barrier_semaphore()
    pl.semaphore_signal(barrier, inc=1, device_id=partner, device_id_type=MESH)
    for side in (0, 1):

        @pl.when(has[side])
        def _():
            pl.semaphore_signal(barrier, inc=1, device_id=peer[side], device_id_type=MESH)

    pl.semaphore_wait(barrier, 1 + has[0].astype(jnp.int32) + has[1].astype(jnp.int32))

    small[0].wait()
    tables = [
        pltpu.make_async_remote_copy(
            src_ref=table_v,
            dst_ref=table_r.at[1 - side],
            send_sem=table_send.at[side],
            recv_sem=table_recv.at[1 - side],
            device_id=peer[side],
            device_id_type=MESH,
        )
        for side in (0, 1)
    ]
    for side in (0, 1):

        @pl.when(has[side])
        def _():
            tables[side].start()

    def full_copy(side, p):
        return pltpu.make_async_remote_copy(
            src_ref=field.at[direction(p)],
            dst_ref=full.at[1 - side, p],
            send_sem=full_send.at[side, p],
            recv_sem=full_recv.at[1 - side, p],
            device_id=peer[side],
            device_id_type=MESH,
        )

    def full_arrival(side, p):
        return pltpu.make_async_remote_copy(
            src_ref=field.at[direction(p)],
            dst_ref=full.at[side, p],
            send_sem=full_send.at[side, p],
            recv_sem=full_recv.at[side, p],
            device_id=peer[side],
            device_id_type=MESH,
        )

    for side in (0, 1):

        @pl.when(has[side])
        def _():
            for p in range(2 * CHUNK):
                full_copy(side, p).start()

    for copy in small[1:]:
        copy.wait()

    sub = lax.broadcasted_iota(jnp.int32, (LANES, LANES), 0)
    lane = lax.broadcasted_iota(jnp.int32, (LANES, LANES), 1)
    one = jnp.float32(1.0)
    zero = jnp.float32(0.0)

    def build(j, carry):
        at = pl.ds(pl.multiple_of(j * LANES, LANES), LANES)
        low = jnp.broadcast_to(cells[0:1, at], (LANES, LANES))
        upp = jnp.broadcast_to(cells[1:2, at], (LANES, LANES))
        for c in range(own // LANES):
            own_hot[c * LANES : (c + 1) * LANES, at] = jnp.where(
                low == sub + c * LANES, one, zero
            ).astype(BF16)
        for c in range(up_hot.shape[0] // LANES):
            up_hot[c * LANES : (c + 1) * LANES, at] = jnp.where(
                upp == sub + c * LANES, one, zero
            ).astype(BF16)
        low_t = low.T
        upp_t = upp.T
        for c in range(own // LANES):
            here = lane + c * LANES
            back_hot[at, c * LANES : (c + 1) * LANES] = (
                jnp.where(low_t == here, one, zero) - jnp.where(upp_t == here, one, zero)
            ).astype(BF16)
        return carry

    lax.fori_loop(0, fblk, build, 0)

    blocks = lax.broadcasted_iota(jnp.int32, (fblk, LANES), 0)
    slot_weight = jnp.where(blocks < live_s[0], weight[...], zero)
    along = jnp.cos(angle[...]) * slot_weight
    across = jnp.sin(angle[...]) * slot_weight
    sign = (1 - 2 * spec).astype(F32)
    along = along * sign
    across = across * sign
    for p in range(dloc):
        theta = (direction(p) + 0.5) * (2.0 * math.pi / NDIR)
        vel[p] = along * math.cos(theta) + across * math.sin(theta)

    freq = lax.broadcasted_iota(jnp.int32, (nfreq, LANES), 0)
    group = jnp.zeros((nfreq, LANES), F32)
    for f in range(nfreq):
        group = jnp.where(freq == f, speed_s[f], group)
    for c in range(own // LANES):
        lev = level[0:1, c * LANES : (c + 1) * LANES]
        area = jnp.exp2(-lev.astype(F32))
        scale[:, c * LANES : (c + 1) * LANES] = group * area
    bend = mask[...].astype(F32) * rate[...]
    turn[0:1, :] = jnp.maximum(bend, 0.0)
    turn[1:2, :] = jnp.minimum(bend, 0.0)

    for side in (0, 1):

        @pl.when(jnp.logical_not(has[side]))
        def _():
            def clear(i, carry):
                def inner(j, c):
                    got[i, side, j] = jnp.zeros(got.shape[3:], F32)
                    return c

                return lax.fori_loop(0, pairs, inner, carry)

            lax.fori_loop(0, ITERS, clear, 0)

    for side in (0, 1):

        @pl.when(has[side])
        def _():
            pltpu.make_async_remote_copy(
                src_ref=table_v,
                dst_ref=table_r.at[side],
                send_sem=table_send.at[side],
                recv_sem=table_recv.at[side],
                device_id=peer[side],
                device_id_type=MESH,
            ).wait_recv()

    for side in (0, 1):
        taken = table_r[side, 0]
        for k in range(hb):
            picks[side * hb + k] = jnp.broadcast_to(
                taken[1 - side : 2 - side, k : k + 1], (8, LANES)
            )

    mine = table_v[0]
    for side in (0, 1):
        for k in range(hb):
            picks[(2 + side) * hb + k] = jnp.broadcast_to(
                mine[side : side + 1, k : k + 1], (8, LANES)
            )

    def pick(value, which):
        wanted = jnp.broadcast_to(picks[which, 0:1, :], (nfreq, LANES))
        chosen = value[:, 0:LANES]
        for c in range(1, own // LANES):
            chosen = jnp.where(wanted == c, value[:, c * LANES : (c + 1) * LANES], chosen)
        return chosen

    def halo_copy(step, side, pair):
        return pltpu.make_async_remote_copy(
            src_ref=sent.at[step, side, pair],
            dst_ref=got.at[step, 1 - side, pair],
            send_sem=send_sem.at[step, side, pair],
            recv_sem=recv_sem.at[step, 1 - side, pair],
            device_id=peer[side],
            device_id_type=MESH,
        )

    def halo_arrival(step, side, pair):
        return pltpu.make_async_remote_copy(
            src_ref=sent.at[step, side, pair],
            dst_ref=got.at[step, side, pair],
            send_sem=send_sem.at[step, side, pair],
            recv_sem=recv_sem.at[step, side, pair],
            device_id=peer[side],
            device_id_type=MESH,
        )

    def send_pair(step, pair):
        for side in (0, 1):
            for e in (0, 1):
                value = cur[2 * pair + e]
                for k in range(hb):
                    sent[step, side, pair, e, k] = pick(value, side * hb + k)

            @pl.when(has[side])
            def _():
                halo_copy(step, side, pair).start()

    def put(p, at, value):
        first = (p // (2 * CHUNK)) * 2 * span + (p % (2 * CHUNK)) * ROWS
        high, low = split(value)
        ext[first : first + nfreq, at] = high
        ext[first + span : first + span + nfreq, at] = low

    def split_own(p):
        put(p, slice(0, own), cur[p])

    for copy in loads:
        copy.wait()
    for pair in range(CHUNK, pairs):
        send_pair(0, pair)
    for p in range(dloc):
        split_own(p)
    for side in (0, 1):

        @pl.when(has[side])
        def _():
            for p in range(2 * CHUNK):
                full_arrival(side, p).wait_recv()
                value = full[side, p]
                for k in range(hb):
                    got[0, side, p // 2, p % 2, k] = pick(value, (2 + side) * hb + k)

    def turn_slot(step, p):
        d = direction(p)
        here = moved[p]
        before = moved[slot(d - 1)] if d > 0 else edge_got[step, 1]
        after = moved[slot(d + 1)] if d < dloc - 1 else edge_got[step, 0]
        cur[p] = here - turn[0:1, :] * (here - before) - turn[1:2, :] * (after - here)
        split_own(p)

    def edge_copy(step):
        return pltpu.make_async_remote_copy(
            src_ref=edge_sent.at[step],
            dst_ref=edge_got.at[step],
            send_sem=edge_send.at[step],
            recv_sem=edge_recv.at[step],
            device_id=partner,
            device_id_type=MESH,
        )

    def finish_pair(step, pair):
        turn_slot(step, 2 * pair)
        turn_slot(step, 2 * pair + 1)

        @pl.when(step < ITERS - 1)
        def _():
            send_pair(step + 1, pair)

        @pl.when(step == ITERS - 1)
        def _():
            for p in (2 * pair, 2 * pair + 1):
                out[direction(p)] = cur[p]

    def compute(step, chunk):
        rows = slice(chunk * 2 * span, (chunk + 1) * 2 * span)
        for i in range(CHUNK):
            pair = chunk * CHUNK + i
            for side in (0, 1):

                awaited = has[side] if chunk > 0 else has[side] & (step > 0)

                @pl.when(awaited)
                def _():
                    halo_arrival(step, side, pair).wait_recv()

            for side in (0, 1):
                for e in (0, 1):
                    for k in range(hb):
                        first = own + (side * hb + k) * LANES
                        put(2 * pair + e, slice(first, first + LANES), got[step, side, pair, e, k])
        width = 2 * LANES
        for n in range(faces // width):
            at = slice(n * width, (n + 1) * width)
            low = jnp.dot(ext[rows, 0:own], own_hot[:, at], preferred_element_type=F32)
            upp = jnp.dot(ext[rows, :], up_hot[:, at], preferred_element_type=F32)
            low = low[0:span] + low[span : 2 * span]
            upp = upp[0:span] + upp[span : 2 * span]
            for i in range(2 * CHUNK):
                p = chunk * 2 * CHUNK + i
                there = slice(i * ROWS, (i + 1) * ROWS)
                for h in range(2):
                    inner = slice(h * LANES, (h + 1) * LANES)
                    u = jnp.broadcast_to(
                        vel[p, 2 * n + h : 2 * n + h + 1, :], (ROWS, LANES)
                    )
                    flow = u * jnp.where(u > 0.0, low[there, inner], upp[there, inner])
                    high, rest = split(flow)
                    outer = slice(n * width + h * LANES, n * width + (h + 1) * LANES)
                    flux[there, outer] = high
                    flux[slice(span + i * ROWS, span + (i + 1) * ROWS), outer] = rest
        total = jnp.dot(flux[...], back_hot[...], preferred_element_type=F32)
        total = total[0:span] + total[span : 2 * span]
        for i in range(2 * CHUNK):
            p = chunk * 2 * CHUNK + i
            moved[p] = cur[p] - scale[...] * total[i * ROWS : i * ROWS + nfreq]

    def one_step(step, carry):
        compute(step, 0)
        edge_sent[step] = moved[0:2]
        edge_copy(step).start()
        finish_pair(step, 1)
        compute(step, 1)
        edge_copy(step).wait_recv()
        for pair in (0, 2, 3, 4):
            finish_pair(step, pair)
        compute(step, 2)
        for pair in (5, 6, 7, 8):
            finish_pair(step, pair)
        return carry

    lax.fori_loop(0, ITERS, one_step, 0)

    for step in range(ITERS):
        edge_copy(step).wait_send()
    for side in (0, 1):

        @pl.when(has[side])
        def _():
            tables[side].wait_send()
            for p in range(2 * CHUNK):
                full_copy(side, p).wait_send()
            for step in range(ITERS):
                for pair in range(CHUNK if step == 0 else 0, pairs):
                    halo_copy(step, side, pair).wait_send()


def on_device(
    field,
    group_speed,
    face_angle,
    face_speed,
    face_cells,
    face_live,
    halo_blocks,
    cell_level,
    polar_mask,
    turn_rate,
):
    dloc, nfreq, own = field.shape
    faces = face_angle.shape[0]
    fblk = faces // LANES
    hb = halo_blocks.shape[2]
    ext = own + 2 * hb * LANES
    pairs = dloc // 2
    any_spec = pl.BlockSpec(memory_space=pl.ANY)
    smem_spec = pl.BlockSpec(memory_space=pltpu.SMEM)
    halo = (ITERS, 2, pairs, 2, hb, nfreq, LANES)
    span = 2 * CHUNK * ROWS
    return pl.pallas_call(
        kernel,
        out_shape=pltpu.VMEM(field.shape, field.dtype),
        in_specs=[
            any_spec,
            smem_spec,
            any_spec,
            any_spec,
            any_spec,
            smem_spec,
            any_spec,
            any_spec,
            any_spec,
            any_spec,
        ],
        out_specs=pl.BlockSpec(memory_space=pltpu.VMEM),
        scratch_shapes=[
            pltpu.VMEM((dloc, nfreq, own), F32),
            pltpu.VMEM((dloc, nfreq, own), F32),
            pltpu.VMEM(halo, F32),
            pltpu.VMEM(halo, F32),
            pltpu.VMEM((ITERS, 2, nfreq, own), F32),
            pltpu.VMEM((ITERS, 2, nfreq, own), F32),
            pltpu.VMEM((2 * dloc * ROWS, ext), BF16),
            pltpu.VMEM((2 * span, faces), BF16),
            pltpu.VMEM((own, faces), BF16),
            pltpu.VMEM((ext, faces), BF16),
            pltpu.VMEM((faces, own), BF16),
            pltpu.VMEM((dloc, fblk, LANES), F32),
            pltpu.VMEM((nfreq, own), F32),
            pltpu.VMEM((2, own), F32),
            pltpu.VMEM((fblk, LANES), F32),
            pltpu.VMEM((fblk, LANES), F32),
            pltpu.VMEM((2, faces), jnp.int32),
            pltpu.VMEM((1, own), jnp.int32),
            pltpu.VMEM((1, own), jnp.int32),
            pltpu.VMEM((1, own), F32),
            pltpu.VMEM((1, 2, hb), jnp.int32),
            pltpu.VMEM((2, 1, 2, hb), jnp.int32),
            pltpu.VMEM((4 * hb, 8, LANES), jnp.int32),
            pltpu.VMEM((2, 2 * CHUNK, nfreq, own), F32),
            pltpu.SemaphoreType.DMA((dloc,)),
            pltpu.SemaphoreType.DMA((7,)),
            pltpu.SemaphoreType.DMA((2,)),
            pltpu.SemaphoreType.DMA((2,)),
            pltpu.SemaphoreType.DMA((2, 2 * CHUNK)),
            pltpu.SemaphoreType.DMA((2, 2 * CHUNK)),
            pltpu.SemaphoreType.DMA((ITERS, 2, pairs)),
            pltpu.SemaphoreType.DMA((ITERS, 2, pairs)),
            pltpu.SemaphoreType.DMA((ITERS,)),
            pltpu.SemaphoreType.DMA((ITERS,)),
        ],
        compiler_params=pltpu.CompilerParams(
            collective_id=0, has_side_effects=True, vmem_limit_bytes=60 * 1024 * 1024
        ),
    )(
        field,
        group_speed,
        face_angle.reshape(fblk, LANES),
        face_speed.reshape(fblk, LANES),
        face_cells,
        face_live,
        halo_blocks,
        cell_level.reshape(1, own),
        polar_mask.reshape(1, own),
        turn_rate.reshape(1, own),
    )


def solution(mesh):
    return jax.shard_map(
        on_device,
        mesh=mesh,
        in_specs=(
            P("spec", None, "rows"),
            P(),
            P("rows"),
            P("rows"),
            P(None, "rows"),
            P("rows"),
            P("rows", None, None),
            P("rows"),
            P("rows"),
            P("rows"),
        ),
        out_specs=P("spec", None, "rows"),
        check_vma=False,
    )
```

```python
import functools
import math

import jax
import jax.numpy as jnp
from jax import lax
from jax.experimental import pallas as pl
from jax.experimental.pallas import tpu as pltpu
from jax.sharding import PartitionSpec as P

MESH = pl.DeviceIdType.MESH
NDIR = 36
ITERS = 3
LANES = 128
ROWS = 32
CHUNKS = ((0, 2), (2, 2), (4, 2), (6, 2), (8, 1))
AHEAD = 2
EDGE_AT = 2
HOT = jnp.float8_e4m3fn
BF16 = jnp.bfloat16
F32 = jnp.float32


def split(value):
    high = value.astype(BF16)
    return high, (value - high.astype(F32)).astype(BF16)


def kernel(
    field,
    speed_s,
    angle_h,
    weight_h,
    cells_h,
    live_s,
    table_h,
    level_h,
    mask_h,
    rate_h,
    out,
    cur,
    moved,
    sent,
    got,
    edge_sent,
    edge_got,
    ext,
    flux,
    own_hot,
    up_hot,
    back_hot,
    vel,
    scale,
    turn,
    angle,
    weight,
    cells,
    level,
    mask,
    rate,
    table_v,
    table_r,
    picks,
    full,
    load_sem,
    small_sem,
    table_send,
    table_recv,
    full_send,
    full_recv,
    send_sem,
    recv_sem,
    edge_send,
    edge_recv,
):
    dloc, nfreq, own = field.shape
    pairs = dloc // 2
    hb = table_h.shape[2]
    faces = cells.shape[1]
    fblk = faces // LANES
    size = lax.axis_size("rows")
    row = lax.axis_index("rows")
    spec = lax.axis_index("spec")
    has = (row > 0, row < size - 1)
    peer = ({"rows": jnp.maximum(row - 1, 0)}, {"rows": jnp.minimum(row + 1, size - 1)})
    partner = {"spec": 1 - spec}

    def slot(d):
        return 2 * d if d < pairs else 2 * (dloc - 1 - d) + 1

    def direction(p):
        return p // 2 if p % 2 == 0 else dloc - 1 - p // 2

    small = [
        pltpu.make_async_copy(src, dst, small_sem.at[i])
        for i, (src, dst) in enumerate(
            (
                (table_h, table_v),
                (cells_h, cells),
                (angle_h, angle),
                (weight_h, weight),
                (level_h, level),
                (mask_h, mask),
                (rate_h, rate),
            )
        )
    ]
    for copy in small:
        copy.start()
    loads = [
        pltpu.make_async_copy(
            field.at[direction(p)], cur.at[p], load_sem.at[p]
        )
        for p in range(dloc)
    ]
    for copy in loads:
        copy.start()
    table_r[...] = jnp.zeros_like(table_r)

    barrier = pltpu.get_barrier_semaphore()
    pl.semaphore_signal(barrier, inc=1, device_id=partner, device_id_type=MESH)
    for side in (0, 1):

        @pl.when(has[side])
        def _():
            pl.semaphore_signal(barrier, inc=1, device_id=peer[side], device_id_type=MESH)

    pl.semaphore_wait(barrier, 1 + has[0].astype(jnp.int32) + has[1].astype(jnp.int32))

    small[0].wait()
    tables = [
        pltpu.make_async_remote_copy(
            src_ref=table_v,
            dst_ref=table_r.at[1 - side],
            send_sem=table_send.at[side],
            recv_sem=table_recv.at[1 - side],
            device_id=peer[side],
            device_id_type=MESH,
        )
        for side in (0, 1)
    ]
    for side in (0, 1):

        @pl.when(has[side])
        def _():
            tables[side].start()

    def full_copy(side, p):
        return pltpu.make_async_remote_copy(
            src_ref=field.at[direction(p)],
            dst_ref=full.at[1 - side, p],
            send_sem=full_send.at[side, p],
            recv_sem=full_recv.at[1 - side, p],
            device_id=peer[side],
            device_id_type=MESH,
        )

    def full_arrival(side, p):
        return pltpu.make_async_remote_copy(
            src_ref=field.at[direction(p)],
            dst_ref=full.at[side, p],
            send_sem=full_send.at[side, p],
            recv_sem=full_recv.at[side, p],
            device_id=peer[side],
            device_id_type=MESH,
        )

    for side in (0, 1):

        @pl.when(has[side])
        def _():
            for p in range(2 * AHEAD):
                full_copy(side, p).start()

    for copy in small[1:]:
        copy.wait()

    sub = lax.broadcasted_iota(jnp.int32, (LANES, LANES), 0)
    lane = lax.broadcasted_iota(jnp.int32, (LANES, LANES), 1)
    one = jnp.float32(1.0)
    zero = jnp.float32(0.0)

    def build(j, carry):
        at = pl.ds(pl.multiple_of(j * LANES, LANES), LANES)
        low = jnp.broadcast_to(cells[0:1, at], (LANES, LANES))
        upp = jnp.broadcast_to(cells[1:2, at], (LANES, LANES))
        for c in range(own // LANES):
            own_hot[c * LANES : (c + 1) * LANES, at] = jnp.where(
                low == sub + c * LANES, one, zero
            ).astype(HOT)
        for c in range(up_hot.shape[0] // LANES):
            up_hot[c * LANES : (c + 1) * LANES, at] = jnp.where(
                upp == sub + c * LANES, one, zero
            ).astype(HOT)
        low_t = low.T
        upp_t = upp.T
        for c in range(own // LANES):
            here = lane + c * LANES
            back_hot[at, c * LANES : (c + 1) * LANES] = (
                jnp.where(low_t == here, one, zero) - jnp.where(upp_t == here, one, zero)
            ).astype(HOT)
        return carry

    lax.fori_loop(0, fblk, build, 0)

    blocks = lax.broadcasted_iota(jnp.int32, (fblk, LANES), 0)
    slot_weight = jnp.where(blocks < live_s[0], weight[...], zero)
    along = jnp.cos(angle[...]) * slot_weight
    across = jnp.sin(angle[...]) * slot_weight
    sign = (1 - 2 * spec).astype(F32)
    along = along * sign
    across = across * sign
    for p in range(dloc):
        theta = (direction(p) + 0.5) * (2.0 * math.pi / NDIR)
        vel[p] = along * math.cos(theta) + across * math.sin(theta)

    freq = lax.broadcasted_iota(jnp.int32, (nfreq, LANES), 0)
    group = jnp.zeros((nfreq, LANES), F32)
    for f in range(nfreq):
        group = jnp.where(freq == f, speed_s[f], group)
    for c in range(own // LANES):
        lev = level[0:1, c * LANES : (c + 1) * LANES]
        area = jnp.exp2(-lev.astype(F32))
        scale[:, c * LANES : (c + 1) * LANES] = group * area
    bend = mask[...].astype(F32) * rate[...]
    turn[0:1, :] = jnp.maximum(bend, 0.0)
    turn[1:2, :] = jnp.minimum(bend, 0.0)

    for side in (0, 1):

        @pl.when(jnp.logical_not(has[side]))
        def _():
            def clear(i, carry):
                def inner(j, c):
                    got[i, side, j] = jnp.zeros(got.shape[3:], F32)
                    return c

                return lax.fori_loop(0, pairs, inner, carry)

            lax.fori_loop(0, ITERS, clear, 0)

    for side in (0, 1):

        @pl.when(has[side])
        def _():
            pltpu.make_async_remote_copy(
                src_ref=table_v,
                dst_ref=table_r.at[side],
                send_sem=table_send.at[side],
                recv_sem=table_recv.at[side],
                device_id=peer[side],
                device_id_type=MESH,
            ).wait_recv()

    for side in (0, 1):
        taken = table_r[side, 0]
        for k in range(hb):
            picks[side * hb + k] = jnp.broadcast_to(
                taken[1 - side : 2 - side, k : k + 1], (8, LANES)
            )

    mine = table_v[0]
    for side in (0, 1):
        for k in range(hb):
            picks[(2 + side) * hb + k] = jnp.broadcast_to(
                mine[side : side + 1, k : k + 1], (8, LANES)
            )

    def pick(value, which):
        wanted = jnp.broadcast_to(picks[which, 0:1, :], (nfreq, LANES))
        chosen = value[:, 0:LANES]
        for c in range(1, own // LANES):
            chosen = jnp.where(wanted == c, value[:, c * LANES : (c + 1) * LANES], chosen)
        return chosen

    def halo_copy(step, side, pair):
        return pltpu.make_async_remote_copy(
            src_ref=sent.at[step, side, pair],
            dst_ref=got.at[step, 1 - side, pair],
            send_sem=send_sem.at[step, side, pair],
            recv_sem=recv_sem.at[step, 1 - side, pair],
            device_id=peer[side],
            device_id_type=MESH,
        )

    def halo_arrival(step, side, pair):
        return pltpu.make_async_remote_copy(
            src_ref=sent.at[step, side, pair],
            dst_ref=got.at[step, side, pair],
            send_sem=send_sem.at[step, side, pair],
            recv_sem=recv_sem.at[step, side, pair],
            device_id=peer[side],
            device_id_type=MESH,
        )

    def send_pair(step, pair):
        for side in (0, 1):
            for e in (0, 1):
                value = cur[2 * pair + e]
                for k in range(hb):
                    sent[step, side, pair, e, k] = pick(value, side * hb + k)

            @pl.when(has[side])
            def _():
                halo_copy(step, side, pair).start()

    home = {}
    for begin, count in CHUNKS:
        for p in range(2 * begin, 2 * (begin + count)):
            home[p] = (4 * begin * ROWS + (p - 2 * begin) * ROWS, 2 * count * ROWS)

    def put(p, at, value):
        first, span = home[p]
        high, low = split(value)
        ext[first : first + nfreq, at] = high
        ext[first + span : first + span + nfreq, at] = low

    def split_own(p):
        put(p, slice(0, own), cur[p])

    for copy in loads:
        copy.wait()
    for pair in range(AHEAD, pairs):
        send_pair(0, pair)
    for p in range(dloc):
        split_own(p)
    for side in (0, 1):

        @pl.when(has[side])
        def _():
            for p in range(2 * AHEAD):
                full_arrival(side, p).wait_recv()
                value = full[side, p]
                for k in range(hb):
                    got[0, side, p // 2, p % 2, k] = pick(value, (2 + side) * hb + k)

    def turn_slot(step, p):
        d = direction(p)
        here = moved[p]
        before = moved[slot(d - 1)] if d > 0 else edge_got[step, 1]
        after = moved[slot(d + 1)] if d < dloc - 1 else edge_got[step, 0]
        cur[p] = here - turn[0:1, :] * (here - before) - turn[1:2, :] * (after - here)
        split_own(p)

    def edge_copy(step):
        return pltpu.make_async_remote_copy(
            src_ref=edge_sent.at[step],
            dst_ref=edge_got.at[step],
            send_sem=edge_send.at[step],
            recv_sem=edge_recv.at[step],
            device_id=partner,
            device_id_type=MESH,
        )

    def finish_pair(step, pair):
        turn_slot(step, 2 * pair)
        turn_slot(step, 2 * pair + 1)

        @pl.when(step < ITERS - 1)
        def _():
            send_pair(step + 1, pair)

        @pl.when(step == ITERS - 1)
        def _():
            for p in (2 * pair, 2 * pair + 1):
                out[direction(p)] = cur[p]

    def compute(step, chunk):
        begin, count = CHUNKS[chunk]
        span = 2 * count * ROWS
        rows = slice(4 * begin * ROWS, 4 * begin * ROWS + 2 * span)
        for pair in range(begin, begin + count):
            for side in (0, 1):
                awaited = has[side] if pair >= AHEAD else has[side] & (step > 0)

                @pl.when(awaited)
                def _():
                    halo_arrival(step, side, pair).wait_recv()

            for side in (0, 1):
                for e in (0, 1):
                    for k in range(hb):
                        first = own + (side * hb + k) * LANES
                        put(2 * pair + e, slice(first, first + LANES), got[step, side, pair, e, k])
        width = 2 * LANES
        for n in range(faces // width):
            at = slice(n * width, (n + 1) * width)
            low = jnp.dot(ext[rows, 0:own], own_hot[:, at], preferred_element_type=F32)
            upp = jnp.dot(ext[rows, :], up_hot[:, at], preferred_element_type=F32)
            low = low[0:span] + low[span : 2 * span]
            upp = upp[0:span] + upp[span : 2 * span]
            for i in range(2 * count):
                p = 2 * begin + i
                there = slice(i * ROWS, (i + 1) * ROWS)
                for h in range(2):
                    inner = slice(h * LANES, (h + 1) * LANES)
                    u = jnp.broadcast_to(
                        vel[p, 2 * n + h : 2 * n + h + 1, :], (ROWS, LANES)
                    )
                    flow = u * jnp.where(u > 0.0, low[there, inner], upp[there, inner])
                    high, rest = split(flow)
                    outer = slice(n * width + h * LANES, n * width + (h + 1) * LANES)
                    flux[there, outer] = high
                    flux[slice(span + i * ROWS, span + (i + 1) * ROWS), outer] = rest
        total = jnp.dot(flux[0 : 2 * span, :], back_hot[...], preferred_element_type=F32)
        total = total[0:span] + total[span : 2 * span]
        for i in range(2 * count):
            p = 2 * begin + i
            moved[p] = cur[p] - scale[...] * total[i * ROWS : i * ROWS + nfreq]

    def one_step(step, carry):
        done = 1
        for chunk, (begin, count) in enumerate(CHUNKS):
            compute(step, chunk)
            if chunk == 0:
                edge_sent[step] = moved[0:2]
                edge_copy(step).start()
            if chunk == EDGE_AT:
                edge_copy(step).wait_recv()
                finish_pair(step, 0)
            last = begin + count == pairs
            ready = pairs if last else begin + count - 1
            for pair in range(done, ready):
                finish_pair(step, pair)
            done = max(done, ready)
        return carry

    lax.fori_loop(0, ITERS, one_step, 0)

    for step in range(ITERS):
        edge_copy(step).wait_send()
    for side in (0, 1):

        @pl.when(has[side])
        def _():
            tables[side].wait_send()
            for p in range(2 * AHEAD):
                full_copy(side, p).wait_send()
            for step in range(ITERS):
                for pair in range(AHEAD if step == 0 else 0, pairs):
                    halo_copy(step, side, pair).wait_send()


def on_device(
    field,
    group_speed,
    face_angle,
    face_speed,
    face_cells,
    face_live,
    halo_blocks,
    cell_level,
    polar_mask,
    turn_rate,
):
    dloc, nfreq, own = field.shape
    faces = face_angle.shape[0]
    fblk = faces // LANES
    hb = halo_blocks.shape[2]
    ext = own + 2 * hb * LANES
    pairs = dloc // 2
    any_spec = pl.BlockSpec(memory_space=pl.ANY)
    smem_spec = pl.BlockSpec(memory_space=pltpu.SMEM)
    halo = (ITERS, 2, pairs, 2, hb, nfreq, LANES)
    span = 2 * max(count for _, count in CHUNKS) * ROWS
    return pl.pallas_call(
        kernel,
        out_shape=pltpu.VMEM(field.shape, field.dtype),
        in_specs=[
            any_spec,
            smem_spec,
            any_spec,
            any_spec,
            any_spec,
            smem_spec,
            any_spec,
            any_spec,
            any_spec,
            any_spec,
        ],
        out_specs=pl.BlockSpec(memory_space=pltpu.VMEM),
        scratch_shapes=[
            pltpu.VMEM((dloc, nfreq, own), F32),
            pltpu.VMEM((dloc, nfreq, own), F32),
            pltpu.VMEM(halo, F32),
            pltpu.VMEM(halo, F32),
            pltpu.VMEM((ITERS, 2, nfreq, own), F32),
            pltpu.VMEM((ITERS, 2, nfreq, own), F32),
            pltpu.VMEM((2 * dloc * ROWS, ext), BF16),
            pltpu.VMEM((2 * span, faces), BF16),
            pltpu.VMEM((own, faces), HOT),
            pltpu.VMEM((ext, faces), HOT),
            pltpu.VMEM((faces, own), HOT),
            pltpu.VMEM((dloc, fblk, LANES), F32),
            pltpu.VMEM((nfreq, own), F32),
            pltpu.VMEM((2, own), F32),
            pltpu.VMEM((fblk, LANES), F32),
            pltpu.VMEM((fblk, LANES), F32),
            pltpu.VMEM((2, faces), jnp.int32),
            pltpu.VMEM((1, own), jnp.int32),
            pltpu.VMEM((1, own), jnp.int32),
            pltpu.VMEM((1, own), F32),
            pltpu.VMEM((1, 2, hb), jnp.int32),
            pltpu.VMEM((2, 1, 2, hb), jnp.int32),
            pltpu.VMEM((4 * hb, 8, LANES), jnp.int32),
            pltpu.VMEM((2, 2 * AHEAD, nfreq, own), F32),
            pltpu.SemaphoreType.DMA((dloc,)),
            pltpu.SemaphoreType.DMA((7,)),
            pltpu.SemaphoreType.DMA((2,)),
            pltpu.SemaphoreType.DMA((2,)),
            pltpu.SemaphoreType.DMA((2, 2 * AHEAD)),
            pltpu.SemaphoreType.DMA((2, 2 * AHEAD)),
            pltpu.SemaphoreType.DMA((ITERS, 2, pairs)),
            pltpu.SemaphoreType.DMA((ITERS, 2, pairs)),
            pltpu.SemaphoreType.DMA((ITERS,)),
            pltpu.SemaphoreType.DMA((ITERS,)),
        ],
        compiler_params=pltpu.CompilerParams(
            collective_id=0, has_side_effects=True, vmem_limit_bytes=60 * 1024 * 1024
        ),
    )(
        field,
        group_speed,
        face_angle.reshape(fblk, LANES),
        face_speed.reshape(fblk, LANES),
        face_cells,
        face_live,
        halo_blocks,
        cell_level.reshape(1, own),
        polar_mask.reshape(1, own),
        turn_rate.reshape(1, own),
    )


def solution(mesh):
    return jax.shard_map(
        on_device,
        mesh=mesh,
        in_specs=(
            P("spec", None, "rows"),
            P(),
            P("rows"),
            P("rows"),
            P(None, "rows"),
            P("rows"),
            P("rows", None, None),
            P("rows"),
            P("rows"),
            P("rows"),
        ),
        out_specs=P("spec", None, "rows"),
        check_vma=False,
    )
```

```python
import functools
import math

import jax
import jax.numpy as jnp
from jax import lax
from jax.experimental import pallas as pl
from jax.experimental.pallas import tpu as pltpu
from jax.sharding import PartitionSpec as P

MESH = pl.DeviceIdType.MESH
NDIR = 36
ITERS = 3
LANES = 128
ROWS = 32
CHUNKS = ((0, 2), (2, 2), (4, 2), (6, 2), (8, 1))
AHEAD = 2
EDGE_AT = 2
PLANE = 32
UP, DOWN = 7, 25
HOT = jnp.float8_e4m3fn
BF16 = jnp.bfloat16
F32 = jnp.float32


def split(value):
    high = value.astype(BF16)
    return high, (value - high.astype(F32)).astype(BF16)


def kernel(
    field,
    speed_s,
    angle_h,
    weight_h,
    cells_h,
    live_s,
    table_h,
    level_h,
    mask_h,
    rate_h,
    out,
    cur,
    moved,
    sent,
    got,
    edge_sent,
    edge_got,
    ext,
    flux,
    own_hot,
    up_hot,
    back_hot,
    vel,
    scale,
    turn,
    angle,
    weight,
    cells,
    level,
    mask,
    rate,
    table_v,
    table_r,
    picks,
    full,
    passing,
    load_sem,
    small_sem,
    table_send,
    table_recv,
    full_send,
    full_recv,
    pass_send,
    pass_recv,
    send_sem,
    recv_sem,
    edge_send,
    edge_recv,
):
    dloc, nfreq, own = field.shape
    pairs = dloc // 2
    hb = table_h.shape[2]
    faces = cells.shape[1]
    fblk = faces // LANES
    size = lax.axis_size("rows")
    row = lax.axis_index("rows")
    spec = lax.axis_index("spec")
    has = (row > 0, row < size - 1)
    peer = ({"rows": jnp.maximum(row - 1, 0)}, {"rows": jnp.minimum(row + 1, size - 1)})
    partner = {"spec": 1 - spec}

    at = lax.rem(row, PLANE)
    odd = spec == 1

    def other(shift):
        return {"rows": jnp.clip(row + shift, 0, size - 1)}

    via = (odd & (at == 0) & (row > 0), odd & (at == PLANE - 1) & (row < size - 1))
    passes_up = odd & (at == UP) & (row < size - PLANE)
    passes_down = odd & (at == DOWN) & (row >= PLANE)
    relay = (other(DOWN), other(UP + 1 - PLANE))
    roles = (
        (via[0], relay[0], other(UP - PLANE)),
        (via[1], relay[1], other(DOWN + 1)),
        (passes_up, other(PLANE - 1 - UP), other(PLANE - UP)),
        (passes_down, other(-DOWN), other(-DOWN - 1)),
    )

    def slot(d):
        return 2 * d if d < pairs else 2 * (dloc - 1 - d) + 1

    def direction(p):
        return p // 2 if p % 2 == 0 else dloc - 1 - p // 2

    small = [
        pltpu.make_async_copy(src, dst, small_sem.at[i])
        for i, (src, dst) in enumerate(
            (
                (table_h, table_v),
                (cells_h, cells),
                (angle_h, angle),
                (weight_h, weight),
                (level_h, level),
                (mask_h, mask),
                (rate_h, rate),
            )
        )
    ]
    for copy in small:
        copy.start()
    loads = [
        pltpu.make_async_copy(
            field.at[direction(p)], cur.at[p], load_sem.at[p]
        )
        for p in range(dloc)
    ]
    for copy in loads:
        copy.start()
    table_r[...] = jnp.zeros_like(table_r)

    barrier = pltpu.get_barrier_semaphore()
    pl.semaphore_signal(barrier, inc=1, device_id=partner, device_id_type=MESH)
    for side in (0, 1):

        @pl.when(has[side])
        def _():
            pl.semaphore_signal(barrier, inc=1, device_id=peer[side], device_id_type=MESH)

    peers = 1 + has[0].astype(jnp.int32) + has[1].astype(jnp.int32)
    for role, first, second in roles:

        @pl.when(role)
        def _():
            pl.semaphore_signal(barrier, inc=1, device_id=first, device_id_type=MESH)
            pl.semaphore_signal(barrier, inc=1, device_id=second, device_id_type=MESH)

        peers = peers + 2 * role.astype(jnp.int32)
    pl.semaphore_wait(barrier, peers)

    small[0].wait()
    tables = [
        pltpu.make_async_remote_copy(
            src_ref=table_v,
            dst_ref=table_r.at[1 - side],
            send_sem=table_send.at[side],
            recv_sem=table_recv.at[1 - side],
            device_id=peer[side],
            device_id_type=MESH,
        )
        for side in (0, 1)
    ]
    for side in (0, 1):

        @pl.when(has[side])
        def _():
            tables[side].start()

    def full_copy(side, p):
        return pltpu.make_async_remote_copy(
            src_ref=field.at[direction(p)],
            dst_ref=full.at[1 - side, p],
            send_sem=full_send.at[side, p],
            recv_sem=full_recv.at[1 - side, p],
            device_id=peer[side],
            device_id_type=MESH,
        )

    def full_arrival(side, p):
        return pltpu.make_async_remote_copy(
            src_ref=field.at[direction(p)],
            dst_ref=full.at[side, p],
            send_sem=full_send.at[side, p],
            recv_sem=full_recv.at[side, p],
            device_id=peer[side],
            device_id_type=MESH,
        )

    for side in (0, 1):

        @pl.when(has[side])
        def _():
            for p in range(2 * AHEAD):
                full_copy(side, p).start()

    for copy in small[1:]:
        copy.wait()

    sub = lax.broadcasted_iota(jnp.int32, (LANES, LANES), 0)
    lane = lax.broadcasted_iota(jnp.int32, (LANES, LANES), 1)
    one = jnp.float32(1.0)
    zero = jnp.float32(0.0)

    def build(j, carry):
        at = pl.ds(pl.multiple_of(j * LANES, LANES), LANES)
        low = jnp.broadcast_to(cells[0:1, at], (LANES, LANES))
        upp = jnp.broadcast_to(cells[1:2, at], (LANES, LANES))
        for c in range(own // LANES):
            own_hot[c * LANES : (c + 1) * LANES, at] = jnp.where(
                low == sub + c * LANES, one, zero
            ).astype(HOT)
        for c in range(up_hot.shape[0] // LANES):
            up_hot[c * LANES : (c + 1) * LANES, at] = jnp.where(
                upp == sub + c * LANES, one, zero
            ).astype(HOT)
        low_t = low.T
        upp_t = upp.T
        for c in range(own // LANES):
            here = lane + c * LANES
            back_hot[at, c * LANES : (c + 1) * LANES] = (
                jnp.where(low_t == here, one, zero) - jnp.where(upp_t == here, one, zero)
            ).astype(HOT)
        return carry

    lax.fori_loop(0, fblk, build, 0)

    blocks = lax.broadcasted_iota(jnp.int32, (fblk, LANES), 0)
    slot_weight = jnp.where(blocks < live_s[0], weight[...], zero)
    along = jnp.cos(angle[...]) * slot_weight
    across = jnp.sin(angle[...]) * slot_weight
    sign = (1 - 2 * spec).astype(F32)
    along = along * sign
    across = across * sign
    for p in range(dloc):
        theta = (direction(p) + 0.5) * (2.0 * math.pi / NDIR)
        vel[p] = along * math.cos(theta) + across * math.sin(theta)

    freq = lax.broadcasted_iota(jnp.int32, (nfreq, LANES), 0)
    group = jnp.zeros((nfreq, LANES), F32)
    for f in range(nfreq):
        group = jnp.where(freq == f, speed_s[f], group)
    for c in range(own // LANES):
        lev = level[0:1, c * LANES : (c + 1) * LANES]
        area = jnp.exp2(-lev.astype(F32))
        scale[:, c * LANES : (c + 1) * LANES] = group * area
    bend = mask[...].astype(F32) * rate[...]
    turn[0:1, :] = jnp.maximum(bend, 0.0)
    turn[1:2, :] = jnp.minimum(bend, 0.0)

    for side in (0, 1):

        @pl.when(jnp.logical_not(has[side]))
        def _():
            def clear(i, carry):
                def inner(j, c):
                    got[i, side, j] = jnp.zeros(got.shape[3:], F32)
                    return c

                return lax.fori_loop(0, pairs, inner, carry)

            lax.fori_loop(0, ITERS, clear, 0)

    for side in (0, 1):

        @pl.when(has[side])
        def _():
            pltpu.make_async_remote_copy(
                src_ref=table_v,
                dst_ref=table_r.at[side],
                send_sem=table_send.at[side],
                recv_sem=table_recv.at[side],
                device_id=peer[side],
                device_id_type=MESH,
            ).wait_recv()

    for side in (0, 1):
        taken = table_r[side, 0]
        for k in range(hb):
            picks[side * hb + k] = jnp.broadcast_to(
                taken[1 - side : 2 - side, k : k + 1], (8, LANES)
            )

    mine = table_v[0]
    for side in (0, 1):
        for k in range(hb):
            picks[(2 + side) * hb + k] = jnp.broadcast_to(
                mine[side : side + 1, k : k + 1], (8, LANES)
            )

    def pick(value, which):
        wanted = jnp.broadcast_to(picks[which, 0:1, :], (nfreq, LANES))
        chosen = value[:, 0:LANES]
        for c in range(1, own // LANES):
            chosen = jnp.where(wanted == c, value[:, c * LANES : (c + 1) * LANES], chosen)
        return chosen

    def halo_copy(step, side, pair):
        return pltpu.make_async_remote_copy(
            src_ref=sent.at[step, side, pair],
            dst_ref=got.at[step, 1 - side, pair],
            send_sem=send_sem.at[step, side, pair],
            recv_sem=recv_sem.at[step, 1 - side, pair],
            device_id=peer[side],
            device_id_type=MESH,
        )

    def via_copy(step, side, pair):
        return pltpu.make_async_remote_copy(
            src_ref=sent.at[step, side, pair],
            dst_ref=passing.at[step, pair],
            send_sem=send_sem.at[step, side, pair],
            recv_sem=pass_recv.at[step, pair],
            device_id=relay[side],
            device_id_type=MESH,
        )

    def pass_copy(step, side, pair):
        return pltpu.make_async_remote_copy(
            src_ref=passing.at[step, pair],
            dst_ref=got.at[step, 1 - side, pair],
            send_sem=pass_send.at[step, pair],
            recv_sem=recv_sem.at[step, 1 - side, pair],
            device_id=other(-DOWN - 1) if side == 0 else other(PLANE - UP),
            device_id_type=MESH,
        )

    def pass_on(step, first):
        for side, role in ((0, passes_down), (1, passes_up)):

            @pl.when(role)
            def _():
                def one(pair, carry):
                    pltpu.make_async_remote_copy(
                        src_ref=passing.at[step, pair],
                        dst_ref=passing.at[step, pair],
                        send_sem=pass_send.at[step, pair],
                        recv_sem=pass_recv.at[step, pair],
                        device_id=other(1),
                        device_id_type=MESH,
                    ).wait_recv()
                    pass_copy(step, side, pair).start()
                    return carry

                lax.fori_loop(first, pairs, one, 0)

    def halo_arrival(step, side, pair):
        return pltpu.make_async_remote_copy(
            src_ref=sent.at[step, side, pair],
            dst_ref=got.at[step, side, pair],
            send_sem=send_sem.at[step, side, pair],
            recv_sem=recv_sem.at[step, side, pair],
            device_id=peer[side],
            device_id_type=MESH,
        )

    def send_pair(step, pair):
        for side in (0, 1):
            for e in (0, 1):
                value = cur[2 * pair + e]
                for k in range(hb):
                    sent[step, side, pair, e, k] = pick(value, side * hb + k)

            @pl.when(has[side] & jnp.logical_not(via[side]))
            def _():
                halo_copy(step, side, pair).start()

            @pl.when(via[side])
            def _():
                via_copy(step, side, pair).start()

    home = {}
    for begin, count in CHUNKS:
        for p in range(2 * begin, 2 * (begin + count)):
            home[p] = (4 * begin * ROWS + (p - 2 * begin) * ROWS, 2 * count * ROWS)

    def put(p, at, value):
        first, span = home[p]
        high, low = split(value)
        ext[first : first + nfreq, at] = high
        ext[first + span : first + span + nfreq, at] = low

    def split_own(p):
        put(p, slice(0, own), cur[p])

    for copy in loads:
        copy.wait()
    for pair in range(AHEAD, pairs):
        send_pair(0, pair)
    for p in range(dloc):
        split_own(p)
    pass_on(0, AHEAD)
    for side in (0, 1):

        @pl.when(has[side])
        def _():
            for p in range(2 * AHEAD):
                full_arrival(side, p).wait_recv()
                value = full[side, p]
                for k in range(hb):
                    got[0, side, p // 2, p % 2, k] = pick(value, (2 + side) * hb + k)

    def turn_slot(step, p):
        d = direction(p)
        here = moved[p]
        before = moved[slot(d - 1)] if d > 0 else edge_got[step, 1]
        after = moved[slot(d + 1)] if d < dloc - 1 else edge_got[step, 0]
        cur[p] = here - turn[0:1, :] * (here - before) - turn[1:2, :] * (after - here)
        split_own(p)

    def edge_copy(step):
        return pltpu.make_async_remote_copy(
            src_ref=edge_sent.at[step],
            dst_ref=edge_got.at[step],
            send_sem=edge_send.at[step],
            recv_sem=edge_recv.at[step],
            device_id=partner,
            device_id_type=MESH,
        )

    def finish_pair(step, pair):
        turn_slot(step, 2 * pair)
        turn_slot(step, 2 * pair + 1)

        @pl.when(step < ITERS - 1)
        def _():
            send_pair(step + 1, pair)

        @pl.when(step == ITERS - 1)
        def _():
            for p in (2 * pair, 2 * pair + 1):
                out[direction(p)] = cur[p]

    def compute(step, chunk):
        begin, count = CHUNKS[chunk]
        span = 2 * count * ROWS
        rows = slice(4 * begin * ROWS, 4 * begin * ROWS + 2 * span)
        for pair in range(begin, begin + count):
            for side in (0, 1):
                awaited = has[side] if pair >= AHEAD else has[side] & (step > 0)

                @pl.when(awaited)
                def _():
                    halo_arrival(step, side, pair).wait_recv()

            for side in (0, 1):
                for e in (0, 1):
                    for k in range(hb):
                        first = own + (side * hb + k) * LANES
                        put(2 * pair + e, slice(first, first + LANES), got[step, side, pair, e, k])
        width = 2 * LANES
        for n in range(faces // width):
            at = slice(n * width, (n + 1) * width)
            low = jnp.dot(ext[rows, 0:own], own_hot[:, at], preferred_element_type=F32)
            upp = jnp.dot(ext[rows, :], up_hot[:, at], preferred_element_type=F32)
            low = low[0:span] + low[span : 2 * span]
            upp = upp[0:span] + upp[span : 2 * span]
            for i in range(2 * count):
                p = 2 * begin + i
                there = slice(i * ROWS, (i + 1) * ROWS)
                for h in range(2):
                    inner = slice(h * LANES, (h + 1) * LANES)
                    u = jnp.broadcast_to(
                        vel[p, 2 * n + h : 2 * n + h + 1, :], (ROWS, LANES)
                    )
                    flow = u * jnp.where(u > 0.0, low[there, inner], upp[there, inner])
                    high, rest = split(flow)
                    outer = slice(n * width + h * LANES, n * width + (h + 1) * LANES)
                    flux[there, outer] = high
                    flux[slice(span + i * ROWS, span + (i + 1) * ROWS), outer] = rest
        total = jnp.dot(flux[0 : 2 * span, :], back_hot[...], preferred_element_type=F32)
        total = total[0:span] + total[span : 2 * span]
        for i in range(2 * count):
            p = 2 * begin + i
            moved[p] = cur[p] - scale[...] * total[i * ROWS : i * ROWS + nfreq]

    def one_step(step, carry):
        @pl.when(step > 0)
        def _():
            pass_on(step, 0)

        done = 1
        for chunk, (begin, count) in enumerate(CHUNKS):
            compute(step, chunk)
            if chunk == 0:
                edge_sent[step] = moved[0:2]
                edge_copy(step).start()
            if chunk == EDGE_AT:
                edge_copy(step).wait_recv()
                finish_pair(step, 0)
            last = begin + count == pairs
            ready = pairs if last else begin + count - 1
            for pair in range(done, ready):
                finish_pair(step, pair)
            done = max(done, ready)
        return carry

    lax.fori_loop(0, ITERS, one_step, 0)

    for step in range(ITERS):
        edge_copy(step).wait_send()
    for side, role in ((0, passes_down), (1, passes_up)):

        @pl.when(role)
        def _():
            for step in range(ITERS):
                for pair in range(AHEAD if step == 0 else 0, pairs):
                    pass_copy(step, side, pair).wait_send()

    for side in (0, 1):

        @pl.when(has[side])
        def _():
            tables[side].wait_send()
            for p in range(2 * AHEAD):
                full_copy(side, p).wait_send()
            for step in range(ITERS):
                for pair in range(AHEAD if step == 0 else 0, pairs):
                    halo_copy(step, side, pair).wait_send()


def on_device(
    field,
    group_speed,
    face_angle,
    face_speed,
    face_cells,
    face_live,
    halo_blocks,
    cell_level,
    polar_mask,
    turn_rate,
):
    dloc, nfreq, own = field.shape
    faces = face_angle.shape[0]
    fblk = faces // LANES
    hb = halo_blocks.shape[2]
    ext = own + 2 * hb * LANES
    pairs = dloc // 2
    any_spec = pl.BlockSpec(memory_space=pl.ANY)
    smem_spec = pl.BlockSpec(memory_space=pltpu.SMEM)
    halo = (ITERS, 2, pairs, 2, hb, nfreq, LANES)
    span = 2 * max(count for _, count in CHUNKS) * ROWS
    return pl.pallas_call(
        kernel,
        out_shape=pltpu.VMEM(field.shape, field.dtype),
        in_specs=[
            any_spec,
            smem_spec,
            any_spec,
            any_spec,
            any_spec,
            smem_spec,
            any_spec,
            any_spec,
            any_spec,
            any_spec,
        ],
        out_specs=pl.BlockSpec(memory_space=pltpu.VMEM),
        scratch_shapes=[
            pltpu.VMEM((dloc, nfreq, own), F32),
            pltpu.VMEM((dloc, nfreq, own), F32),
            pltpu.VMEM(halo, F32),
            pltpu.VMEM(halo, F32),
            pltpu.VMEM((ITERS, 2, nfreq, own), F32),
            pltpu.VMEM((ITERS, 2, nfreq, own), F32),
            pltpu.VMEM((2 * dloc * ROWS, ext), BF16),
            pltpu.VMEM((2 * span, faces), BF16),
            pltpu.VMEM((own, faces), HOT),
            pltpu.VMEM((ext, faces), HOT),
            pltpu.VMEM((faces, own), HOT),
            pltpu.VMEM((dloc, fblk, LANES), F32),
            pltpu.VMEM((nfreq, own), F32),
            pltpu.VMEM((2, own), F32),
            pltpu.VMEM((fblk, LANES), F32),
            pltpu.VMEM((fblk, LANES), F32),
            pltpu.VMEM((2, faces), jnp.int32),
            pltpu.VMEM((1, own), jnp.int32),
            pltpu.VMEM((1, own), jnp.int32),
            pltpu.VMEM((1, own), F32),
            pltpu.VMEM((1, 2, hb), jnp.int32),
            pltpu.VMEM((2, 1, 2, hb), jnp.int32),
            pltpu.VMEM((4 * hb, 8, LANES), jnp.int32),
            pltpu.VMEM((2, 2 * AHEAD, nfreq, own), F32),
            pltpu.VMEM((ITERS, pairs, 2, hb, nfreq, LANES), F32),
            pltpu.SemaphoreType.DMA((dloc,)),
            pltpu.SemaphoreType.DMA((7,)),
            pltpu.SemaphoreType.DMA((2,)),
            pltpu.SemaphoreType.DMA((2,)),
            pltpu.SemaphoreType.DMA((2, 2 * AHEAD)),
            pltpu.SemaphoreType.DMA((2, 2 * AHEAD)),
            pltpu.SemaphoreType.DMA((ITERS, pairs)),
            pltpu.SemaphoreType.DMA((ITERS, pairs)),
            pltpu.SemaphoreType.DMA((ITERS, 2, pairs)),
            pltpu.SemaphoreType.DMA((ITERS, 2, pairs)),
            pltpu.SemaphoreType.DMA((ITERS,)),
            pltpu.SemaphoreType.DMA((ITERS,)),
        ],
        compiler_params=pltpu.CompilerParams(
            collective_id=0, has_side_effects=True, vmem_limit_bytes=60 * 1024 * 1024
        ),
    )(
        field,
        group_speed,
        face_angle.reshape(fblk, LANES),
        face_speed.reshape(fblk, LANES),
        face_cells,
        face_live,
        halo_blocks,
        cell_level.reshape(1, own),
        polar_mask.reshape(1, own),
        turn_rate.reshape(1, own),
    )


def solution(mesh):
    return jax.shard_map(
        on_device,
        mesh=mesh,
        in_specs=(
            P("spec", None, "rows"),
            P(),
            P("rows"),
            P("rows"),
            P(None, "rows"),
            P("rows"),
            P("rows", None, None),
            P("rows"),
            P("rows"),
            P("rows"),
        ),
        out_specs=P("spec", None, "rows"),
        check_vma=False,
    )
```

```python
import functools
import math

import jax
import jax.numpy as jnp
from jax import lax
from jax.experimental import pallas as pl
from jax.experimental.pallas import tpu as pltpu
from jax.sharding import PartitionSpec as P

MESH = pl.DeviceIdType.MESH
NDIR = 36
ITERS = 3
LANES = 128
ROWS = 32
CHUNKS = ((0, 2), (2, 2), (4, 2), (6, 2), (8, 1))
GROUPS = ((0, 1), (2, 3, 4))
AHEAD = 2
EDGE_AT = 2
PLANE = 32
UP, DOWN = 7, 25
HOT = jnp.float8_e4m3fn
BF16 = jnp.bfloat16
F32 = jnp.float32


def split(value):
    high = value.astype(BF16)
    return high, (value - high.astype(F32)).astype(BF16)


def kernel(
    field,
    speed_s,
    angle_h,
    weight_h,
    cells_h,
    live_s,
    table_h,
    level_h,
    mask_h,
    rate_h,
    out,
    cur,
    moved,
    sent,
    got,
    edge_sent,
    edge_got,
    ext,
    flux,
    pre_low,
    pre_upp,
    own_hot,
    up_hot,
    back_hot,
    vel,
    scale,
    turn,
    angle,
    weight,
    cells,
    level,
    mask,
    rate,
    table_v,
    table_r,
    picks,
    full,
    passing,
    load_sem,
    small_sem,
    table_send,
    table_recv,
    full_send,
    full_recv,
    pass_send,
    pass_recv,
    send_sem,
    recv_sem,
    edge_send,
    edge_recv,
):
    dloc, nfreq, own = field.shape
    pairs = dloc // 2
    hb = table_h.shape[2]
    faces = cells.shape[1]
    fblk = faces // LANES
    size = lax.axis_size("rows")
    row = lax.axis_index("rows")
    spec = lax.axis_index("spec")
    has = (row > 0, row < size - 1)
    peer = ({"rows": jnp.maximum(row - 1, 0)}, {"rows": jnp.minimum(row + 1, size - 1)})
    partner = {"spec": 1 - spec}

    at = lax.rem(row, PLANE)
    odd = spec == 1

    def other(shift):
        return {"rows": jnp.clip(row + shift, 0, size - 1)}

    via = (odd & (at == 0) & (row > 0), odd & (at == PLANE - 1) & (row < size - 1))
    passes_up = odd & (at == UP) & (row < size - PLANE)
    passes_down = odd & (at == DOWN) & (row >= PLANE)
    relay = (other(DOWN), other(UP + 1 - PLANE))
    roles = (
        (via[0], relay[0], other(UP - PLANE)),
        (via[1], relay[1], other(DOWN + 1)),
        (passes_up, other(PLANE - 1 - UP), other(PLANE - UP)),
        (passes_down, other(-DOWN), other(-DOWN - 1)),
    )

    def slot(d):
        return 2 * d if d < pairs else 2 * (dloc - 1 - d) + 1

    def direction(p):
        return p // 2 if p % 2 == 0 else dloc - 1 - p // 2

    small = [
        pltpu.make_async_copy(src, dst, small_sem.at[i])
        for i, (src, dst) in enumerate(
            (
                (table_h, table_v),
                (cells_h, cells),
                (angle_h, angle),
                (weight_h, weight),
                (level_h, level),
                (mask_h, mask),
                (rate_h, rate),
            )
        )
    ]
    for copy in small:
        copy.start()
    loads = [
        pltpu.make_async_copy(
            field.at[direction(p)], cur.at[p], load_sem.at[p]
        )
        for p in range(dloc)
    ]
    for copy in loads:
        copy.start()
    table_r[...] = jnp.zeros_like(table_r)

    barrier = pltpu.get_barrier_semaphore()
    pl.semaphore_signal(barrier, inc=1, device_id=partner, device_id_type=MESH)
    for side in (0, 1):

        @pl.when(has[side])
        def _():
            pl.semaphore_signal(barrier, inc=1, device_id=peer[side], device_id_type=MESH)

    peers = 1 + has[0].astype(jnp.int32) + has[1].astype(jnp.int32)
    for role, first, second in roles:

        @pl.when(role)
        def _():
            pl.semaphore_signal(barrier, inc=1, device_id=first, device_id_type=MESH)
            pl.semaphore_signal(barrier, inc=1, device_id=second, device_id_type=MESH)

        peers = peers + 2 * role.astype(jnp.int32)
    pl.semaphore_wait(barrier, peers)

    small[0].wait()
    tables = [
        pltpu.make_async_remote_copy(
            src_ref=table_v,
            dst_ref=table_r.at[1 - side],
            send_sem=table_send.at[side],
            recv_sem=table_recv.at[1 - side],
            device_id=peer[side],
            device_id_type=MESH,
        )
        for side in (0, 1)
    ]
    for side in (0, 1):

        @pl.when(has[side])
        def _():
            tables[side].start()

    for copy in loads[0 : 2 * AHEAD]:
        copy.wait()

    def full_copy(side, p):
        return pltpu.make_async_remote_copy(
            src_ref=cur.at[p],
            dst_ref=full.at[1 - side, p],
            send_sem=full_send.at[side, p],
            recv_sem=full_recv.at[1 - side, p],
            device_id=peer[side],
            device_id_type=MESH,
        )

    def full_arrival(side, p):
        return pltpu.make_async_remote_copy(
            src_ref=cur.at[p],
            dst_ref=full.at[side, p],
            send_sem=full_send.at[side, p],
            recv_sem=full_recv.at[side, p],
            device_id=peer[side],
            device_id_type=MESH,
        )

    for side in (0, 1):

        @pl.when(has[side])
        def _():
            for p in range(2 * AHEAD):
                full_copy(side, p).start()

    for copy in small[1:]:
        copy.wait()

    sub = lax.broadcasted_iota(jnp.int32, (LANES, LANES), 0)
    lane = lax.broadcasted_iota(jnp.int32, (LANES, LANES), 1)
    one = jnp.float32(1.0)
    zero = jnp.float32(0.0)

    def build(j, carry):
        at = pl.ds(pl.multiple_of(j * LANES, LANES), LANES)
        low = jnp.broadcast_to(cells[0:1, at], (LANES, LANES))
        upp = jnp.broadcast_to(cells[1:2, at], (LANES, LANES))
        for c in range(own // LANES):
            own_hot[c * LANES : (c + 1) * LANES, at] = jnp.where(
                low == sub + c * LANES, one, zero
            ).astype(HOT)
        for c in range(up_hot.shape[0] // LANES):
            up_hot[c * LANES : (c + 1) * LANES, at] = jnp.where(
                upp == sub + c * LANES, one, zero
            ).astype(HOT)
        low_t = low.T
        upp_t = upp.T
        for c in range(own // LANES):
            here = lane + c * LANES
            back_hot[at, c * LANES : (c + 1) * LANES] = (
                jnp.where(low_t == here, one, zero) - jnp.where(upp_t == here, one, zero)
            ).astype(HOT)
        return carry

    lax.fori_loop(0, fblk, build, 0)

    blocks = lax.broadcasted_iota(jnp.int32, (fblk, LANES), 0)
    slot_weight = jnp.where(blocks < live_s[0], weight[...], zero)
    along = jnp.cos(angle[...]) * slot_weight
    across = jnp.sin(angle[...]) * slot_weight
    sign = (1 - 2 * spec).astype(F32)
    along = along * sign
    across = across * sign
    for p in range(dloc):
        theta = (direction(p) + 0.5) * (2.0 * math.pi / NDIR)
        vel[p] = along * math.cos(theta) + across * math.sin(theta)

    freq = lax.broadcasted_iota(jnp.int32, (nfreq, LANES), 0)
    group = jnp.zeros((nfreq, LANES), F32)
    for f in range(nfreq):
        group = jnp.where(freq == f, speed_s[f], group)
    for c in range(own // LANES):
        lev = level[0:1, c * LANES : (c + 1) * LANES]
        area = jnp.exp2(-lev.astype(F32))
        scale[:, c * LANES : (c + 1) * LANES] = group * area
    bend = mask[...].astype(F32) * rate[...]
    turn[0:1, :] = jnp.maximum(bend, 0.0)
    turn[1:2, :] = jnp.minimum(bend, 0.0)

    for side in (0, 1):

        @pl.when(jnp.logical_not(has[side]))
        def _():
            def clear(i, carry):
                def inner(j, c):
                    got[i, side, j] = jnp.zeros(got.shape[3:], F32)
                    return c

                return lax.fori_loop(0, pairs, inner, carry)

            lax.fori_loop(0, ITERS, clear, 0)

    for side in (0, 1):

        @pl.when(has[side])
        def _():
            pltpu.make_async_remote_copy(
                src_ref=table_v,
                dst_ref=table_r.at[side],
                send_sem=table_send.at[side],
                recv_sem=table_recv.at[side],
                device_id=peer[side],
                device_id_type=MESH,
            ).wait_recv()

    for side in (0, 1):
        taken = table_r[side, 0]
        for k in range(hb):
            picks[side * hb + k] = jnp.broadcast_to(
                taken[1 - side : 2 - side, k : k + 1], (8, LANES)
            )

    mine = table_v[0]
    for side in (0, 1):
        for k in range(hb):
            picks[(2 + side) * hb + k] = jnp.broadcast_to(
                mine[side : side + 1, k : k + 1], (8, LANES)
            )

    def pick(value, which):
        wanted = jnp.broadcast_to(picks[which, 0:1, :], (nfreq, LANES))
        chosen = value[:, 0:LANES]
        for c in range(1, own // LANES):
            chosen = jnp.where(wanted == c, value[:, c * LANES : (c + 1) * LANES], chosen)
        return chosen

    def halo_copy(step, side, pair):
        return pltpu.make_async_remote_copy(
            src_ref=sent.at[step, side, pair],
            dst_ref=got.at[step, 1 - side, pair],
            send_sem=send_sem.at[step, side, pair],
            recv_sem=recv_sem.at[step, 1 - side, pair],
            device_id=peer[side],
            device_id_type=MESH,
        )

    def via_copy(step, side, pair):
        return pltpu.make_async_remote_copy(
            src_ref=sent.at[step, side, pair],
            dst_ref=passing.at[step, pair],
            send_sem=send_sem.at[step, side, pair],
            recv_sem=pass_recv.at[step, pair],
            device_id=relay[side],
            device_id_type=MESH,
        )

    def pass_copy(step, side, pair):
        return pltpu.make_async_remote_copy(
            src_ref=passing.at[step, pair],
            dst_ref=got.at[step, 1 - side, pair],
            send_sem=pass_send.at[step, pair],
            recv_sem=recv_sem.at[step, 1 - side, pair],
            device_id=other(-DOWN - 1) if side == 0 else other(PLANE - UP),
            device_id_type=MESH,
        )

    def pass_on(step, first):
        for side, role in ((0, passes_down), (1, passes_up)):

            @pl.when(role)
            def _():
                def one(pair, carry):
                    pltpu.make_async_remote_copy(
                        src_ref=passing.at[step, pair],
                        dst_ref=passing.at[step, pair],
                        send_sem=pass_send.at[step, pair],
                        recv_sem=pass_recv.at[step, pair],
                        device_id=other(1),
                        device_id_type=MESH,
                    ).wait_recv()
                    pass_copy(step, side, pair).start()
                    return carry

                lax.fori_loop(first, pairs, one, 0)

    def halo_arrival(step, side, pair):
        return pltpu.make_async_remote_copy(
            src_ref=sent.at[step, side, pair],
            dst_ref=got.at[step, side, pair],
            send_sem=send_sem.at[step, side, pair],
            recv_sem=recv_sem.at[step, side, pair],
            device_id=peer[side],
            device_id_type=MESH,
        )

    def send_pair(step, pair):
        for side in (0, 1):
            for e in (0, 1):
                value = cur[2 * pair + e]
                for k in range(hb):
                    sent[step, side, pair, e, k] = pick(value, side * hb + k)

            @pl.when(has[side] & jnp.logical_not(via[side]))
            def _():
                halo_copy(step, side, pair).start()

            @pl.when(via[side])
            def _():
                via_copy(step, side, pair).start()

    home = {}
    for begin, count in CHUNKS:
        for p in range(2 * begin, 2 * (begin + count)):
            home[p] = (4 * begin * ROWS + (p - 2 * begin) * ROWS, 2 * count * ROWS)

    def put(p, at, value):
        first, span = home[p]
        high, low = split(value)
        ext[first : first + nfreq, at] = high
        ext[first + span : first + span + nfreq, at] = low

    def split_own(p):
        put(p, slice(0, own), cur[p])

    for copy in loads[2 * AHEAD :]:
        copy.wait()
    for pair in range(AHEAD, pairs):
        send_pair(0, pair)
    for p in range(dloc):
        split_own(p)
    def first_arrivals():
        pass_on(0, AHEAD)
        for side in (0, 1):

            @pl.when(has[side])
            def _():
                for p in range(2 * AHEAD):
                    full_arrival(side, p).wait_recv()
                    value = full[side, p]
                    for k in range(hb):
                        got[0, side, p // 2, p % 2, k] = pick(value, (2 + side) * hb + k)
        for side in (0, 1):

            @pl.when(has[side])
            def _():
                for p in range(2 * AHEAD):
                    full_copy(side, p).wait_send()

    def turn_slot(step, p):
        d = direction(p)
        here = moved[p]
        before = moved[slot(d - 1)] if d > 0 else edge_got[step, 1]
        after = moved[slot(d + 1)] if d < dloc - 1 else edge_got[step, 0]
        cur[p] = here - turn[0:1, :] * (here - before) - turn[1:2, :] * (after - here)
        split_own(p)

    def edge_copy(step):
        return pltpu.make_async_remote_copy(
            src_ref=edge_sent.at[step],
            dst_ref=edge_got.at[step],
            send_sem=edge_send.at[step],
            recv_sem=edge_recv.at[step],
            device_id=partner,
            device_id_type=MESH,
        )

    def finish_pair(step, pair):
        turn_slot(step, 2 * pair)
        turn_slot(step, 2 * pair + 1)

        @pl.when(step < ITERS - 1)
        def _():
            send_pair(step + 1, pair)

        @pl.when(step == ITERS - 1)
        def _():
            for p in (2 * pair, 2 * pair + 1):
                out[direction(p)] = cur[p]

    def prepare():
        width = 2 * LANES
        for group in GROUPS:
            start = 4 * CHUNKS[group[0]][0] * ROWS
            stop = 4 * sum(CHUNKS[group[-1]]) * ROWS
            for n in range(faces // width):
                at = slice(n * width, (n + 1) * width)
                for hot, kept in ((own_hot[:, at], pre_low), (up_hot[0:own, at], pre_upp)):
                    both = jnp.dot(ext[start:stop, 0:own], hot, preferred_element_type=F32)
                    for chunk in group:
                        begin, count = CHUNKS[chunk]
                        span = 2 * count * ROWS
                        here = 4 * begin * ROWS - start
                        kept[2 * begin * ROWS : 2 * begin * ROWS + span, at] = (
                            both[here : here + span] + both[here + span : here + 2 * span]
                        )

    def compute(step, chunk):
        begin, count = CHUNKS[chunk]
        span = 2 * count * ROWS
        rows = slice(4 * begin * ROWS, 4 * begin * ROWS + 2 * span)
        for pair in range(begin, begin + count):
            for side in (0, 1):
                awaited = has[side] if pair >= AHEAD else has[side] & (step > 0)

                @pl.when(awaited)
                def _():
                    halo_arrival(step, side, pair).wait_recv()

            for side in (0, 1):
                for e in (0, 1):
                    for k in range(hb):
                        first = own + (side * hb + k) * LANES
                        put(2 * pair + e, slice(first, first + LANES), got[step, side, pair, e, k])
        width = 2 * LANES
        for n in range(faces // width):
            at = slice(n * width, (n + 1) * width)
            upp = jnp.dot(ext[rows, own:], up_hot[own:, at], preferred_element_type=F32)
            kept = slice(2 * begin * ROWS, 2 * begin * ROWS + span)
            low = pre_low[kept, at]
            upp = upp[0:span] + upp[span : 2 * span] + pre_upp[kept, at]
            for i in range(2 * count):
                p = 2 * begin + i
                there = slice(i * ROWS, (i + 1) * ROWS)
                for h in range(2):
                    inner = slice(h * LANES, (h + 1) * LANES)
                    u = jnp.broadcast_to(
                        vel[p, 2 * n + h : 2 * n + h + 1, :], (ROWS, LANES)
                    )
                    flow = u * jnp.where(u > 0.0, low[there, inner], upp[there, inner])
                    high, rest = split(flow)
                    outer = slice(n * width + h * LANES, n * width + (h + 1) * LANES)
                    flux[there, outer] = high
                    flux[slice(span + i * ROWS, span + (i + 1) * ROWS), outer] = rest
        total = jnp.dot(flux[0 : 2 * span, :], back_hot[...], preferred_element_type=F32)
        total = total[0:span] + total[span : 2 * span]
        for i in range(2 * count):
            p = 2 * begin + i
            moved[p] = cur[p] - scale[...] * total[i * ROWS : i * ROWS + nfreq]

    def one_step(step, carry):
        prepare()

        @pl.when(step > 0)
        def _():
            pass_on(step, 0)

        @pl.when(step == 0)
        def _():
            first_arrivals()

        done = 1
        for chunk, (begin, count) in enumerate(CHUNKS):
            compute(step, chunk)
            if chunk == 0:
                edge_sent[step] = moved[0:2]
                edge_copy(step).start()
            if chunk == EDGE_AT:
                edge_copy(step).wait_recv()
                finish_pair(step, 0)
            last = begin + count == pairs
            ready = pairs if last else begin + count - 1
            for pair in range(done, ready):
                finish_pair(step, pair)
            done = max(done, ready)
        return carry

    lax.fori_loop(0, ITERS, one_step, 0)

    for step in range(ITERS):
        edge_copy(step).wait_send()
    for side, role in ((0, passes_down), (1, passes_up)):

        @pl.when(role)
        def _():
            for step in range(ITERS):
                for pair in range(AHEAD if step == 0 else 0, pairs):
                    pass_copy(step, side, pair).wait_send()

    for side in (0, 1):

        @pl.when(has[side])
        def _():
            tables[side].wait_send()
            for step in range(ITERS):
                for pair in range(AHEAD if step == 0 else 0, pairs):
                    halo_copy(step, side, pair).wait_send()


def on_device(
    field,
    group_speed,
    face_angle,
    face_speed,
    face_cells,
    face_live,
    halo_blocks,
    cell_level,
    polar_mask,
    turn_rate,
):
    dloc, nfreq, own = field.shape
    faces = face_angle.shape[0]
    fblk = faces // LANES
    hb = halo_blocks.shape[2]
    ext = own + 2 * hb * LANES
    pairs = dloc // 2
    any_spec = pl.BlockSpec(memory_space=pl.ANY)
    smem_spec = pl.BlockSpec(memory_space=pltpu.SMEM)
    halo = (ITERS, 2, pairs, 2, hb, nfreq, LANES)
    span = 2 * max(count for _, count in CHUNKS) * ROWS
    return pl.pallas_call(
        kernel,
        out_shape=pltpu.VMEM(field.shape, field.dtype),
        in_specs=[
            any_spec,
            smem_spec,
            any_spec,
            any_spec,
            any_spec,
            smem_spec,
            any_spec,
            any_spec,
            any_spec,
            any_spec,
        ],
        out_specs=pl.BlockSpec(memory_space=pltpu.VMEM),
        scratch_shapes=[
            pltpu.VMEM((dloc, nfreq, own), F32),
            pltpu.VMEM((dloc, nfreq, own), F32),
            pltpu.VMEM(halo, F32),
            pltpu.VMEM(halo, F32),
            pltpu.VMEM((ITERS, 2, nfreq, own), F32),
            pltpu.VMEM((ITERS, 2, nfreq, own), F32),
            pltpu.VMEM((2 * dloc * ROWS, ext), BF16),
            pltpu.VMEM((2 * span, faces), BF16),
            pltpu.VMEM((dloc * ROWS, faces), F32),
            pltpu.VMEM((dloc * ROWS, faces), F32),
            pltpu.VMEM((own, faces), HOT),
            pltpu.VMEM((ext, faces), HOT),
            pltpu.VMEM((faces, own), HOT),
            pltpu.VMEM((dloc, fblk, LANES), F32),
            pltpu.VMEM((nfreq, own), F32),
            pltpu.VMEM((2, own), F32),
            pltpu.VMEM((fblk, LANES), F32),
            pltpu.VMEM((fblk, LANES), F32),
            pltpu.VMEM((2, faces), jnp.int32),
            pltpu.VMEM((1, own), jnp.int32),
            pltpu.VMEM((1, own), jnp.int32),
            pltpu.VMEM((1, own), F32),
            pltpu.VMEM((1, 2, hb), jnp.int32),
            pltpu.VMEM((2, 1, 2, hb), jnp.int32),
            pltpu.VMEM((4 * hb, 8, LANES), jnp.int32),
            pltpu.VMEM((2, 2 * AHEAD, nfreq, own), F32),
            pltpu.VMEM((ITERS, pairs, 2, hb, nfreq, LANES), F32),
            pltpu.SemaphoreType.DMA((dloc,)),
            pltpu.SemaphoreType.DMA((7,)),
            pltpu.SemaphoreType.DMA((2,)),
            pltpu.SemaphoreType.DMA((2,)),
            pltpu.SemaphoreType.DMA((2, 2 * AHEAD)),
            pltpu.SemaphoreType.DMA((2, 2 * AHEAD)),
            pltpu.SemaphoreType.DMA((ITERS, pairs)),
            pltpu.SemaphoreType.DMA((ITERS, pairs)),
            pltpu.SemaphoreType.DMA((ITERS, 2, pairs)),
            pltpu.SemaphoreType.DMA((ITERS, 2, pairs)),
            pltpu.SemaphoreType.DMA((ITERS,)),
            pltpu.SemaphoreType.DMA((ITERS,)),
        ],
        compiler_params=pltpu.CompilerParams(
            collective_id=0, has_side_effects=True, vmem_limit_bytes=60 * 1024 * 1024
        ),
    )(
        field,
        group_speed,
        face_angle.reshape(fblk, LANES),
        face_speed.reshape(fblk, LANES),
        face_cells,
        face_live,
        halo_blocks,
        cell_level.reshape(1, own),
        polar_mask.reshape(1, own),
        turn_rate.reshape(1, own),
    )


def solution(mesh):
    return jax.shard_map(
        on_device,
        mesh=mesh,
        in_specs=(
            P("spec", None, "rows"),
            P(),
            P("rows"),
            P("rows"),
            P(None, "rows"),
            P("rows"),
            P("rows", None, None),
            P("rows"),
            P("rows"),
            P("rows"),
        ),
        out_specs=P("spec", None, "rows"),
        check_vma=False,
    )
```

```python
import functools
import math

import jax
import jax.numpy as jnp
from jax import lax
from jax.experimental import pallas as pl
from jax.experimental.pallas import tpu as pltpu
from jax.sharding import PartitionSpec as P

MESH = pl.DeviceIdType.MESH
NDIR = 36
ITERS = 3
LANES = 128
ROWS = 32
CHUNKS = ((0, 1), (1, 2), (3, 2), (5, 2), (7, 1), (8, 1))
AHEAD = 2
EDGE_AT = 2
PLANE = 32
UP, DOWN = 7, 25
HOT = jnp.float8_e4m3fn
BF16 = jnp.bfloat16
F32 = jnp.float32


def split(value):
    high = value.astype(BF16)
    return high, (value - high.astype(F32)).astype(BF16)


def kernel(
    field,
    speed_s,
    angle_h,
    weight_h,
    cells_h,
    live_s,
    table_h,
    level_h,
    mask_h,
    rate_h,
    out,
    cur,
    moved,
    sent,
    got,
    edge_sent,
    edge_got,
    ext,
    flux,
    own_hot,
    up_hot,
    back_hot,
    vel,
    scale,
    turn,
    angle,
    weight,
    cells,
    level,
    mask,
    rate,
    table_v,
    table_r,
    picks,
    full,
    passing,
    load_sem,
    small_sem,
    table_send,
    table_recv,
    full_send,
    full_recv,
    pass_send,
    pass_recv,
    send_sem,
    recv_sem,
    edge_send,
    edge_recv,
):
    dloc, nfreq, own = field.shape
    pairs = dloc // 2
    hb = table_h.shape[2]
    faces = cells.shape[1]
    fblk = faces // LANES
    size = lax.axis_size("rows")
    row = lax.axis_index("rows")
    spec = lax.axis_index("spec")
    has = (row > 0, row < size - 1)
    peer = ({"rows": jnp.maximum(row - 1, 0)}, {"rows": jnp.minimum(row + 1, size - 1)})
    partner = {"spec": 1 - spec}

    at = lax.rem(row, PLANE)
    odd = spec == 1

    def other(shift):
        return {"rows": jnp.clip(row + shift, 0, size - 1)}

    via = (odd & (at == 0) & (row > 0), odd & (at == PLANE - 1) & (row < size - 1))
    passes_up = odd & (at == UP) & (row < size - PLANE)
    passes_down = odd & (at == DOWN) & (row >= PLANE)
    relay = (other(DOWN), other(UP + 1 - PLANE))
    roles = (
        (via[0], relay[0], other(UP - PLANE)),
        (via[1], relay[1], other(DOWN + 1)),
        (passes_up, other(PLANE - 1 - UP), other(PLANE - UP)),
        (passes_down, other(-DOWN), other(-DOWN - 1)),
    )

    def slot(d):
        return 2 * d if d < pairs else 2 * (dloc - 1 - d) + 1

    def direction(p):
        return p // 2 if p % 2 == 0 else dloc - 1 - p // 2

    small = [
        pltpu.make_async_copy(src, dst, small_sem.at[i])
        for i, (src, dst) in enumerate(
            (
                (table_h, table_v),
                (cells_h, cells),
                (angle_h, angle),
                (weight_h, weight),
                (level_h, level),
                (mask_h, mask),
                (rate_h, rate),
            )
        )
    ]
    for copy in small:
        copy.start()
    loads = [
        pltpu.make_async_copy(
            field.at[direction(p)], cur.at[p], load_sem.at[p]
        )
        for p in range(dloc)
    ]
    for copy in loads:
        copy.start()
    table_r[...] = jnp.zeros_like(table_r)

    barrier = pltpu.get_barrier_semaphore()
    pl.semaphore_signal(barrier, inc=1, device_id=partner, device_id_type=MESH)
    for side in (0, 1):

        @pl.when(has[side])
        def _():
            pl.semaphore_signal(barrier, inc=1, device_id=peer[side], device_id_type=MESH)

    peers = 1 + has[0].astype(jnp.int32) + has[1].astype(jnp.int32)
    for role, first, second in roles:

        @pl.when(role)
        def _():
            pl.semaphore_signal(barrier, inc=1, device_id=first, device_id_type=MESH)
            pl.semaphore_signal(barrier, inc=1, device_id=second, device_id_type=MESH)

        peers = peers + 2 * role.astype(jnp.int32)
    pl.semaphore_wait(barrier, peers)

    small[0].wait()
    tables = [
        pltpu.make_async_remote_copy(
            src_ref=table_v,
            dst_ref=table_r.at[1 - side],
            send_sem=table_send.at[side],
            recv_sem=table_recv.at[1 - side],
            device_id=peer[side],
            device_id_type=MESH,
        )
        for side in (0, 1)
    ]
    for side in (0, 1):

        @pl.when(has[side])
        def _():
            tables[side].start()

    for copy in loads[0 : 2 * AHEAD]:
        copy.wait()

    def full_copy(side, p):
        return pltpu.make_async_remote_copy(
            src_ref=cur.at[p],
            dst_ref=full.at[1 - side, p],
            send_sem=full_send.at[side, p],
            recv_sem=full_recv.at[1 - side, p],
            device_id=peer[side],
            device_id_type=MESH,
        )

    def full_arrival(side, p):
        return pltpu.make_async_remote_copy(
            src_ref=cur.at[p],
            dst_ref=full.at[side, p],
            send_sem=full_send.at[side, p],
            recv_sem=full_recv.at[side, p],
            device_id=peer[side],
            device_id_type=MESH,
        )

    for side in (0, 1):

        @pl.when(has[side])
        def _():
            for p in range(2 * AHEAD):
                full_copy(side, p).start()

    for copy in small[1:]:
        copy.wait()

    sub = lax.broadcasted_iota(jnp.int32, (LANES, LANES), 0)
    lane = lax.broadcasted_iota(jnp.int32, (LANES, LANES), 1)
    one = jnp.float32(1.0)
    zero = jnp.float32(0.0)

    def build(j, carry):
        at = pl.ds(pl.multiple_of(j * LANES, LANES), LANES)
        low = jnp.broadcast_to(cells[0:1, at], (LANES, LANES))
        upp = jnp.broadcast_to(cells[1:2, at], (LANES, LANES))
        for c in range(own // LANES):
            own_hot[c * LANES : (c + 1) * LANES, at] = jnp.where(
                low == sub + c * LANES, one, zero
            ).astype(HOT)
        for c in range(up_hot.shape[0] // LANES):
            up_hot[c * LANES : (c + 1) * LANES, at] = jnp.where(
                upp == sub + c * LANES, one, zero
            ).astype(HOT)
        low_t = low.T
        upp_t = upp.T
        for c in range(own // LANES):
            here = lane + c * LANES
            back_hot[at, c * LANES : (c + 1) * LANES] = (
                jnp.where(low_t == here, one, zero) - jnp.where(upp_t == here, one, zero)
            ).astype(HOT)
        return carry

    lax.fori_loop(0, fblk, build, 0)

    blocks = lax.broadcasted_iota(jnp.int32, (fblk, LANES), 0)
    slot_weight = jnp.where(blocks < live_s[0], weight[...], zero)
    along = jnp.cos(angle[...]) * slot_weight
    across = jnp.sin(angle[...]) * slot_weight
    sign = (1 - 2 * spec).astype(F32)
    along = along * sign
    across = across * sign
    for p in range(dloc):
        theta = (direction(p) + 0.5) * (2.0 * math.pi / NDIR)
        vel[p] = along * math.cos(theta) + across * math.sin(theta)

    freq = lax.broadcasted_iota(jnp.int32, (nfreq, LANES), 0)
    group = jnp.zeros((nfreq, LANES), F32)
    for f in range(nfreq):
        group = jnp.where(freq == f, speed_s[f], group)
    for c in range(own // LANES):
        lev = level[0:1, c * LANES : (c + 1) * LANES]
        area = jnp.exp2(-lev.astype(F32))
        scale[:, c * LANES : (c + 1) * LANES] = group * area
    bend = mask[...].astype(F32) * rate[...]
    turn[0:1, :] = jnp.maximum(bend, 0.0)
    turn[1:2, :] = jnp.minimum(bend, 0.0)

    for side in (0, 1):

        @pl.when(jnp.logical_not(has[side]))
        def _():
            def clear(i, carry):
                def inner(j, c):
                    got[i, side, j] = jnp.zeros(got.shape[3:], F32)
                    return c

                return lax.fori_loop(0, pairs, inner, carry)

            lax.fori_loop(0, ITERS, clear, 0)

    for side in (0, 1):

        @pl.when(has[side])
        def _():
            pltpu.make_async_remote_copy(
                src_ref=table_v,
                dst_ref=table_r.at[side],
                send_sem=table_send.at[side],
                recv_sem=table_recv.at[side],
                device_id=peer[side],
                device_id_type=MESH,
            ).wait_recv()

    for side in (0, 1):
        taken = table_r[side, 0]
        for k in range(hb):
            picks[side * hb + k] = jnp.broadcast_to(
                taken[1 - side : 2 - side, k : k + 1], (8, LANES)
            )

    mine = table_v[0]
    for side in (0, 1):
        for k in range(hb):
            picks[(2 + side) * hb + k] = jnp.broadcast_to(
                mine[side : side + 1, k : k + 1], (8, LANES)
            )

    def pick(value, which):
        wanted = jnp.broadcast_to(picks[which, 0:1, :], (nfreq, LANES))
        chosen = value[:, 0:LANES]
        for c in range(1, own // LANES):
            chosen = jnp.where(wanted == c, value[:, c * LANES : (c + 1) * LANES], chosen)
        return chosen

    def halo_copy(step, side, pair):
        return pltpu.make_async_remote_copy(
            src_ref=sent.at[step, side, pair],
            dst_ref=got.at[step, 1 - side, pair],
            send_sem=send_sem.at[step, side, pair],
            recv_sem=recv_sem.at[step, 1 - side, pair],
            device_id=peer[side],
            device_id_type=MESH,
        )

    def via_copy(step, side, pair):
        return pltpu.make_async_remote_copy(
            src_ref=sent.at[step, side, pair],
            dst_ref=passing.at[step, pair],
            send_sem=send_sem.at[step, side, pair],
            recv_sem=pass_recv.at[step, pair],
            device_id=relay[side],
            device_id_type=MESH,
        )

    def pass_copy(step, side, pair):
        return pltpu.make_async_remote_copy(
            src_ref=passing.at[step, pair],
            dst_ref=got.at[step, 1 - side, pair],
            send_sem=pass_send.at[step, pair],
            recv_sem=recv_sem.at[step, 1 - side, pair],
            device_id=other(-DOWN - 1) if side == 0 else other(PLANE - UP),
            device_id_type=MESH,
        )

    def pass_on(step, first):
        for side, role in ((0, passes_down), (1, passes_up)):

            @pl.when(role)
            def _():
                def one(pair, carry):
                    pltpu.make_async_remote_copy(
                        src_ref=passing.at[step, pair],
                        dst_ref=passing.at[step, pair],
                        send_sem=pass_send.at[step, pair],
                        recv_sem=pass_recv.at[step, pair],
                        device_id=other(1),
                        device_id_type=MESH,
                    ).wait_recv()
                    pass_copy(step, side, pair).start()
                    return carry

                lax.fori_loop(first, pairs, one, 0)

    def halo_arrival(step, side, pair):
        return pltpu.make_async_remote_copy(
            src_ref=sent.at[step, side, pair],
            dst_ref=got.at[step, side, pair],
            send_sem=send_sem.at[step, side, pair],
            recv_sem=recv_sem.at[step, side, pair],
            device_id=peer[side],
            device_id_type=MESH,
        )

    def send_pair(step, pair):
        for side in (0, 1):
            for e in (0, 1):
                value = cur[2 * pair + e]
                for k in range(hb):
                    sent[step, side, pair, e, k] = pick(value, side * hb + k)

            @pl.when(has[side] & jnp.logical_not(via[side]))
            def _():
                halo_copy(step, side, pair).start()

            @pl.when(via[side])
            def _():
                via_copy(step, side, pair).start()

    home = {}
    for begin, count in CHUNKS:
        for p in range(2 * begin, 2 * (begin + count)):
            home[p] = (4 * begin * ROWS + (p - 2 * begin) * ROWS, 2 * count * ROWS)

    def put(p, at, value):
        first, span = home[p]
        high, low = split(value)
        ext[first : first + nfreq, at] = high
        ext[first + span : first + span + nfreq, at] = low

    def split_own(p):
        put(p, slice(0, own), cur[p])

    for copy in loads[2 * AHEAD :]:
        copy.wait()
    for pair in range(AHEAD, pairs):
        send_pair(0, pair)
    for p in range(dloc):
        split_own(p)
    pass_on(0, AHEAD)
    for side in (0, 1):

        @pl.when(has[side])
        def _():
            for p in range(2 * AHEAD):
                full_arrival(side, p).wait_recv()
                value = full[side, p]
                for k in range(hb):
                    got[0, side, p // 2, p % 2, k] = pick(value, (2 + side) * hb + k)
            for p in range(2 * AHEAD):
                full_copy(side, p).wait_send()

    def turn_slot(step, p):
        d = direction(p)
        here = moved[p]
        before = moved[slot(d - 1)] if d > 0 else edge_got[step, 1]
        after = moved[slot(d + 1)] if d < dloc - 1 else edge_got[step, 0]
        cur[p] = here - turn[0:1, :] * (here - before) - turn[1:2, :] * (after - here)
        split_own(p)

    def edge_copy(step):
        return pltpu.make_async_remote_copy(
            src_ref=edge_sent.at[step],
            dst_ref=edge_got.at[step],
            send_sem=edge_send.at[step],
            recv_sem=edge_recv.at[step],
            device_id=partner,
            device_id_type=MESH,
        )

    def finish_pair(step, pair):
        turn_slot(step, 2 * pair)
        turn_slot(step, 2 * pair + 1)

        @pl.when(step < ITERS - 1)
        def _():
            send_pair(step + 1, pair)

        @pl.when(step == ITERS - 1)
        def _():
            for p in (2 * pair, 2 * pair + 1):
                out[direction(p)] = cur[p]

    def compute(step, chunk):
        begin, count = CHUNKS[chunk]
        span = 2 * count * ROWS
        rows = slice(4 * begin * ROWS, 4 * begin * ROWS + 2 * span)
        for pair in range(begin, begin + count):
            for side in (0, 1):
                awaited = has[side] if pair >= AHEAD else has[side] & (step > 0)

                @pl.when(awaited)
                def _():
                    halo_arrival(step, side, pair).wait_recv()

            for side in (0, 1):
                for e in (0, 1):
                    for k in range(hb):
                        first = own + (side * hb + k) * LANES
                        put(2 * pair + e, slice(first, first + LANES), got[step, side, pair, e, k])
        width = 2 * LANES
        for n in range(faces // width):
            at = slice(n * width, (n + 1) * width)
            low = jnp.dot(ext[rows, 0:own], own_hot[:, at], preferred_element_type=F32)
            upp = jnp.dot(ext[rows, :], up_hot[:, at], preferred_element_type=F32)
            low = low[0:span] + low[span : 2 * span]
            upp = upp[0:span] + upp[span : 2 * span]
            for i in range(2 * count):
                p = 2 * begin + i
                there = slice(i * ROWS, (i + 1) * ROWS)
                for h in range(2):
                    inner = slice(h * LANES, (h + 1) * LANES)
                    u = jnp.broadcast_to(
                        vel[p, 2 * n + h : 2 * n + h + 1, :], (ROWS, LANES)
                    )
                    flow = u * jnp.where(u > 0.0, low[there, inner], upp[there, inner])
                    high, rest = split(flow)
                    outer = slice(n * width + h * LANES, n * width + (h + 1) * LANES)
                    flux[there, outer] = high
                    flux[slice(span + i * ROWS, span + (i + 1) * ROWS), outer] = rest
        total = jnp.dot(flux[0 : 2 * span, :], back_hot[...], preferred_element_type=F32)
        total = total[0:span] + total[span : 2 * span]
        for i in range(2 * count):
            p = 2 * begin + i
            moved[p] = cur[p] - scale[...] * total[i * ROWS : i * ROWS + nfreq]

    def one_step(step, carry):
        @pl.when(step > 0)
        def _():
            pass_on(step, 0)

        done = 1
        for chunk, (begin, count) in enumerate(CHUNKS):
            compute(step, chunk)
            if chunk == 0:
                edge_sent[step] = moved[0:2]
                edge_copy(step).start()
            if chunk == EDGE_AT:
                edge_copy(step).wait_recv()
                finish_pair(step, 0)
            last = begin + count == pairs
            ready = pairs if last else begin + count - 1
            for pair in range(done, ready):
                finish_pair(step, pair)
            done = max(done, ready)
        return carry

    lax.fori_loop(0, ITERS, one_step, 0)

    for step in range(ITERS):
        edge_copy(step).wait_send()
    for side, role in ((0, passes_down), (1, passes_up)):

        @pl.when(role)
        def _():
            for step in range(ITERS):
                for pair in range(AHEAD if step == 0 else 0, pairs):
                    pass_copy(step, side, pair).wait_send()

    for side in (0, 1):

        @pl.when(has[side])
        def _():
            tables[side].wait_send()
            for step in range(ITERS):
                for pair in range(AHEAD if step == 0 else 0, pairs):
                    halo_copy(step, side, pair).wait_send()


def on_device(
    field,
    group_speed,
    face_angle,
    face_speed,
    face_cells,
    face_live,
    halo_blocks,
    cell_level,
    polar_mask,
    turn_rate,
):
    dloc, nfreq, own = field.shape
    faces = face_angle.shape[0]
    fblk = faces // LANES
    hb = halo_blocks.shape[2]
    ext = own + 2 * hb * LANES
    pairs = dloc // 2
    any_spec = pl.BlockSpec(memory_space=pl.ANY)
    smem_spec = pl.BlockSpec(memory_space=pltpu.SMEM)
    halo = (ITERS, 2, pairs, 2, hb, nfreq, LANES)
    span = 2 * max(count for _, count in CHUNKS) * ROWS
    return pl.pallas_call(
        kernel,
        out_shape=pltpu.VMEM(field.shape, field.dtype),
        in_specs=[
            any_spec,
            smem_spec,
            any_spec,
            any_spec,
            any_spec,
            smem_spec,
            any_spec,
            any_spec,
            any_spec,
            any_spec,
        ],
        out_specs=pl.BlockSpec(memory_space=pltpu.VMEM),
        scratch_shapes=[
            pltpu.VMEM((dloc, nfreq, own), F32),
            pltpu.VMEM((dloc, nfreq, own), F32),
            pltpu.VMEM(halo, F32),
            pltpu.VMEM(halo, F32),
            pltpu.VMEM((ITERS, 2, nfreq, own), F32),
            pltpu.VMEM((ITERS, 2, nfreq, own), F32),
            pltpu.VMEM((2 * dloc * ROWS, ext), BF16),
            pltpu.VMEM((2 * span, faces), BF16),
            pltpu.VMEM((own, faces), HOT),
            pltpu.VMEM((ext, faces), HOT),
            pltpu.VMEM((faces, own), HOT),
            pltpu.VMEM((dloc, fblk, LANES), F32),
            pltpu.VMEM((nfreq, own), F32),
            pltpu.VMEM((2, own), F32),
            pltpu.VMEM((fblk, LANES), F32),
            pltpu.VMEM((fblk, LANES), F32),
            pltpu.VMEM((2, faces), jnp.int32),
            pltpu.VMEM((1, own), jnp.int32),
            pltpu.VMEM((1, own), jnp.int32),
            pltpu.VMEM((1, own), F32),
            pltpu.VMEM((1, 2, hb), jnp.int32),
            pltpu.VMEM((2, 1, 2, hb), jnp.int32),
            pltpu.VMEM((4 * hb, 8, LANES), jnp.int32),
            pltpu.VMEM((2, 2 * AHEAD, nfreq, own), F32),
            pltpu.VMEM((ITERS, pairs, 2, hb, nfreq, LANES), F32),
            pltpu.SemaphoreType.DMA((dloc,)),
            pltpu.SemaphoreType.DMA((7,)),
            pltpu.SemaphoreType.DMA((2,)),
            pltpu.SemaphoreType.DMA((2,)),
            pltpu.SemaphoreType.DMA((2, 2 * AHEAD)),
            pltpu.SemaphoreType.DMA((2, 2 * AHEAD)),
            pltpu.SemaphoreType.DMA((ITERS, pairs)),
            pltpu.SemaphoreType.DMA((ITERS, pairs)),
            pltpu.SemaphoreType.DMA((ITERS, 2, pairs)),
            pltpu.SemaphoreType.DMA((ITERS, 2, pairs)),
            pltpu.SemaphoreType.DMA((ITERS,)),
            pltpu.SemaphoreType.DMA((ITERS,)),
        ],
        compiler_params=pltpu.CompilerParams(
            collective_id=0, has_side_effects=True, vmem_limit_bytes=60 * 1024 * 1024
        ),
    )(
        field,
        group_speed,
        face_angle.reshape(fblk, LANES),
        face_speed.reshape(fblk, LANES),
        face_cells,
        face_live,
        halo_blocks,
        cell_level.reshape(1, own),
        polar_mask.reshape(1, own),
        turn_rate.reshape(1, own),
    )


def solution(mesh):
    return jax.shard_map(
        on_device,
        mesh=mesh,
        in_specs=(
            P("spec", None, "rows"),
            P(),
            P("rows"),
            P("rows"),
            P(None, "rows"),
            P("rows"),
            P("rows", None, None),
            P("rows"),
            P("rows"),
            P("rows"),
        ),
        out_specs=P("spec", None, "rows"),
        check_vma=False,
    )
```

```python
import functools
import math

import jax
import jax.numpy as jnp
from jax import lax
from jax.experimental import pallas as pl
from jax.experimental.pallas import tpu as pltpu
from jax.sharding import PartitionSpec as P

MESH = pl.DeviceIdType.MESH
NDIR = 36
ITERS = 3
LANES = 128
ROWS = 32
CHUNKS = ((0, 1), (1, 2), (3, 2), (5, 2), (7, 1), (8, 1))
LATE = 6
AHEAD = 4
EDGE_AT = 2
PLANE = 32
UP, DOWN = 7, 25
HOT = jnp.float8_e4m3fn
BF16 = jnp.bfloat16
F32 = jnp.float32


def split(value):
    high = value.astype(BF16)
    return high, (value - high.astype(F32)).astype(BF16)


def kernel(
    field,
    speed_s,
    angle_h,
    weight_h,
    cells_h,
    live_s,
    table_h,
    level_h,
    mask_h,
    rate_h,
    out,
    cur,
    moved,
    sent,
    got,
    edge_sent,
    edge_got,
    ext,
    flux,
    own_hot,
    up_hot,
    back_hot,
    vel,
    scale,
    turn,
    angle,
    weight,
    cells,
    level,
    mask,
    rate,
    table_v,
    table_r,
    picks,
    full,
    passing,
    pass_full,
    load_sem,
    small_sem,
    table_send,
    table_recv,
    full_send,
    full_recv,
    pass_full_send,
    pass_full_recv,
    pass_send,
    pass_recv,
    send_sem,
    recv_sem,
    edge_send,
    edge_recv,
):
    dloc, nfreq, own = field.shape
    pairs = dloc // 2
    hb = table_h.shape[2]
    faces = cells.shape[1]
    fblk = faces // LANES
    size = lax.axis_size("rows")
    row = lax.axis_index("rows")
    spec = lax.axis_index("spec")
    has = (row > 0, row < size - 1)
    peer = ({"rows": jnp.maximum(row - 1, 0)}, {"rows": jnp.minimum(row + 1, size - 1)})
    partner = {"spec": 1 - spec}

    at = lax.rem(row, PLANE)
    odd = spec == 1

    def other(shift):
        return {"rows": jnp.clip(row + shift, 0, size - 1)}

    via = (odd & (at == 0) & (row > 0), odd & (at == PLANE - 1) & (row < size - 1))
    passes_up = odd & (at == UP) & (row < size - PLANE)
    passes_down = odd & (at == DOWN) & (row >= PLANE)
    relay = (other(DOWN), other(UP + 1 - PLANE))
    roles = (
        (via[0], relay[0], other(UP - PLANE)),
        (via[1], relay[1], other(DOWN + 1)),
        (passes_up, other(PLANE - 1 - UP), other(PLANE - UP)),
        (passes_down, other(-DOWN), other(-DOWN - 1)),
    )

    def slot(d):
        return 2 * d if d < pairs else 2 * (dloc - 1 - d) + 1

    def direction(p):
        return p // 2 if p % 2 == 0 else dloc - 1 - p // 2

    small = [
        pltpu.make_async_copy(src, dst, small_sem.at[i])
        for i, (src, dst) in enumerate(
            (
                (table_h, table_v),
                (cells_h, cells),
                (angle_h, angle),
                (weight_h, weight),
                (level_h, level),
                (mask_h, mask),
                (rate_h, rate),
            )
        )
    ]
    for copy in small:
        copy.start()
    loads = [
        pltpu.make_async_copy(
            field.at[direction(p)], cur.at[p], load_sem.at[p]
        )
        for p in range(dloc)
    ]
    for copy in loads:
        copy.start()
    table_r[...] = jnp.zeros_like(table_r)

    barrier = pltpu.get_barrier_semaphore()
    pl.semaphore_signal(barrier, inc=1, device_id=partner, device_id_type=MESH)
    for side in (0, 1):

        @pl.when(has[side])
        def _():
            pl.semaphore_signal(barrier, inc=1, device_id=peer[side], device_id_type=MESH)

    peers = 1 + has[0].astype(jnp.int32) + has[1].astype(jnp.int32)
    for role, first, second in roles:

        @pl.when(role)
        def _():
            pl.semaphore_signal(barrier, inc=1, device_id=first, device_id_type=MESH)
            pl.semaphore_signal(barrier, inc=1, device_id=second, device_id_type=MESH)

        peers = peers + 2 * role.astype(jnp.int32)
    pl.semaphore_wait(barrier, peers)

    small[0].wait()
    tables = [
        pltpu.make_async_remote_copy(
            src_ref=table_v,
            dst_ref=table_r.at[1 - side],
            send_sem=table_send.at[side],
            recv_sem=table_recv.at[1 - side],
            device_id=peer[side],
            device_id_type=MESH,
        )
        for side in (0, 1)
    ]
    for side in (0, 1):

        @pl.when(has[side])
        def _():
            tables[side].start()

    for copy in loads[0 : 2 * AHEAD]:
        copy.wait()

    def full_copy(side, p):
        return pltpu.make_async_remote_copy(
            src_ref=cur.at[p],
            dst_ref=full.at[1 - side, p],
            send_sem=full_send.at[side, p],
            recv_sem=full_recv.at[1 - side, p],
            device_id=peer[side],
            device_id_type=MESH,
        )

    def full_arrival(side, p):
        return pltpu.make_async_remote_copy(
            src_ref=cur.at[p],
            dst_ref=full.at[side, p],
            send_sem=full_send.at[side, p],
            recv_sem=full_recv.at[side, p],
            device_id=peer[side],
            device_id_type=MESH,
        )

    def full_via(side, p):
        return pltpu.make_async_remote_copy(
            src_ref=cur.at[p],
            dst_ref=pass_full.at[p],
            send_sem=full_send.at[side, p],
            recv_sem=pass_full_recv.at[p],
            device_id=relay[side],
            device_id_type=MESH,
        )

    beyond = (other(-DOWN - 1), other(PLANE - UP))

    def full_pass(side, p):
        return pltpu.make_async_remote_copy(
            src_ref=pass_full.at[p],
            dst_ref=full.at[1 - side, p],
            send_sem=pass_full_send.at[p],
            recv_sem=full_recv.at[1 - side, p],
            device_id=beyond[side],
            device_id_type=MESH,
        )

    for side in (0, 1):

        @pl.when(has[side] & jnp.logical_not(via[side]))
        def _():
            for p in range(2 * AHEAD):
                full_copy(side, p).start()

        @pl.when(via[side])
        def _():
            for p in range(2 * AHEAD):
                full_via(side, p).start()

    for copy in small[1:]:
        copy.wait()

    sub = lax.broadcasted_iota(jnp.int32, (LANES, LANES), 0)
    lane = lax.broadcasted_iota(jnp.int32, (LANES, LANES), 1)
    one = jnp.float32(1.0)
    zero = jnp.float32(0.0)

    def build(j, carry):
        at = pl.ds(pl.multiple_of(j * LANES, LANES), LANES)
        low = jnp.broadcast_to(cells[0:1, at], (LANES, LANES))
        upp = jnp.broadcast_to(cells[1:2, at], (LANES, LANES))
        for c in range(own // LANES):
            own_hot[c * LANES : (c + 1) * LANES, at] = jnp.where(
                low == sub + c * LANES, one, zero
            ).astype(HOT)
        for c in range(up_hot.shape[0] // LANES):
            up_hot[c * LANES : (c + 1) * LANES, at] = jnp.where(
                upp == sub + c * LANES, one, zero
            ).astype(HOT)
        low_t = low.T
        upp_t = upp.T
        for c in range(own // LANES):
            here = lane + c * LANES
            back_hot[at, c * LANES : (c + 1) * LANES] = (
                jnp.where(low_t == here, one, zero) - jnp.where(upp_t == here, one, zero)
            ).astype(HOT)
        return carry

    lax.fori_loop(0, fblk, build, 0)

    blocks = lax.broadcasted_iota(jnp.int32, (fblk, LANES), 0)
    slot_weight = jnp.where(blocks < live_s[0], weight[...], zero)
    along = jnp.cos(angle[...]) * slot_weight
    across = jnp.sin(angle[...]) * slot_weight
    sign = (1 - 2 * spec).astype(F32)
    along = along * sign
    across = across * sign
    for p in range(dloc):
        theta = (direction(p) + 0.5) * (2.0 * math.pi / NDIR)
        vel[p] = along * math.cos(theta) + across * math.sin(theta)

    freq = lax.broadcasted_iota(jnp.int32, (nfreq, LANES), 0)
    group = jnp.zeros((nfreq, LANES), F32)
    for f in range(nfreq):
        group = jnp.where(freq == f, speed_s[f], group)
    for c in range(own // LANES):
        lev = level[0:1, c * LANES : (c + 1) * LANES]
        area = jnp.exp2(-lev.astype(F32))
        scale[:, c * LANES : (c + 1) * LANES] = group * area
    bend = mask[...].astype(F32) * rate[...]
    turn[0:1, :] = jnp.maximum(bend, 0.0)
    turn[1:2, :] = jnp.minimum(bend, 0.0)

    for side in (0, 1):

        @pl.when(jnp.logical_not(has[side]))
        def _():
            def clear(i, carry):
                def inner(j, c):
                    got[i, side, j] = jnp.zeros(got.shape[3:], F32)
                    return c

                return lax.fori_loop(0, pairs, inner, carry)

            lax.fori_loop(0, ITERS, clear, 0)

    for side in (0, 1):

        @pl.when(has[side])
        def _():
            pltpu.make_async_remote_copy(
                src_ref=table_v,
                dst_ref=table_r.at[side],
                send_sem=table_send.at[side],
                recv_sem=table_recv.at[side],
                device_id=peer[side],
                device_id_type=MESH,
            ).wait_recv()

    for side in (0, 1):
        taken = table_r[side, 0]
        for k in range(hb):
            picks[side * hb + k] = jnp.broadcast_to(
                taken[1 - side : 2 - side, k : k + 1], (8, LANES)
            )

    mine = table_v[0]
    for side in (0, 1):
        for k in range(hb):
            picks[(2 + side) * hb + k] = jnp.broadcast_to(
                mine[side : side + 1, k : k + 1], (8, LANES)
            )

    def pick(value, which):
        wanted = jnp.broadcast_to(picks[which, 0:1, :], (nfreq, LANES))
        chosen = value[:, 0:LANES]
        for c in range(1, own // LANES):
            chosen = jnp.where(wanted == c, value[:, c * LANES : (c + 1) * LANES], chosen)
        return chosen

    def halo_copy(step, side, pair):
        return pltpu.make_async_remote_copy(
            src_ref=sent.at[step, side, pair],
            dst_ref=got.at[step, 1 - side, pair],
            send_sem=send_sem.at[step, side, pair],
            recv_sem=recv_sem.at[step, 1 - side, pair],
            device_id=peer[side],
            device_id_type=MESH,
        )

    def via_copy(step, side, pair, e):
        return pltpu.make_async_remote_copy(
            src_ref=sent.at[step, side, pair, e],
            dst_ref=passing.at[step, pair, e],
            send_sem=send_sem.at[step, side, pair],
            recv_sem=pass_recv.at[step, pair, e],
            device_id=relay[side],
            device_id_type=MESH,
        )

    def pass_copy(step, side, pair, e):
        return pltpu.make_async_remote_copy(
            src_ref=passing.at[step, pair, e],
            dst_ref=got.at[step, 1 - side, pair, e],
            send_sem=pass_send.at[step, pair, e],
            recv_sem=recv_sem.at[step, 1 - side, pair],
            device_id=beyond[side],
            device_id_type=MESH,
        )

    def came(ref, send, recv):
        pltpu.make_async_remote_copy(
            src_ref=ref,
            dst_ref=ref,
            send_sem=send,
            recv_sem=recv,
            device_id=other(1),
            device_id_type=MESH,
        ).wait_recv()

    def pass_on(step, first, last):
        for side, role in ((0, passes_down), (1, passes_up)):

            @pl.when(role)
            def _():
                def one(pair, carry):
                    for e in (0, 1):
                        came(
                            passing.at[step, pair, e],
                            pass_send.at[step, pair, e],
                            pass_recv.at[step, pair, e],
                        )
                        pass_copy(step, side, pair, e).start()
                    return carry

                lax.fori_loop(first, last, one, 0)

    def pass_full_on():
        for side, role in ((0, passes_down), (1, passes_up)):

            @pl.when(role)
            def _():
                for p in range(2 * AHEAD):
                    came(pass_full.at[p], pass_full_send.at[p], pass_full_recv.at[p])
                    full_pass(side, p).start()

    def halo_arrival(step, side, pair):
        return pltpu.make_async_remote_copy(
            src_ref=sent.at[step, side, pair],
            dst_ref=got.at[step, side, pair],
            send_sem=send_sem.at[step, side, pair],
            recv_sem=recv_sem.at[step, side, pair],
            device_id=peer[side],
            device_id_type=MESH,
        )

    def send_pair(step, pair):
        for side in (0, 1):
            for e in (0, 1):
                value = cur[2 * pair + e]
                for k in range(hb):
                    sent[step, side, pair, e, k] = pick(value, side * hb + k)

            @pl.when(has[side] & jnp.logical_not(via[side]))
            def _():
                halo_copy(step, side, pair).start()

            @pl.when(via[side])
            def _():
                for e in (0, 1):
                    via_copy(step, side, pair, e).start()

    home = {}
    for begin, count in CHUNKS:
        for p in range(2 * begin, 2 * (begin + count)):
            home[p] = (4 * begin * ROWS + (p - 2 * begin) * ROWS, 2 * count * ROWS)

    def put(p, at, value):
        first, span = home[p]
        high, low = split(value)
        ext[first : first + nfreq, at] = high
        ext[first + span : first + span + nfreq, at] = low

    def split_own(p):
        put(p, slice(0, own), cur[p])

    for copy in loads[2 * AHEAD :]:
        copy.wait()
    for pair in range(AHEAD, pairs):
        send_pair(0, pair)
    for p in range(dloc):
        split_own(p)
    pass_full_on()
    pass_on(0, AHEAD, pairs)
    for side in (0, 1):

        @pl.when(has[side])
        def _():
            for p in range(2 * AHEAD):
                full_arrival(side, p).wait_recv()
                value = full[side, p]
                for k in range(hb):
                    got[0, side, p // 2, p % 2, k] = pick(value, (2 + side) * hb + k)
            for p in range(2 * AHEAD):
                full_copy(side, p).wait_send()

    def turn_slot(step, p):
        d = direction(p)
        here = moved[p]
        before = moved[slot(d - 1)] if d > 0 else edge_got[step, 1]
        after = moved[slot(d + 1)] if d < dloc - 1 else edge_got[step, 0]
        cur[p] = here - turn[0:1, :] * (here - before) - turn[1:2, :] * (after - here)
        split_own(p)

    def edge_copy(step):
        return pltpu.make_async_remote_copy(
            src_ref=edge_sent.at[step],
            dst_ref=edge_got.at[step],
            send_sem=edge_send.at[step],
            recv_sem=edge_recv.at[step],
            device_id=partner,
            device_id_type=MESH,
        )

    def finish_pair(step, pair):
        turn_slot(step, 2 * pair)
        turn_slot(step, 2 * pair + 1)

        @pl.when(step < ITERS - 1)
        def _():
            send_pair(step + 1, pair)

        @pl.when(step == ITERS - 1)
        def _():
            for p in (2 * pair, 2 * pair + 1):
                out[direction(p)] = cur[p]

    def compute(step, chunk):
        begin, count = CHUNKS[chunk]
        span = 2 * count * ROWS
        rows = slice(4 * begin * ROWS, 4 * begin * ROWS + 2 * span)
        for pair in range(begin, begin + count):
            for side in (0, 1):
                awaited = has[side] if pair >= AHEAD else has[side] & (step > 0)

                @pl.when(awaited)
                def _():
                    halo_arrival(step, side, pair).wait_recv()

            for side in (0, 1):
                for e in (0, 1):
                    for k in range(hb):
                        first = own + (side * hb + k) * LANES
                        put(2 * pair + e, slice(first, first + LANES), got[step, side, pair, e, k])
        width = 2 * LANES
        for n in range(faces // width):
            at = slice(n * width, (n + 1) * width)
            low = jnp.dot(ext[rows, 0:own], own_hot[:, at], preferred_element_type=F32)
            upp = jnp.dot(ext[rows, :], up_hot[:, at], preferred_element_type=F32)
            low = low[0:span] + low[span : 2 * span]
            upp = upp[0:span] + upp[span : 2 * span]
            for i in range(2 * count):
                p = 2 * begin + i
                there = slice(i * ROWS, (i + 1) * ROWS)
                for h in range(2):
                    inner = slice(h * LANES, (h + 1) * LANES)
                    u = jnp.broadcast_to(
                        vel[p, 2 * n + h : 2 * n + h + 1, :], (ROWS, LANES)
                    )
                    flow = u * jnp.where(u > 0.0, low[there, inner], upp[there, inner])
                    high, rest = split(flow)
                    outer = slice(n * width + h * LANES, n * width + (h + 1) * LANES)
                    flux[there, outer] = high
                    flux[slice(span + i * ROWS, span + (i + 1) * ROWS), outer] = rest
        total = jnp.dot(flux[0 : 2 * span, :], back_hot[...], preferred_element_type=F32)
        total = total[0:span] + total[span : 2 * span]
        for i in range(2 * count):
            p = 2 * begin + i
            moved[p] = cur[p] - scale[...] * total[i * ROWS : i * ROWS + nfreq]

    def one_step(step, carry):
        @pl.when(step > 0)
        def _():
            pass_on(step, 0, LATE)

        done = 1
        for chunk, (begin, count) in enumerate(CHUNKS):
            compute(step, chunk)
            if chunk == 0:
                edge_sent[step] = moved[0:2]
                edge_copy(step).start()

                @pl.when(step > 0)
                def _():
                    pass_on(step, LATE, pairs)

            if chunk == EDGE_AT:
                edge_copy(step).wait_recv()
                finish_pair(step, 0)
            last = begin + count == pairs
            ready = pairs if last else begin + count - 1
            for pair in range(done, ready):
                finish_pair(step, pair)
            done = max(done, ready)
        return carry

    lax.fori_loop(0, ITERS, one_step, 0)

    for step in range(ITERS):
        edge_copy(step).wait_send()
    for side, role in ((0, passes_down), (1, passes_up)):

        @pl.when(role)
        def _():
            for step in range(ITERS):
                for pair in range(AHEAD if step == 0 else 0, pairs):
                    for e in (0, 1):
                        pass_copy(step, side, pair, e).wait_send()
            for p in range(2 * AHEAD):
                full_pass(side, p).wait_send()

    for side in (0, 1):

        @pl.when(has[side])
        def _():
            tables[side].wait_send()
            for step in range(ITERS):
                for pair in range(AHEAD if step == 0 else 0, pairs):
                    halo_copy(step, side, pair).wait_send()


def on_device(
    field,
    group_speed,
    face_angle,
    face_speed,
    face_cells,
    face_live,
    halo_blocks,
    cell_level,
    polar_mask,
    turn_rate,
):
    dloc, nfreq, own = field.shape
    faces = face_angle.shape[0]
    fblk = faces // LANES
    hb = halo_blocks.shape[2]
    ext = own + 2 * hb * LANES
    pairs = dloc // 2
    any_spec = pl.BlockSpec(memory_space=pl.ANY)
    smem_spec = pl.BlockSpec(memory_space=pltpu.SMEM)
    halo = (ITERS, 2, pairs, 2, hb, nfreq, LANES)
    span = 2 * max(count for _, count in CHUNKS) * ROWS
    return pl.pallas_call(
        kernel,
        out_shape=pltpu.VMEM(field.shape, field.dtype),
        in_specs=[
            any_spec,
            smem_spec,
            any_spec,
            any_spec,
            any_spec,
            smem_spec,
            any_spec,
            any_spec,
            any_spec,
            any_spec,
        ],
        out_specs=pl.BlockSpec(memory_space=pltpu.VMEM),
        scratch_shapes=[
            pltpu.VMEM((dloc, nfreq, own), F32),
            pltpu.VMEM((dloc, nfreq, own), F32),
            pltpu.VMEM(halo, F32),
            pltpu.VMEM(halo, F32),
            pltpu.VMEM((ITERS, 2, nfreq, own), F32),
            pltpu.VMEM((ITERS, 2, nfreq, own), F32),
            pltpu.VMEM((2 * dloc * ROWS, ext), BF16),
            pltpu.VMEM((2 * span, faces), BF16),
            pltpu.VMEM((own, faces), HOT),
            pltpu.VMEM((ext, faces), HOT),
            pltpu.VMEM((faces, own), HOT),
            pltpu.VMEM((dloc, fblk, LANES), F32),
            pltpu.VMEM((nfreq, own), F32),
            pltpu.VMEM((2, own), F32),
            pltpu.VMEM((fblk, LANES), F32),
            pltpu.VMEM((fblk, LANES), F32),
            pltpu.VMEM((2, faces), jnp.int32),
            pltpu.VMEM((1, own), jnp.int32),
            pltpu.VMEM((1, own), jnp.int32),
            pltpu.VMEM((1, own), F32),
            pltpu.VMEM((1, 2, hb), jnp.int32),
            pltpu.VMEM((2, 1, 2, hb), jnp.int32),
            pltpu.VMEM((4 * hb, 8, LANES), jnp.int32),
            pltpu.VMEM((2, 2 * AHEAD, nfreq, own), F32),
            pltpu.VMEM((ITERS, pairs, 2, hb, nfreq, LANES), F32),
            pltpu.VMEM((2 * AHEAD, nfreq, own), F32),
            pltpu.SemaphoreType.DMA((dloc,)),
            pltpu.SemaphoreType.DMA((7,)),
            pltpu.SemaphoreType.DMA((2,)),
            pltpu.SemaphoreType.DMA((2,)),
            pltpu.SemaphoreType.DMA((2, 2 * AHEAD)),
            pltpu.SemaphoreType.DMA((2, 2 * AHEAD)),
            pltpu.SemaphoreType.DMA((2 * AHEAD,)),
            pltpu.SemaphoreType.DMA((2 * AHEAD,)),
            pltpu.SemaphoreType.DMA((ITERS, pairs, 2)),
            pltpu.SemaphoreType.DMA((ITERS, pairs, 2)),
            pltpu.SemaphoreType.DMA((ITERS, 2, pairs)),
            pltpu.SemaphoreType.DMA((ITERS, 2, pairs)),
            pltpu.SemaphoreType.DMA((ITERS,)),
            pltpu.SemaphoreType.DMA((ITERS,)),
        ],
        compiler_params=pltpu.CompilerParams(
            collective_id=0, has_side_effects=True, vmem_limit_bytes=60 * 1024 * 1024
        ),
    )(
        field,
        group_speed,
        face_angle.reshape(fblk, LANES),
        face_speed.reshape(fblk, LANES),
        face_cells,
        face_live,
        halo_blocks,
        cell_level.reshape(1, own),
        polar_mask.reshape(1, own),
        turn_rate.reshape(1, own),
    )


def solution(mesh):
    return jax.shard_map(
        on_device,
        mesh=mesh,
        in_specs=(
            P("spec", None, "rows"),
            P(),
            P("rows"),
            P("rows"),
            P(None, "rows"),
            P("rows"),
            P("rows", None, None),
            P("rows"),
            P("rows"),
            P("rows"),
        ),
        out_specs=P("spec", None, "rows"),
        check_vma=False,
    )
```

```python
import functools
import math

import jax
import jax.numpy as jnp
from jax import lax
from jax.experimental import pallas as pl
from jax.experimental.pallas import tpu as pltpu
from jax.sharding import PartitionSpec as P

MESH = pl.DeviceIdType.MESH
NDIR = 36
ITERS = 3
LANES = 128
ROWS = 32
CHUNKS = ((0, 1), (1, 2), (3, 2), (5, 2), (7, 1), (8, 1))
LATE = 6
AHEAD = 1
EDGE_AT = 2
PLANE = 32
UP, DOWN = 7, 25
HOT = jnp.float8_e4m3fn
BF16 = jnp.bfloat16
F32 = jnp.float32


def split(value):
    high = value.astype(BF16)
    return high, (value - high.astype(F32)).astype(BF16)


def kernel(
    field,
    speed_s,
    angle_h,
    weight_h,
    cells_h,
    live_s,
    table_h,
    level_h,
    mask_h,
    rate_h,
    out,
    cur,
    moved,
    sent,
    got,
    edge_sent,
    edge_got,
    ext,
    flux,
    own_hot,
    up_hot,
    back_hot,
    vel,
    scale,
    turn,
    angle,
    weight,
    cells,
    level,
    mask,
    rate,
    table_v,
    table_r,
    picks,
    full,
    passing,
    pass_full,
    load_sem,
    small_sem,
    table_send,
    table_recv,
    full_send,
    full_recv,
    pass_full_send,
    pass_full_recv,
    pass_send,
    pass_recv,
    send_sem,
    recv_sem,
    edge_send,
    edge_recv,
):
    dloc, nfreq, own = field.shape
    pairs = dloc // 2
    hb = table_h.shape[2]
    faces = cells.shape[1]
    fblk = faces // LANES
    size = lax.axis_size("rows")
    row = lax.axis_index("rows")
    spec = lax.axis_index("spec")
    has = (row > 0, row < size - 1)
    peer = ({"rows": jnp.maximum(row - 1, 0)}, {"rows": jnp.minimum(row + 1, size - 1)})
    partner = {"spec": 1 - spec}

    at = lax.rem(row, PLANE)
    odd = spec == 1

    def other(shift):
        return {"rows": jnp.clip(row + shift, 0, size - 1)}

    via = (odd & (at == 0) & (row > 0), odd & (at == PLANE - 1) & (row < size - 1))
    passes_up = odd & (at == UP) & (row < size - PLANE)
    passes_down = odd & (at == DOWN) & (row >= PLANE)
    relay = (other(DOWN), other(UP + 1 - PLANE))
    roles = (
        (via[0], relay[0], other(UP - PLANE)),
        (via[1], relay[1], other(DOWN + 1)),
        (passes_up, other(PLANE - 1 - UP), other(PLANE - UP)),
        (passes_down, other(-DOWN), other(-DOWN - 1)),
    )

    def slot(d):
        return 2 * d if d < pairs else 2 * (dloc - 1 - d) + 1

    def direction(p):
        return p // 2 if p % 2 == 0 else dloc - 1 - p // 2

    small = [
        pltpu.make_async_copy(src, dst, small_sem.at[i])
        for i, (src, dst) in enumerate(
            (
                (table_h, table_v),
                (cells_h, cells),
                (angle_h, angle),
                (weight_h, weight),
                (level_h, level),
                (mask_h, mask),
                (rate_h, rate),
            )
        )
    ]
    for copy in small:
        copy.start()
    loads = [
        pltpu.make_async_copy(
            field.at[direction(p)], cur.at[p], load_sem.at[p]
        )
        for p in range(dloc)
    ]
    for copy in loads:
        copy.start()
    table_r[...] = jnp.zeros_like(table_r)

    barrier = pltpu.get_barrier_semaphore()
    pl.semaphore_signal(barrier, inc=1, device_id=partner, device_id_type=MESH)
    for side in (0, 1):

        @pl.when(has[side])
        def _():
            pl.semaphore_signal(barrier, inc=1, device_id=peer[side], device_id_type=MESH)

    peers = 1 + has[0].astype(jnp.int32) + has[1].astype(jnp.int32)
    for role, first, second in roles:

        @pl.when(role)
        def _():
            pl.semaphore_signal(barrier, inc=1, device_id=first, device_id_type=MESH)
            pl.semaphore_signal(barrier, inc=1, device_id=second, device_id_type=MESH)

        peers = peers + 2 * role.astype(jnp.int32)
    pl.semaphore_wait(barrier, peers)

    small[0].wait()
    tables = [
        pltpu.make_async_remote_copy(
            src_ref=table_v,
            dst_ref=table_r.at[1 - side],
            send_sem=table_send.at[side],
            recv_sem=table_recv.at[1 - side],
            device_id=peer[side],
            device_id_type=MESH,
        )
        for side in (0, 1)
    ]
    for side in (0, 1):

        @pl.when(has[side])
        def _():
            tables[side].start()

    for copy in loads[0 : 2 * AHEAD]:
        copy.wait()

    def full_copy(side, p):
        return pltpu.make_async_remote_copy(
            src_ref=cur.at[p],
            dst_ref=full.at[1 - side, p],
            send_sem=full_send.at[side, p],
            recv_sem=full_recv.at[1 - side, p],
            device_id=peer[side],
            device_id_type=MESH,
        )

    def full_arrival(side, p):
        return pltpu.make_async_remote_copy(
            src_ref=cur.at[p],
            dst_ref=full.at[side, p],
            send_sem=full_send.at[side, p],
            recv_sem=full_recv.at[side, p],
            device_id=peer[side],
            device_id_type=MESH,
        )

    def full_via(side, p):
        return pltpu.make_async_remote_copy(
            src_ref=cur.at[p],
            dst_ref=pass_full.at[p],
            send_sem=full_send.at[side, p],
            recv_sem=pass_full_recv.at[p],
            device_id=relay[side],
            device_id_type=MESH,
        )

    beyond = (other(-DOWN - 1), other(PLANE - UP))

    def full_pass(side, p):
        return pltpu.make_async_remote_copy(
            src_ref=pass_full.at[p],
            dst_ref=full.at[1 - side, p],
            send_sem=pass_full_send.at[p],
            recv_sem=full_recv.at[1 - side, p],
            device_id=beyond[side],
            device_id_type=MESH,
        )

    for side in (0, 1):

        @pl.when(has[side] & jnp.logical_not(via[side]))
        def _():
            for p in range(2 * AHEAD):
                full_copy(side, p).start()

        @pl.when(via[side])
        def _():
            for p in range(2 * AHEAD):
                full_via(side, p).start()

    for copy in small[1:]:
        copy.wait()

    sub = lax.broadcasted_iota(jnp.int32, (LANES, LANES), 0)
    lane = lax.broadcasted_iota(jnp.int32, (LANES, LANES), 1)
    one = jnp.float32(1.0)
    zero = jnp.float32(0.0)

    def build(j, carry):
        at = pl.ds(pl.multiple_of(j * LANES, LANES), LANES)
        low = jnp.broadcast_to(cells[0:1, at], (LANES, LANES))
        upp = jnp.broadcast_to(cells[1:2, at], (LANES, LANES))
        for c in range(own // LANES):
            own_hot[c * LANES : (c + 1) * LANES, at] = jnp.where(
                low == sub + c * LANES, one, zero
            ).astype(HOT)
        for c in range(up_hot.shape[0] // LANES):
            up_hot[c * LANES : (c + 1) * LANES, at] = jnp.where(
                upp == sub + c * LANES, one, zero
            ).astype(HOT)
        low_t = low.T
        upp_t = upp.T
        for c in range(own // LANES):
            here = lane + c * LANES
            back_hot[at, c * LANES : (c + 1) * LANES] = (
                jnp.where(low_t == here, one, zero) - jnp.where(upp_t == here, one, zero)
            ).astype(HOT)
        return carry

    lax.fori_loop(0, fblk, build, 0)

    blocks = lax.broadcasted_iota(jnp.int32, (fblk, LANES), 0)
    slot_weight = jnp.where(blocks < live_s[0], weight[...], zero)
    along = jnp.cos(angle[...]) * slot_weight
    across = jnp.sin(angle[...]) * slot_weight
    sign = (1 - 2 * spec).astype(F32)
    along = along * sign
    across = across * sign
    for p in range(dloc):
        theta = (direction(p) + 0.5) * (2.0 * math.pi / NDIR)
        vel[p] = along * math.cos(theta) + across * math.sin(theta)

    freq = lax.broadcasted_iota(jnp.int32, (nfreq, LANES), 0)
    group = jnp.zeros((nfreq, LANES), F32)
    for f in range(nfreq):
        group = jnp.where(freq == f, speed_s[f], group)
    for c in range(own // LANES):
        lev = level[0:1, c * LANES : (c + 1) * LANES]
        area = jnp.exp2(-lev.astype(F32))
        scale[:, c * LANES : (c + 1) * LANES] = group * area
    bend = mask[...].astype(F32) * rate[...]
    turn[0:1, :] = jnp.maximum(bend, 0.0)
    turn[1:2, :] = jnp.minimum(bend, 0.0)

    for side in (0, 1):

        @pl.when(jnp.logical_not(has[side]))
        def _():
            def clear(i, carry):
                def inner(j, c):
                    got[i, side, j] = jnp.zeros(got.shape[3:], F32)
                    return c

                return lax.fori_loop(0, pairs, inner, carry)

            lax.fori_loop(0, ITERS, clear, 0)

    for side in (0, 1):

        @pl.when(has[side])
        def _():
            pltpu.make_async_remote_copy(
                src_ref=table_v,
                dst_ref=table_r.at[side],
                send_sem=table_send.at[side],
                recv_sem=table_recv.at[side],
                device_id=peer[side],
                device_id_type=MESH,
            ).wait_recv()

    for side in (0, 1):
        taken = table_r[side, 0]
        for k in range(hb):
            picks[side * hb + k] = jnp.broadcast_to(
                taken[1 - side : 2 - side, k : k + 1], (8, LANES)
            )

    mine = table_v[0]
    for side in (0, 1):
        for k in range(hb):
            picks[(2 + side) * hb + k] = jnp.broadcast_to(
                mine[side : side + 1, k : k + 1], (8, LANES)
            )

    def pick(value, which):
        wanted = jnp.broadcast_to(picks[which, 0:1, :], (nfreq, LANES))
        chosen = value[:, 0:LANES]
        for c in range(1, own // LANES):
            chosen = jnp.where(wanted == c, value[:, c * LANES : (c + 1) * LANES], chosen)
        return chosen

    def halo_copy(step, side, pair):
        return pltpu.make_async_remote_copy(
            src_ref=sent.at[step, side, pair],
            dst_ref=got.at[step, 1 - side, pair],
            send_sem=send_sem.at[step, side, pair],
            recv_sem=recv_sem.at[step, 1 - side, pair],
            device_id=peer[side],
            device_id_type=MESH,
        )

    def via_copy(step, side, pair, e):
        return pltpu.make_async_remote_copy(
            src_ref=sent.at[step, side, pair, e],
            dst_ref=passing.at[step, pair, e],
            send_sem=send_sem.at[step, side, pair],
            recv_sem=pass_recv.at[step, pair, e],
            device_id=relay[side],
            device_id_type=MESH,
        )

    def pass_copy(step, side, pair, e):
        return pltpu.make_async_remote_copy(
            src_ref=passing.at[step, pair, e],
            dst_ref=got.at[step, 1 - side, pair, e],
            send_sem=pass_send.at[step, pair, e],
            recv_sem=recv_sem.at[step, 1 - side, pair],
            device_id=beyond[side],
            device_id_type=MESH,
        )

    def came(ref, send, recv):
        pltpu.make_async_remote_copy(
            src_ref=ref,
            dst_ref=ref,
            send_sem=send,
            recv_sem=recv,
            device_id=other(1),
            device_id_type=MESH,
        ).wait_recv()

    def pass_on(step, first, last):
        for side, role in ((0, passes_down), (1, passes_up)):

            @pl.when(role)
            def _():
                def one(pair, carry):
                    for e in (0, 1):
                        came(
                            passing.at[step, pair, e],
                            pass_send.at[step, pair, e],
                            pass_recv.at[step, pair, e],
                        )
                        pass_copy(step, side, pair, e).start()
                    return carry

                lax.fori_loop(first, last, one, 0)

    def pass_full_on():
        for side, role in ((0, passes_down), (1, passes_up)):

            @pl.when(role)
            def _():
                for p in range(2 * AHEAD):
                    came(pass_full.at[p], pass_full_send.at[p], pass_full_recv.at[p])
                    full_pass(side, p).start()

    def halo_arrival(step, side, pair):
        return pltpu.make_async_remote_copy(
            src_ref=sent.at[step, side, pair],
            dst_ref=got.at[step, side, pair],
            send_sem=send_sem.at[step, side, pair],
            recv_sem=recv_sem.at[step, side, pair],
            device_id=peer[side],
            device_id_type=MESH,
        )

    def send_pair(step, pair):
        for side in (0, 1):
            for e in (0, 1):
                value = cur[2 * pair + e]
                for k in range(hb):
                    sent[step, side, pair, e, k] = pick(value, side * hb + k)

            @pl.when(has[side] & jnp.logical_not(via[side]))
            def _():
                halo_copy(step, side, pair).start()

            @pl.when(via[side])
            def _():
                for e in (0, 1):
                    via_copy(step, side, pair, e).start()

    home = {}
    for begin, count in CHUNKS:
        for p in range(2 * begin, 2 * (begin + count)):
            home[p] = (4 * begin * ROWS + (p - 2 * begin) * ROWS, 2 * count * ROWS)

    def put(p, at, value):
        first, span = home[p]
        high, low = split(value)
        ext[first : first + nfreq, at] = high
        ext[first + span : first + span + nfreq, at] = low

    def split_own(p):
        put(p, slice(0, own), cur[p])

    for copy in loads[2 * AHEAD :]:
        copy.wait()
    for pair in range(AHEAD, pairs):
        send_pair(0, pair)
    for p in range(dloc):
        split_own(p)
    pass_full_on()
    pass_on(0, AHEAD, pairs)
    for side in (0, 1):

        @pl.when(has[side])
        def _():
            for p in range(2 * AHEAD):
                full_arrival(side, p).wait_recv()
                value = full[side, p]
                for k in range(hb):
                    got[0, side, p // 2, p % 2, k] = pick(value, (2 + side) * hb + k)
            for p in range(2 * AHEAD):
                full_copy(side, p).wait_send()

    def turn_slot(step, p):
        d = direction(p)
        here = moved[p]
        before = moved[slot(d - 1)] if d > 0 else edge_got[step, 1]
        after = moved[slot(d + 1)] if d < dloc - 1 else edge_got[step, 0]
        cur[p] = here - turn[0:1, :] * (here - before) - turn[1:2, :] * (after - here)
        split_own(p)

    def edge_copy(step):
        return pltpu.make_async_remote_copy(
            src_ref=edge_sent.at[step],
            dst_ref=edge_got.at[step],
            send_sem=edge_send.at[step],
            recv_sem=edge_recv.at[step],
            device_id=partner,
            device_id_type=MESH,
        )

    def finish_pair(step, pair):
        turn_slot(step, 2 * pair)
        turn_slot(step, 2 * pair + 1)

        @pl.when(step < ITERS - 1)
        def _():
            send_pair(step + 1, pair)

        @pl.when(step == ITERS - 1)
        def _():
            for p in (2 * pair, 2 * pair + 1):
                out[direction(p)] = cur[p]

    def compute(step, chunk):
        begin, count = CHUNKS[chunk]
        span = 2 * count * ROWS
        rows = slice(4 * begin * ROWS, 4 * begin * ROWS + 2 * span)
        for pair in range(begin, begin + count):
            for side in (0, 1):
                awaited = has[side] if pair >= AHEAD else has[side] & (step > 0)

                @pl.when(awaited)
                def _():
                    halo_arrival(step, side, pair).wait_recv()

            for side in (0, 1):
                for e in (0, 1):
                    for k in range(hb):
                        first = own + (side * hb + k) * LANES
                        put(2 * pair + e, slice(first, first + LANES), got[step, side, pair, e, k])
        width = 2 * LANES
        for n in range(faces // width):
            at = slice(n * width, (n + 1) * width)
            low = jnp.dot(ext[rows, 0:own], own_hot[:, at], preferred_element_type=F32)
            upp = jnp.dot(ext[rows, :], up_hot[:, at], preferred_element_type=F32)
            low = low[0:span] + low[span : 2 * span]
            upp = upp[0:span] + upp[span : 2 * span]
            for i in range(2 * count):
                p = 2 * begin + i
                there = slice(i * ROWS, (i + 1) * ROWS)
                for h in range(2):
                    inner = slice(h * LANES, (h + 1) * LANES)
                    u = jnp.broadcast_to(
                        vel[p, 2 * n + h : 2 * n + h + 1, :], (ROWS, LANES)
                    )
                    flow = u * jnp.where(u > 0.0, low[there, inner], upp[there, inner])
                    high, rest = split(flow)
                    outer = slice(n * width + h * LANES, n * width + (h + 1) * LANES)
                    flux[there, outer] = high
                    flux[slice(span + i * ROWS, span + (i + 1) * ROWS), outer] = rest
        total = jnp.dot(flux[0 : 2 * span, :], back_hot[...], preferred_element_type=F32)
        total = total[0:span] + total[span : 2 * span]
        for i in range(2 * count):
            p = 2 * begin + i
            moved[p] = cur[p] - scale[...] * total[i * ROWS : i * ROWS + nfreq]

    def one_step(step, carry):
        @pl.when(step > 0)
        def _():
            pass_on(step, 0, LATE)

        done = 1
        for chunk, (begin, count) in enumerate(CHUNKS):
            compute(step, chunk)
            if chunk == 0:
                edge_sent[step] = moved[0:2]
                edge_copy(step).start()

                @pl.when(step > 0)
                def _():
                    pass_on(step, LATE, pairs)

            if chunk == EDGE_AT:
                edge_copy(step).wait_recv()
                finish_pair(step, 0)
            last = begin + count == pairs
            ready = pairs if last else begin + count - 1
            for pair in range(done, ready):
                finish_pair(step, pair)
            done = max(done, ready)
        return carry

    lax.fori_loop(0, ITERS, one_step, 0)

    for step in range(ITERS):
        edge_copy(step).wait_send()
    for side, role in ((0, passes_down), (1, passes_up)):

        @pl.when(role)
        def _():
            for step in range(ITERS):
                for pair in range(AHEAD if step == 0 else 0, pairs):
                    for e in (0, 1):
                        pass_copy(step, side, pair, e).wait_send()
            for p in range(2 * AHEAD):
                full_pass(side, p).wait_send()

    for side in (0, 1):

        @pl.when(has[side])
        def _():
            tables[side].wait_send()
            for step in range(ITERS):
                for pair in range(AHEAD if step == 0 else 0, pairs):
                    halo_copy(step, side, pair).wait_send()


def on_device(
    field,
    group_speed,
    face_angle,
    face_speed,
    face_cells,
    face_live,
    halo_blocks,
    cell_level,
    polar_mask,
    turn_rate,
):
    dloc, nfreq, own = field.shape
    faces = face_angle.shape[0]
    fblk = faces // LANES
    hb = halo_blocks.shape[2]
    ext = own + 2 * hb * LANES
    pairs = dloc // 2
    any_spec = pl.BlockSpec(memory_space=pl.ANY)
    smem_spec = pl.BlockSpec(memory_space=pltpu.SMEM)
    halo = (ITERS, 2, pairs, 2, hb, nfreq, LANES)
    span = 2 * max(count for _, count in CHUNKS) * ROWS
    return pl.pallas_call(
        kernel,
        out_shape=pltpu.VMEM(field.shape, field.dtype),
        in_specs=[
            any_spec,
            smem_spec,
            any_spec,
            any_spec,
            any_spec,
            smem_spec,
            any_spec,
            any_spec,
            any_spec,
            any_spec,
        ],
        out_specs=pl.BlockSpec(memory_space=pltpu.VMEM),
        scratch_shapes=[
            pltpu.VMEM((dloc, nfreq, own), F32),
            pltpu.VMEM((dloc, nfreq, own), F32),
            pltpu.VMEM(halo, F32),
            pltpu.VMEM(halo, F32),
            pltpu.VMEM((ITERS, 2, nfreq, own), F32),
            pltpu.VMEM((ITERS, 2, nfreq, own), F32),
            pltpu.VMEM((2 * dloc * ROWS, ext), BF16),
            pltpu.VMEM((2 * span, faces), BF16),
            pltpu.VMEM((own, faces), HOT),
            pltpu.VMEM((ext, faces), HOT),
            pltpu.VMEM((faces, own), HOT),
            pltpu.VMEM((dloc, fblk, LANES), F32),
            pltpu.VMEM((nfreq, own), F32),
            pltpu.VMEM((2, own), F32),
            pltpu.VMEM((fblk, LANES), F32),
            pltpu.VMEM((fblk, LANES), F32),
            pltpu.VMEM((2, faces), jnp.int32),
            pltpu.VMEM((1, own), jnp.int32),
            pltpu.VMEM((1, own), jnp.int32),
            pltpu.VMEM((1, own), F32),
            pltpu.VMEM((1, 2, hb), jnp.int32),
            pltpu.VMEM((2, 1, 2, hb), jnp.int32),
            pltpu.VMEM((4 * hb, 8, LANES), jnp.int32),
            pltpu.VMEM((2, 2 * AHEAD, nfreq, own), F32),
            pltpu.VMEM((ITERS, pairs, 2, hb, nfreq, LANES), F32),
            pltpu.VMEM((2 * AHEAD, nfreq, own), F32),
            pltpu.SemaphoreType.DMA((dloc,)),
            pltpu.SemaphoreType.DMA((7,)),
            pltpu.SemaphoreType.DMA((2,)),
            pltpu.SemaphoreType.DMA((2,)),
            pltpu.SemaphoreType.DMA((2, 2 * AHEAD)),
            pltpu.SemaphoreType.DMA((2, 2 * AHEAD)),
            pltpu.SemaphoreType.DMA((2 * AHEAD,)),
            pltpu.SemaphoreType.DMA((2 * AHEAD,)),
            pltpu.SemaphoreType.DMA((ITERS, pairs, 2)),
            pltpu.SemaphoreType.DMA((ITERS, pairs, 2)),
            pltpu.SemaphoreType.DMA((ITERS, 2, pairs)),
            pltpu.SemaphoreType.DMA((ITERS, 2, pairs)),
            pltpu.SemaphoreType.DMA((ITERS,)),
            pltpu.SemaphoreType.DMA((ITERS,)),
        ],
        compiler_params=pltpu.CompilerParams(
            collective_id=0, has_side_effects=True, vmem_limit_bytes=60 * 1024 * 1024
        ),
    )(
        field,
        group_speed,
        face_angle.reshape(fblk, LANES),
        face_speed.reshape(fblk, LANES),
        face_cells,
        face_live,
        halo_blocks,
        cell_level.reshape(1, own),
        polar_mask.reshape(1, own),
        turn_rate.reshape(1, own),
    )


def solution(mesh):
    return jax.shard_map(
        on_device,
        mesh=mesh,
        in_specs=(
            P("spec", None, "rows"),
            P(),
            P("rows"),
            P("rows"),
            P(None, "rows"),
            P("rows"),
            P("rows", None, None),
            P("rows"),
            P("rows"),
            P("rows"),
        ),
        out_specs=P("spec", None, "rows"),
        check_vma=False,
    )
```

```python
import functools
import math

import jax
import jax.numpy as jnp
from jax import lax
from jax.experimental import pallas as pl
from jax.experimental.pallas import tpu as pltpu
from jax.sharding import PartitionSpec as P

MESH = pl.DeviceIdType.MESH
NDIR = 36
ITERS = 3
LANES = 128
ROWS = 32
CHUNKS = ((0, 1), (1, 2), (3, 2), (5, 2), (7, 1), (8, 1))
LATE = 9
AHEAD = 2
EDGE_AT = 2
PLANE = 32
UP, DOWN = 7, 25
HOT = jnp.float8_e4m3fn
BF16 = jnp.bfloat16
F32 = jnp.float32


def split(value):
    high = value.astype(BF16)
    return high, (value - high.astype(F32)).astype(BF16)


def kernel(
    field,
    speed_s,
    angle_h,
    weight_h,
    cells_h,
    live_s,
    table_h,
    level_h,
    mask_h,
    rate_h,
    out,
    cur,
    moved,
    sent,
    got,
    edge_sent,
    edge_got,
    ext,
    flux,
    own_hot,
    up_hot,
    back_hot,
    vel,
    scale,
    turn,
    angle,
    weight,
    cells,
    level,
    mask,
    rate,
    table_v,
    table_r,
    picks,
    full,
    passing,
    pass_full,
    load_sem,
    small_sem,
    table_send,
    table_recv,
    full_send,
    full_recv,
    pass_full_send,
    pass_full_recv,
    pass_send,
    pass_recv,
    send_sem,
    recv_sem,
    edge_send,
    edge_recv,
):
    dloc, nfreq, own = field.shape
    pairs = dloc // 2
    hb = table_h.shape[2]
    faces = cells.shape[1]
    fblk = faces // LANES
    size = lax.axis_size("rows")
    row = lax.axis_index("rows")
    spec = lax.axis_index("spec")
    has = (row > 0, row < size - 1)
    peer = ({"rows": jnp.maximum(row - 1, 0)}, {"rows": jnp.minimum(row + 1, size - 1)})
    partner = {"spec": 1 - spec}

    at = lax.rem(row, PLANE)
    odd = spec == 1

    def other(shift):
        return {"rows": jnp.clip(row + shift, 0, size - 1)}

    via = (odd & (at == 0) & (row > 0), odd & (at == PLANE - 1) & (row < size - 1))
    passes_up = odd & (at == UP) & (row < size - PLANE)
    passes_down = odd & (at == DOWN) & (row >= PLANE)
    relay = (other(DOWN), other(UP + 1 - PLANE))
    roles = (
        (via[0], relay[0], other(UP - PLANE)),
        (via[1], relay[1], other(DOWN + 1)),
        (passes_up, other(PLANE - 1 - UP), other(PLANE - UP)),
        (passes_down, other(-DOWN), other(-DOWN - 1)),
    )

    def slot(d):
        return 2 * d if d < pairs else 2 * (dloc - 1 - d) + 1

    def direction(p):
        return p // 2 if p % 2 == 0 else dloc - 1 - p // 2

    small = [
        pltpu.make_async_copy(src, dst, small_sem.at[i])
        for i, (src, dst) in enumerate(
            (
                (table_h, table_v),
                (cells_h, cells),
                (angle_h, angle),
                (weight_h, weight),
                (level_h, level),
                (mask_h, mask),
                (rate_h, rate),
            )
        )
    ]
    for copy in small:
        copy.start()
    loads = [
        pltpu.make_async_copy(
            field.at[direction(p)], cur.at[p], load_sem.at[p]
        )
        for p in range(dloc)
    ]
    for copy in loads:
        copy.start()
    table_r[...] = jnp.zeros_like(table_r)

    barrier = pltpu.get_barrier_semaphore()
    pl.semaphore_signal(barrier, inc=1, device_id=partner, device_id_type=MESH)
    for side in (0, 1):

        @pl.when(has[side])
        def _():
            pl.semaphore_signal(barrier, inc=1, device_id=peer[side], device_id_type=MESH)

    peers = 1 + has[0].astype(jnp.int32) + has[1].astype(jnp.int32)
    for role, first, second in roles:

        @pl.when(role)
        def _():
            pl.semaphore_signal(barrier, inc=1, device_id=first, device_id_type=MESH)
            pl.semaphore_signal(barrier, inc=1, device_id=second, device_id_type=MESH)

        peers = peers + 2 * role.astype(jnp.int32)
    pl.semaphore_wait(barrier, peers)

    small[0].wait()
    tables = [
        pltpu.make_async_remote_copy(
            src_ref=table_v,
            dst_ref=table_r.at[1 - side],
            send_sem=table_send.at[side],
            recv_sem=table_recv.at[1 - side],
            device_id=peer[side],
            device_id_type=MESH,
        )
        for side in (0, 1)
    ]
    for side in (0, 1):

        @pl.when(has[side])
        def _():
            tables[side].start()

    for copy in loads[0 : 2 * AHEAD]:
        copy.wait()

    def full_copy(side, p):
        return pltpu.make_async_remote_copy(
            src_ref=cur.at[p],
            dst_ref=full.at[1 - side, p],
            send_sem=full_send.at[side, p],
            recv_sem=full_recv.at[1 - side, p],
            device_id=peer[side],
            device_id_type=MESH,
        )

    def full_arrival(side, p):
        return pltpu.make_async_remote_copy(
            src_ref=cur.at[p],
            dst_ref=full.at[side, p],
            send_sem=full_send.at[side, p],
            recv_sem=full_recv.at[side, p],
            device_id=peer[side],
            device_id_type=MESH,
        )

    def full_via(side, p):
        return pltpu.make_async_remote_copy(
            src_ref=cur.at[p],
            dst_ref=pass_full.at[p],
            send_sem=full_send.at[side, p],
            recv_sem=pass_full_recv.at[p],
            device_id=relay[side],
            device_id_type=MESH,
        )

    beyond = (other(-DOWN - 1), other(PLANE - UP))

    def full_pass(side, p):
        return pltpu.make_async_remote_copy(
            src_ref=pass_full.at[p],
            dst_ref=full.at[1 - side, p],
            send_sem=pass_full_send.at[p],
            recv_sem=full_recv.at[1 - side, p],
            device_id=beyond[side],
            device_id_type=MESH,
        )

    for side in (0, 1):

        @pl.when(has[side] & jnp.logical_not(via[side]))
        def _():
            for p in range(2 * AHEAD):
                full_copy(side, p).start()

        @pl.when(via[side])
        def _():
            for p in range(2 * AHEAD):
                full_via(side, p).start()

    for copy in small[1:]:
        copy.wait()

    sub = lax.broadcasted_iota(jnp.int32, (LANES, LANES), 0)
    lane = lax.broadcasted_iota(jnp.int32, (LANES, LANES), 1)
    one = jnp.float32(1.0)
    zero = jnp.float32(0.0)

    def build(j, carry):
        at = pl.ds(pl.multiple_of(j * LANES, LANES), LANES)
        low = jnp.broadcast_to(cells[0:1, at], (LANES, LANES))
        upp = jnp.broadcast_to(cells[1:2, at], (LANES, LANES))
        for c in range(own // LANES):
            own_hot[c * LANES : (c + 1) * LANES, at] = jnp.where(
                low == sub + c * LANES, one, zero
            ).astype(HOT)
        for c in range(up_hot.shape[0] // LANES):
            up_hot[c * LANES : (c + 1) * LANES, at] = jnp.where(
                upp == sub + c * LANES, one, zero
            ).astype(HOT)
        low_t = low.T
        upp_t = upp.T
        for c in range(own // LANES):
            here = lane + c * LANES
            back_hot[at, c * LANES : (c + 1) * LANES] = (
                jnp.where(low_t == here, one, zero) - jnp.where(upp_t == here, one, zero)
            ).astype(HOT)
        return carry

    lax.fori_loop(0, fblk, build, 0)

    blocks = lax.broadcasted_iota(jnp.int32, (fblk, LANES), 0)
    slot_weight = jnp.where(blocks < live_s[0], weight[...], zero)
    along = jnp.cos(angle[...]) * slot_weight
    across = jnp.sin(angle[...]) * slot_weight
    sign = (1 - 2 * spec).astype(F32)
    along = along * sign
    across = across * sign
    for p in range(dloc):
        theta = (direction(p) + 0.5) * (2.0 * math.pi / NDIR)
        vel[p] = along * math.cos(theta) + across * math.sin(theta)

    freq = lax.broadcasted_iota(jnp.int32, (nfreq, LANES), 0)
    group = jnp.zeros((nfreq, LANES), F32)
    for f in range(nfreq):
        group = jnp.where(freq == f, speed_s[f], group)
    for c in range(own // LANES):
        lev = level[0:1, c * LANES : (c + 1) * LANES]
        area = jnp.exp2(-lev.astype(F32))
        scale[:, c * LANES : (c + 1) * LANES] = group * area
    bend = mask[...].astype(F32) * rate[...]
    turn[0:1, :] = jnp.maximum(bend, 0.0)
    turn[1:2, :] = jnp.minimum(bend, 0.0)

    for side in (0, 1):

        @pl.when(jnp.logical_not(has[side]))
        def _():
            def clear(i, carry):
                def inner(j, c):
                    got[i, side, j] = jnp.zeros(got.shape[3:], F32)
                    return c

                return lax.fori_loop(0, pairs, inner, carry)

            lax.fori_loop(0, ITERS, clear, 0)

    for side in (0, 1):

        @pl.when(has[side])
        def _():
            pltpu.make_async_remote_copy(
                src_ref=table_v,
                dst_ref=table_r.at[side],
                send_sem=table_send.at[side],
                recv_sem=table_recv.at[side],
                device_id=peer[side],
                device_id_type=MESH,
            ).wait_recv()

    for side in (0, 1):
        taken = table_r[side, 0]
        for k in range(hb):
            picks[side * hb + k] = jnp.broadcast_to(
                taken[1 - side : 2 - side, k : k + 1], (8, LANES)
            )

    mine = table_v[0]
    for side in (0, 1):
        for k in range(hb):
            picks[(2 + side) * hb + k] = jnp.broadcast_to(
                mine[side : side + 1, k : k + 1], (8, LANES)
            )

    def pick(value, which):
        wanted = jnp.broadcast_to(picks[which, 0:1, :], (nfreq, LANES))
        chosen = value[:, 0:LANES]
        for c in range(1, own // LANES):
            chosen = jnp.where(wanted == c, value[:, c * LANES : (c + 1) * LANES], chosen)
        return chosen

    def halo_copy(step, side, pair):
        return pltpu.make_async_remote_copy(
            src_ref=sent.at[step, side, pair],
            dst_ref=got.at[step, 1 - side, pair],
            send_sem=send_sem.at[step, side, pair],
            recv_sem=recv_sem.at[step, 1 - side, pair],
            device_id=peer[side],
            device_id_type=MESH,
        )

    def via_copy(step, side, pair, e):
        return pltpu.make_async_remote_copy(
            src_ref=sent.at[step, side, pair, e],
            dst_ref=passing.at[step, pair, e],
            send_sem=send_sem.at[step, side, pair],
            recv_sem=pass_recv.at[step, pair, e],
            device_id=relay[side],
            device_id_type=MESH,
        )

    def pass_copy(step, side, pair, e):
        return pltpu.make_async_remote_copy(
            src_ref=passing.at[step, pair, e],
            dst_ref=got.at[step, 1 - side, pair, e],
            send_sem=pass_send.at[step, pair, e],
            recv_sem=recv_sem.at[step, 1 - side, pair],
            device_id=beyond[side],
            device_id_type=MESH,
        )

    def came(ref, send, recv):
        pltpu.make_async_remote_copy(
            src_ref=ref,
            dst_ref=ref,
            send_sem=send,
            recv_sem=recv,
            device_id=other(1),
            device_id_type=MESH,
        ).wait_recv()

    def pass_on(step, first, last):
        for side, role in ((0, passes_down), (1, passes_up)):

            @pl.when(role)
            def _():
                def one(pair, carry):
                    for e in (0, 1):
                        came(
                            passing.at[step, pair, e],
                            pass_send.at[step, pair, e],
                            pass_recv.at[step, pair, e],
                        )
                        pass_copy(step, side, pair, e).start()
                    return carry

                lax.fori_loop(first, last, one, 0)

    def pass_full_on():
        for side, role in ((0, passes_down), (1, passes_up)):

            @pl.when(role)
            def _():
                for p in range(2 * AHEAD):
                    came(pass_full.at[p], pass_full_send.at[p], pass_full_recv.at[p])
                    full_pass(side, p).start()

    def halo_arrival(step, side, pair):
        return pltpu.make_async_remote_copy(
            src_ref=sent.at[step, side, pair],
            dst_ref=got.at[step, side, pair],
            send_sem=send_sem.at[step, side, pair],
            recv_sem=recv_sem.at[step, side, pair],
            device_id=peer[side],
            device_id_type=MESH,
        )

    def send_pair(step, pair):
        for side in (0, 1):
            for e in (0, 1):
                value = cur[2 * pair + e]
                for k in range(hb):
                    sent[step, side, pair, e, k] = pick(value, side * hb + k)

            @pl.when(has[side] & jnp.logical_not(via[side]))
            def _():
                halo_copy(step, side, pair).start()

            @pl.when(via[side])
            def _():
                for e in (0, 1):
                    via_copy(step, side, pair, e).start()

    home = {}
    for begin, count in CHUNKS:
        for p in range(2 * begin, 2 * (begin + count)):
            home[p] = (4 * begin * ROWS + (p - 2 * begin) * ROWS, 2 * count * ROWS)

    def put(p, at, value):
        first, span = home[p]
        high, low = split(value)
        ext[first : first + nfreq, at] = high
        ext[first + span : first + span + nfreq, at] = low

    def split_own(p):
        put(p, slice(0, own), cur[p])

    for copy in loads[2 * AHEAD :]:
        copy.wait()
    for pair in range(AHEAD, pairs):
        send_pair(0, pair)
    for p in range(dloc):
        split_own(p)
    pass_full_on()
    pass_on(0, AHEAD, pairs)
    for side in (0, 1):

        @pl.when(has[side])
        def _():
            for p in range(2 * AHEAD):
                full_arrival(side, p).wait_recv()
                value = full[side, p]
                for k in range(hb):
                    got[0, side, p // 2, p % 2, k] = pick(value, (2 + side) * hb + k)
            for p in range(2 * AHEAD):
                full_copy(side, p).wait_send()

    def turn_slot(step, p):
        d = direction(p)
        here = moved[p]
        before = moved[slot(d - 1)] if d > 0 else edge_got[step, 1]
        after = moved[slot(d + 1)] if d < dloc - 1 else edge_got[step, 0]
        cur[p] = here - turn[0:1, :] * (here - before) - turn[1:2, :] * (after - here)
        split_own(p)

    def edge_copy(step):
        return pltpu.make_async_remote_copy(
            src_ref=edge_sent.at[step],
            dst_ref=edge_got.at[step],
            send_sem=edge_send.at[step],
            recv_sem=edge_recv.at[step],
            device_id=partner,
            device_id_type=MESH,
        )

    def finish_pair(step, pair):
        turn_slot(step, 2 * pair)
        turn_slot(step, 2 * pair + 1)

        @pl.when(step < ITERS - 1)
        def _():
            send_pair(step + 1, pair)

        @pl.when(step == ITERS - 1)
        def _():
            for p in (2 * pair, 2 * pair + 1):
                out[direction(p)] = cur[p]

    def compute(step, chunk):
        begin, count = CHUNKS[chunk]
        span = 2 * count * ROWS
        rows = slice(4 * begin * ROWS, 4 * begin * ROWS + 2 * span)
        for pair in range(begin, begin + count):
            for side in (0, 1):
                awaited = has[side] if pair >= AHEAD else has[side] & (step > 0)

                @pl.when(awaited)
                def _():
                    halo_arrival(step, side, pair).wait_recv()

            for side in (0, 1):
                for e in (0, 1):
                    for k in range(hb):
                        first = own + (side * hb + k) * LANES
                        put(2 * pair + e, slice(first, first + LANES), got[step, side, pair, e, k])
        width = 2 * LANES
        for n in range(faces // width):
            at = slice(n * width, (n + 1) * width)
            low = jnp.dot(ext[rows, 0:own], own_hot[:, at], preferred_element_type=F32)
            upp = jnp.dot(ext[rows, :], up_hot[:, at], preferred_element_type=F32)
            low = low[0:span] + low[span : 2 * span]
            upp = upp[0:span] + upp[span : 2 * span]
            for i in range(2 * count):
                p = 2 * begin + i
                there = slice(i * ROWS, (i + 1) * ROWS)
                for h in range(2):
                    inner = slice(h * LANES, (h + 1) * LANES)
                    u = jnp.broadcast_to(
                        vel[p, 2 * n + h : 2 * n + h + 1, :], (ROWS, LANES)
                    )
                    flow = u * jnp.where(u > 0.0, low[there, inner], upp[there, inner])
                    high, rest = split(flow)
                    outer = slice(n * width + h * LANES, n * width + (h + 1) * LANES)
                    flux[there, outer] = high
                    flux[slice(span + i * ROWS, span + (i + 1) * ROWS), outer] = rest
        total = jnp.dot(flux[0 : 2 * span, :], back_hot[...], preferred_element_type=F32)
        total = total[0:span] + total[span : 2 * span]
        for i in range(2 * count):
            p = 2 * begin + i
            moved[p] = cur[p] - scale[...] * total[i * ROWS : i * ROWS + nfreq]

    def one_step(step, carry):
        @pl.when(step > 0)
        def _():
            pass_on(step, 0, LATE)

        done = 1
        for chunk, (begin, count) in enumerate(CHUNKS):
            compute(step, chunk)
            if chunk == 0:
                edge_sent[step] = moved[0:2]
                edge_copy(step).start()

                @pl.when(step > 0)
                def _():
                    pass_on(step, LATE, pairs)

            if chunk == EDGE_AT:
                edge_copy(step).wait_recv()
                finish_pair(step, 0)
            last = begin + count == pairs
            ready = pairs if last else begin + count - 1
            for pair in range(done, ready):
                finish_pair(step, pair)
            done = max(done, ready)
        return carry

    lax.fori_loop(0, ITERS, one_step, 0)

    for step in range(ITERS):
        edge_copy(step).wait_send()
    for side, role in ((0, passes_down), (1, passes_up)):

        @pl.when(role)
        def _():
            for step in range(ITERS):
                for pair in range(AHEAD if step == 0 else 0, pairs):
                    for e in (0, 1):
                        pass_copy(step, side, pair, e).wait_send()
            for p in range(2 * AHEAD):
                full_pass(side, p).wait_send()

    for side in (0, 1):

        @pl.when(has[side])
        def _():
            tables[side].wait_send()
            for step in range(ITERS):
                for pair in range(AHEAD if step == 0 else 0, pairs):
                    halo_copy(step, side, pair).wait_send()


def on_device(
    field,
    group_speed,
    face_angle,
    face_speed,
    face_cells,
    face_live,
    halo_blocks,
    cell_level,
    polar_mask,
    turn_rate,
):
    dloc, nfreq, own = field.shape
    faces = face_angle.shape[0]
    fblk = faces // LANES
    hb = halo_blocks.shape[2]
    ext = own + 2 * hb * LANES
    pairs = dloc // 2
    any_spec = pl.BlockSpec(memory_space=pl.ANY)
    smem_spec = pl.BlockSpec(memory_space=pltpu.SMEM)
    halo = (ITERS, 2, pairs, 2, hb, nfreq, LANES)
    span = 2 * max(count for _, count in CHUNKS) * ROWS
    return pl.pallas_call(
        kernel,
        out_shape=pltpu.VMEM(field.shape, field.dtype),
        in_specs=[
            any_spec,
            smem_spec,
            any_spec,
            any_spec,
            any_spec,
            smem_spec,
            any_spec,
            any_spec,
            any_spec,
            any_spec,
        ],
        out_specs=pl.BlockSpec(memory_space=pltpu.VMEM),
        scratch_shapes=[
            pltpu.VMEM((dloc, nfreq, own), F32),
            pltpu.VMEM((dloc, nfreq, own), F32),
            pltpu.VMEM(halo, F32),
            pltpu.VMEM(halo, F32),
            pltpu.VMEM((ITERS, 2, nfreq, own), F32),
            pltpu.VMEM((ITERS, 2, nfreq, own), F32),
            pltpu.VMEM((2 * dloc * ROWS, ext), BF16),
            pltpu.VMEM((2 * span, faces), BF16),
            pltpu.VMEM((own, faces), HOT),
            pltpu.VMEM((ext, faces), HOT),
            pltpu.VMEM((faces, own), HOT),
            pltpu.VMEM((dloc, fblk, LANES), F32),
            pltpu.VMEM((nfreq, own), F32),
            pltpu.VMEM((2, own), F32),
            pltpu.VMEM((fblk, LANES), F32),
            pltpu.VMEM((fblk, LANES), F32),
            pltpu.VMEM((2, faces), jnp.int32),
            pltpu.VMEM((1, own), jnp.int32),
            pltpu.VMEM((1, own), jnp.int32),
            pltpu.VMEM((1, own), F32),
            pltpu.VMEM((1, 2, hb), jnp.int32),
            pltpu.VMEM((2, 1, 2, hb), jnp.int32),
            pltpu.VMEM((4 * hb, 8, LANES), jnp.int32),
            pltpu.VMEM((2, 2 * AHEAD, nfreq, own), F32),
            pltpu.VMEM((ITERS, pairs, 2, hb, nfreq, LANES), F32),
            pltpu.VMEM((2 * AHEAD, nfreq, own), F32),
            pltpu.SemaphoreType.DMA((dloc,)),
            pltpu.SemaphoreType.DMA((7,)),
            pltpu.SemaphoreType.DMA((2,)),
            pltpu.SemaphoreType.DMA((2,)),
            pltpu.SemaphoreType.DMA((2, 2 * AHEAD)),
            pltpu.SemaphoreType.DMA((2, 2 * AHEAD)),
            pltpu.SemaphoreType.DMA((2 * AHEAD,)),
            pltpu.SemaphoreType.DMA((2 * AHEAD,)),
            pltpu.SemaphoreType.DMA((ITERS, pairs, 2)),
            pltpu.SemaphoreType.DMA((ITERS, pairs, 2)),
            pltpu.SemaphoreType.DMA((ITERS, 2, pairs)),
            pltpu.SemaphoreType.DMA((ITERS, 2, pairs)),
            pltpu.SemaphoreType.DMA((ITERS,)),
            pltpu.SemaphoreType.DMA((ITERS,)),
        ],
        compiler_params=pltpu.CompilerParams(
            collective_id=0, has_side_effects=True, vmem_limit_bytes=60 * 1024 * 1024
        ),
    )(
        field,
        group_speed,
        face_angle.reshape(fblk, LANES),
        face_speed.reshape(fblk, LANES),
        face_cells,
        face_live,
        halo_blocks,
        cell_level.reshape(1, own),
        polar_mask.reshape(1, own),
        turn_rate.reshape(1, own),
    )


def solution(mesh):
    return jax.shard_map(
        on_device,
        mesh=mesh,
        in_specs=(
            P("spec", None, "rows"),
            P(),
            P("rows"),
            P("rows"),
            P(None, "rows"),
            P("rows"),
            P("rows", None, None),
            P("rows"),
            P("rows"),
            P("rows"),
        ),
        out_specs=P("spec", None, "rows"),
        check_vma=False,
    )
```

```python
import functools
import math

import jax
import jax.numpy as jnp
from jax import lax
from jax.experimental import pallas as pl
from jax.experimental.pallas import tpu as pltpu
from jax.sharding import PartitionSpec as P

MESH = pl.DeviceIdType.MESH
NDIR = 36
ITERS = 3
LANES = 128
ROWS = 32
CHUNKS = ((0, 1), (1, 2), (3, 2), (5, 2), (7, 1), (8, 1))
AHEAD = 2
EDGE_AT = 2
PLANE = 32
UP, DOWN = 7, 25
HOT = jnp.float8_e4m3fn
BF16 = jnp.bfloat16
F32 = jnp.float32


def split(value):
    high = value.astype(BF16)
    return high, (value - high.astype(F32)).astype(BF16)


def kernel(
    field,
    speed_s,
    angle_h,
    weight_h,
    cells_h,
    live_s,
    table_h,
    level_h,
    mask_h,
    rate_h,
    out,
    cur,
    moved,
    sent,
    got,
    edge_sent,
    edge_got,
    ext,
    flux,
    own_hot,
    up_hot,
    back_hot,
    vel,
    scale,
    turn,
    angle,
    weight,
    cells,
    level,
    mask,
    rate,
    table_v,
    table_r,
    picks,
    full,
    passing,
    load_sem,
    small_sem,
    table_send,
    table_recv,
    full_send,
    full_recv,
    pass_send,
    pass_recv,
    send_sem,
    recv_sem,
    edge_send,
    edge_recv,
):
    dloc, nfreq, own = field.shape
    pairs = dloc // 2
    hb = table_h.shape[2]
    faces = cells.shape[1]
    fblk = faces // LANES
    size = lax.axis_size("rows")
    row = lax.axis_index("rows")
    spec = lax.axis_index("spec")
    has = (row > 0, row < size - 1)
    peer = ({"rows": jnp.maximum(row - 1, 0)}, {"rows": jnp.minimum(row + 1, size - 1)})
    partner = {"spec": 1 - spec}

    at = lax.rem(row, PLANE)
    odd = spec == 1

    def other(shift):
        return {"rows": jnp.clip(row + shift, 0, size - 1)}

    via = (odd & (at == 0) & (row > 0), odd & (at == PLANE - 1) & (row < size - 1))
    passes_up = odd & (at == UP) & (row < size - PLANE)
    passes_down = odd & (at == DOWN) & (row >= PLANE)
    relay = (other(DOWN), other(UP + 1 - PLANE))
    roles = (
        (via[0], relay[0], other(UP - PLANE)),
        (via[1], relay[1], other(DOWN + 1)),
        (passes_up, other(PLANE - 1 - UP), other(PLANE - UP)),
        (passes_down, other(-DOWN), other(-DOWN - 1)),
    )

    def slot(d):
        return 2 * d if d < pairs else 2 * (dloc - 1 - d) + 1

    def direction(p):
        return p // 2 if p % 2 == 0 else dloc - 1 - p // 2

    small = [
        pltpu.make_async_copy(src, dst, small_sem.at[i])
        for i, (src, dst) in enumerate(
            (
                (table_h, table_v),
                (cells_h, cells),
                (angle_h, angle),
                (weight_h, weight),
                (level_h, level),
                (mask_h, mask),
                (rate_h, rate),
            )
        )
    ]
    for copy in small:
        copy.start()
    loads = [
        pltpu.make_async_copy(
            field.at[direction(p)], cur.at[p], load_sem.at[p]
        )
        for p in range(dloc)
    ]
    for copy in loads:
        copy.start()
    table_r[...] = jnp.zeros_like(table_r)

    barrier = pltpu.get_barrier_semaphore()
    pl.semaphore_signal(barrier, inc=1, device_id=partner, device_id_type=MESH)
    for side in (0, 1):

        @pl.when(has[side])
        def _():
            pl.semaphore_signal(barrier, inc=1, device_id=peer[side], device_id_type=MESH)

    peers = 1 + has[0].astype(jnp.int32) + has[1].astype(jnp.int32)
    for role, first, second in roles:

        @pl.when(role)
        def _():
            pl.semaphore_signal(barrier, inc=1, device_id=first, device_id_type=MESH)
            pl.semaphore_signal(barrier, inc=1, device_id=second, device_id_type=MESH)

        peers = peers + 2 * role.astype(jnp.int32)
    pl.semaphore_wait(barrier, peers)

    small[0].wait()
    tables = [
        pltpu.make_async_remote_copy(
            src_ref=table_v,
            dst_ref=table_r.at[1 - side],
            send_sem=table_send.at[side],
            recv_sem=table_recv.at[1 - side],
            device_id=peer[side],
            device_id_type=MESH,
        )
        for side in (0, 1)
    ]
    for side in (0, 1):

        @pl.when(has[side])
        def _():
            tables[side].start()

    for copy in loads[0 : 2 * AHEAD]:
        copy.wait()

    def full_copy(side, p):
        return pltpu.make_async_remote_copy(
            src_ref=cur.at[p],
            dst_ref=full.at[1 - side, p],
            send_sem=full_send.at[side, p],
            recv_sem=full_recv.at[1 - side, p],
            device_id=peer[side],
            device_id_type=MESH,
        )

    def full_arrival(side, p):
        return pltpu.make_async_remote_copy(
            src_ref=cur.at[p],
            dst_ref=full.at[side, p],
            send_sem=full_send.at[side, p],
            recv_sem=full_recv.at[side, p],
            device_id=peer[side],
            device_id_type=MESH,
        )

    beyond = (other(-DOWN - 1), other(PLANE - UP))

    for side in (0, 1):

        @pl.when(has[side])
        def _():
            for p in range(2 * AHEAD):
                full_copy(side, p).start()

    for copy in small[1:]:
        copy.wait()

    sub = lax.broadcasted_iota(jnp.int32, (LANES, LANES), 0)
    lane = lax.broadcasted_iota(jnp.int32, (LANES, LANES), 1)
    one = jnp.float32(1.0)
    zero = jnp.float32(0.0)

    def build(j, carry):
        at = pl.ds(pl.multiple_of(j * LANES, LANES), LANES)
        low = jnp.broadcast_to(cells[0:1, at], (LANES, LANES))
        upp = jnp.broadcast_to(cells[1:2, at], (LANES, LANES))
        for c in range(own // LANES):
            own_hot[c * LANES : (c + 1) * LANES, at] = jnp.where(
                low == sub + c * LANES, one, zero
            ).astype(HOT)
        for c in range(up_hot.shape[0] // LANES):
            up_hot[c * LANES : (c + 1) * LANES, at] = jnp.where(
                upp == sub + c * LANES, one, zero
            ).astype(HOT)
        low_t = low.T
        upp_t = upp.T
        for c in range(own // LANES):
            here = lane + c * LANES
            back_hot[at, c * LANES : (c + 1) * LANES] = (
                jnp.where(low_t == here, one, zero) - jnp.where(upp_t == here, one, zero)
            ).astype(HOT)
        return carry

    lax.fori_loop(0, fblk, build, 0)

    blocks = lax.broadcasted_iota(jnp.int32, (fblk, LANES), 0)
    slot_weight = jnp.where(blocks < live_s[0], weight[...], zero)
    along = jnp.cos(angle[...]) * slot_weight
    across = jnp.sin(angle[...]) * slot_weight
    sign = (1 - 2 * spec).astype(F32)
    along = along * sign
    across = across * sign
    for p in range(dloc):
        theta = (direction(p) + 0.5) * (2.0 * math.pi / NDIR)
        vel[p] = along * math.cos(theta) + across * math.sin(theta)

    freq = lax.broadcasted_iota(jnp.int32, (nfreq, LANES), 0)
    group = jnp.zeros((nfreq, LANES), F32)
    for f in range(nfreq):
        group = jnp.where(freq == f, speed_s[f], group)
    for c in range(own // LANES):
        lev = level[0:1, c * LANES : (c + 1) * LANES]
        area = jnp.exp2(-lev.astype(F32))
        scale[:, c * LANES : (c + 1) * LANES] = group * area
    bend = mask[...].astype(F32) * rate[...]
    turn[0:1, :] = jnp.maximum(bend, 0.0)
    turn[1:2, :] = jnp.minimum(bend, 0.0)

    for side in (0, 1):

        @pl.when(jnp.logical_not(has[side]))
        def _():
            def clear(i, carry):
                def inner(j, c):
                    got[i, side, j] = jnp.zeros(got.shape[3:], F32)
                    return c

                return lax.fori_loop(0, pairs, inner, carry)

            lax.fori_loop(0, ITERS, clear, 0)

    for side in (0, 1):

        @pl.when(has[side])
        def _():
            pltpu.make_async_remote_copy(
                src_ref=table_v,
                dst_ref=table_r.at[side],
                send_sem=table_send.at[side],
                recv_sem=table_recv.at[side],
                device_id=peer[side],
                device_id_type=MESH,
            ).wait_recv()

    for side in (0, 1):
        taken = table_r[side, 0]
        for k in range(hb):
            picks[side * hb + k] = jnp.broadcast_to(
                taken[1 - side : 2 - side, k : k + 1], (8, LANES)
            )

    mine = table_v[0]
    for side in (0, 1):
        for k in range(hb):
            picks[(2 + side) * hb + k] = jnp.broadcast_to(
                mine[side : side + 1, k : k + 1], (8, LANES)
            )

    def pick(value, which):
        wanted = jnp.broadcast_to(picks[which, 0:1, :], (nfreq, LANES))
        chosen = value[:, 0:LANES]
        for c in range(1, own // LANES):
            chosen = jnp.where(wanted == c, value[:, c * LANES : (c + 1) * LANES], chosen)
        return chosen

    def halo_copy(step, side, pair):
        return pltpu.make_async_remote_copy(
            src_ref=sent.at[step, side, pair],
            dst_ref=got.at[step, 1 - side, pair],
            send_sem=send_sem.at[step, side, pair],
            recv_sem=recv_sem.at[step, 1 - side, pair],
            device_id=peer[side],
            device_id_type=MESH,
        )

    def via_copy(step, side, pair, e):
        return pltpu.make_async_remote_copy(
            src_ref=sent.at[step, side, pair, e],
            dst_ref=passing.at[step, pair, e],
            send_sem=send_sem.at[step, side, pair],
            recv_sem=pass_recv.at[step, pair, e],
            device_id=relay[side],
            device_id_type=MESH,
        )

    def pass_copy(step, side, pair, e):
        return pltpu.make_async_remote_copy(
            src_ref=passing.at[step, pair, e],
            dst_ref=got.at[step, 1 - side, pair, e],
            send_sem=pass_send.at[step, pair, e],
            recv_sem=recv_sem.at[step, 1 - side, pair],
            device_id=beyond[side],
            device_id_type=MESH,
        )

    def came(ref, send, recv):
        pltpu.make_async_remote_copy(
            src_ref=ref,
            dst_ref=ref,
            send_sem=send,
            recv_sem=recv,
            device_id=other(1),
            device_id_type=MESH,
        ).wait_recv()

    def pass_on(step, first, last):
        for side, role in ((0, passes_down), (1, passes_up)):

            @pl.when(role)
            def _():
                def one(pair, carry):
                    for e in (0, 1):
                        came(
                            passing.at[step, pair, e],
                            pass_send.at[step, pair, e],
                            pass_recv.at[step, pair, e],
                        )
                        pass_copy(step, side, pair, e).start()
                    return carry

                lax.fori_loop(first, last, one, 0)

    def halo_arrival(step, side, pair):
        return pltpu.make_async_remote_copy(
            src_ref=sent.at[step, side, pair],
            dst_ref=got.at[step, side, pair],
            send_sem=send_sem.at[step, side, pair],
            recv_sem=recv_sem.at[step, side, pair],
            device_id=peer[side],
            device_id_type=MESH,
        )

    def send_pair(step, pair):
        for side in (0, 1):
            for e in (0, 1):
                value = cur[2 * pair + e]
                for k in range(hb):
                    sent[step, side, pair, e, k] = pick(value, side * hb + k)

            @pl.when(has[side] & jnp.logical_not(via[side]))
            def _():
                halo_copy(step, side, pair).start()

            @pl.when(via[side])
            def _():
                for e in (0, 1):
                    via_copy(step, side, pair, e).start()

    home = {}
    for begin, count in CHUNKS:
        for p in range(2 * begin, 2 * (begin + count)):
            home[p] = (4 * begin * ROWS + (p - 2 * begin) * ROWS, 2 * count * ROWS)

    def put(p, at, value):
        first, span = home[p]
        high, low = split(value)
        ext[first : first + nfreq, at] = high
        ext[first + span : first + span + nfreq, at] = low

    def split_own(p):
        put(p, slice(0, own), cur[p])

    for copy in loads[2 * AHEAD :]:
        copy.wait()
    for pair in range(AHEAD, pairs):
        send_pair(0, pair)
    for p in range(dloc):
        split_own(p)
    pass_on(0, AHEAD, pairs)
    for side in (0, 1):

        @pl.when(has[side])
        def _():
            for p in range(2 * AHEAD):
                full_arrival(side, p).wait_recv()
                value = full[side, p]
                for k in range(hb):
                    got[0, side, p // 2, p % 2, k] = pick(value, (2 + side) * hb + k)
            for p in range(2 * AHEAD):
                full_copy(side, p).wait_send()

    def turn_slot(step, p):
        d = direction(p)
        here = moved[p]
        before = moved[slot(d - 1)] if d > 0 else edge_got[step, 1]
        after = moved[slot(d + 1)] if d < dloc - 1 else edge_got[step, 0]
        cur[p] = here - turn[0:1, :] * (here - before) - turn[1:2, :] * (after - here)
        split_own(p)

    def edge_copy(step):
        return pltpu.make_async_remote_copy(
            src_ref=edge_sent.at[step],
            dst_ref=edge_got.at[step],
            send_sem=edge_send.at[step],
            recv_sem=edge_recv.at[step],
            device_id=partner,
            device_id_type=MESH,
        )

    def finish_pair(step, pair):
        turn_slot(step, 2 * pair)
        turn_slot(step, 2 * pair + 1)

        @pl.when(step < ITERS - 1)
        def _():
            send_pair(step + 1, pair)

        @pl.when(step == ITERS - 1)
        def _():
            for p in (2 * pair, 2 * pair + 1):
                out[direction(p)] = cur[p]

    def compute(step, chunk):
        begin, count = CHUNKS[chunk]
        span = 2 * count * ROWS
        rows = slice(4 * begin * ROWS, 4 * begin * ROWS + 2 * span)
        for pair in range(begin, begin + count):
            for side in (0, 1):
                awaited = has[side] if pair >= AHEAD else has[side] & (step > 0)

                @pl.when(awaited)
                def _():
                    halo_arrival(step, side, pair).wait_recv()

            for side in (0, 1):
                for e in (0, 1):
                    for k in range(hb):
                        first = own + (side * hb + k) * LANES
                        put(2 * pair + e, slice(first, first + LANES), got[step, side, pair, e, k])
        width = 2 * LANES
        for n in range(faces // width):
            at = slice(n * width, (n + 1) * width)
            low = jnp.dot(ext[rows, 0:own], own_hot[:, at], preferred_element_type=F32)
            upp = jnp.dot(ext[rows, :], up_hot[:, at], preferred_element_type=F32)
            low = low[0:span] + low[span : 2 * span]
            upp = upp[0:span] + upp[span : 2 * span]
            for i in range(2 * count):
                p = 2 * begin + i
                there = slice(i * ROWS, (i + 1) * ROWS)
                for h in range(2):
                    inner = slice(h * LANES, (h + 1) * LANES)
                    u = jnp.broadcast_to(
                        vel[p, 2 * n + h : 2 * n + h + 1, :], (ROWS, LANES)
                    )
                    flow = u * jnp.where(u > 0.0, low[there, inner], upp[there, inner])
                    high, rest = split(flow)
                    outer = slice(n * width + h * LANES, n * width + (h + 1) * LANES)
                    flux[there, outer] = high
                    flux[slice(span + i * ROWS, span + (i + 1) * ROWS), outer] = rest
        total = jnp.dot(flux[0 : 2 * span, :], back_hot[...], preferred_element_type=F32)
        total = total[0:span] + total[span : 2 * span]
        for i in range(2 * count):
            p = 2 * begin + i
            moved[p] = cur[p] - scale[...] * total[i * ROWS : i * ROWS + nfreq]

    def one_step(step, carry):
        @pl.when(step > 0)
        def _():
            pass_on(step, 0, pairs)

        done = 1
        for chunk, (begin, count) in enumerate(CHUNKS):
            compute(step, chunk)
            if chunk == 0:
                edge_sent[step] = moved[0:2]
                edge_copy(step).start()
            if chunk == EDGE_AT:
                edge_copy(step).wait_recv()
                finish_pair(step, 0)
            last = begin + count == pairs
            ready = pairs if last else begin + count - 1
            for pair in range(done, ready):
                finish_pair(step, pair)
            done = max(done, ready)
        return carry

    lax.fori_loop(0, ITERS, one_step, 0)

    for step in range(ITERS):
        edge_copy(step).wait_send()
    for side, role in ((0, passes_down), (1, passes_up)):

        @pl.when(role)
        def _():
            for step in range(ITERS):
                for pair in range(AHEAD if step == 0 else 0, pairs):
                    for e in (0, 1):
                        pass_copy(step, side, pair, e).wait_send()

    for side in (0, 1):

        @pl.when(has[side])
        def _():
            tables[side].wait_send()
            for step in range(ITERS):
                for pair in range(AHEAD if step == 0 else 0, pairs):
                    halo_copy(step, side, pair).wait_send()


def on_device(
    field,
    group_speed,
    face_angle,
    face_speed,
    face_cells,
    face_live,
    halo_blocks,
    cell_level,
    polar_mask,
    turn_rate,
):
    dloc, nfreq, own = field.shape
    faces = face_angle.shape[0]
    fblk = faces // LANES
    hb = halo_blocks.shape[2]
    ext = own + 2 * hb * LANES
    pairs = dloc // 2
    any_spec = pl.BlockSpec(memory_space=pl.ANY)
    smem_spec = pl.BlockSpec(memory_space=pltpu.SMEM)
    halo = (ITERS, 2, pairs, 2, hb, nfreq, LANES)
    span = 2 * max(count for _, count in CHUNKS) * ROWS
    return pl.pallas_call(
        kernel,
        out_shape=pltpu.VMEM(field.shape, field.dtype),
        in_specs=[
            any_spec,
            smem_spec,
            any_spec,
            any_spec,
            any_spec,
            smem_spec,
            any_spec,
            any_spec,
            any_spec,
            any_spec,
        ],
        out_specs=pl.BlockSpec(memory_space=pltpu.VMEM),
        scratch_shapes=[
            pltpu.VMEM((dloc, nfreq, own), F32),
            pltpu.VMEM((dloc, nfreq, own), F32),
            pltpu.VMEM(halo, F32),
            pltpu.VMEM(halo, F32),
            pltpu.VMEM((ITERS, 2, nfreq, own), F32),
            pltpu.VMEM((ITERS, 2, nfreq, own), F32),
            pltpu.VMEM((2 * dloc * ROWS, ext), BF16),
            pltpu.VMEM((2 * span, faces), BF16),
            pltpu.VMEM((own, faces), HOT),
            pltpu.VMEM((ext, faces), HOT),
            pltpu.VMEM((faces, own), HOT),
            pltpu.VMEM((dloc, fblk, LANES), F32),
            pltpu.VMEM((nfreq, own), F32),
            pltpu.VMEM((2, own), F32),
            pltpu.VMEM((fblk, LANES), F32),
            pltpu.VMEM((fblk, LANES), F32),
            pltpu.VMEM((2, faces), jnp.int32),
            pltpu.VMEM((1, own), jnp.int32),
            pltpu.VMEM((1, own), jnp.int32),
            pltpu.VMEM((1, own), F32),
            pltpu.VMEM((1, 2, hb), jnp.int32),
            pltpu.VMEM((2, 1, 2, hb), jnp.int32),
            pltpu.VMEM((4 * hb, 8, LANES), jnp.int32),
            pltpu.VMEM((2, 2 * AHEAD, nfreq, own), F32),
            pltpu.VMEM((ITERS, pairs, 2, hb, nfreq, LANES), F32),
            pltpu.SemaphoreType.DMA((dloc,)),
            pltpu.SemaphoreType.DMA((7,)),
            pltpu.SemaphoreType.DMA((2,)),
            pltpu.SemaphoreType.DMA((2,)),
            pltpu.SemaphoreType.DMA((2, 2 * AHEAD)),
            pltpu.SemaphoreType.DMA((2, 2 * AHEAD)),
            pltpu.SemaphoreType.DMA((ITERS, pairs, 2)),
            pltpu.SemaphoreType.DMA((ITERS, pairs, 2)),
            pltpu.SemaphoreType.DMA((ITERS, 2, pairs)),
            pltpu.SemaphoreType.DMA((ITERS, 2, pairs)),
            pltpu.SemaphoreType.DMA((ITERS,)),
            pltpu.SemaphoreType.DMA((ITERS,)),
        ],
        compiler_params=pltpu.CompilerParams(
            collective_id=0, has_side_effects=True, vmem_limit_bytes=60 * 1024 * 1024
        ),
    )(
        field,
        group_speed,
        face_angle.reshape(fblk, LANES),
        face_speed.reshape(fblk, LANES),
        face_cells,
        face_live,
        halo_blocks,
        cell_level.reshape(1, own),
        polar_mask.reshape(1, own),
        turn_rate.reshape(1, own),
    )


def solution(mesh):
    return jax.shard_map(
        on_device,
        mesh=mesh,
        in_specs=(
            P("spec", None, "rows"),
            P(),
            P("rows"),
            P("rows"),
            P(None, "rows"),
            P("rows"),
            P("rows", None, None),
            P("rows"),
            P("rows"),
            P("rows"),
        ),
        out_specs=P("spec", None, "rows"),
        check_vma=False,
    )
```

```python
import functools
import math

import jax
import jax.numpy as jnp
from jax import lax
from jax.experimental import pallas as pl
from jax.experimental.pallas import tpu as pltpu
from jax.sharding import PartitionSpec as P

MESH = pl.DeviceIdType.MESH
NDIR = 36
ITERS = 3
LANES = 128
ROWS = 32
CHUNKS = ((0, 1), (1, 2), (3, 2), (5, 2), (7, 1), (8, 1))
AHEAD = 2
EDGE_AT = 1
PLANE = 32
UP, DOWN = 7, 25
HOT = jnp.float8_e4m3fn
BF16 = jnp.bfloat16
F32 = jnp.float32


def split(value):
    high = value.astype(BF16)
    return high, (value - high.astype(F32)).astype(BF16)


def kernel(
    field,
    speed_s,
    angle_h,
    weight_h,
    cells_h,
    live_s,
    table_h,
    level_h,
    mask_h,
    rate_h,
    out,
    cur,
    moved,
    sent,
    got,
    edge_sent,
    edge_got,
    ext,
    flux,
    own_hot,
    up_hot,
    back_hot,
    vel,
    scale,
    turn,
    angle,
    weight,
    cells,
    level,
    mask,
    rate,
    table_v,
    table_r,
    picks,
    full,
    passing,
    load_sem,
    small_sem,
    table_send,
    table_recv,
    full_send,
    full_recv,
    pass_send,
    pass_recv,
    send_sem,
    recv_sem,
    edge_send,
    edge_recv,
):
    dloc, nfreq, own = field.shape
    pairs = dloc // 2
    hb = table_h.shape[2]
    faces = cells.shape[1]
    fblk = faces // LANES
    size = lax.axis_size("rows")
    row = lax.axis_index("rows")
    spec = lax.axis_index("spec")
    has = (row > 0, row < size - 1)
    peer = ({"rows": jnp.maximum(row - 1, 0)}, {"rows": jnp.minimum(row + 1, size - 1)})
    partner = {"spec": 1 - spec}

    at = lax.rem(row, PLANE)
    odd = spec == 1

    def other(shift):
        return {"rows": jnp.clip(row + shift, 0, size - 1)}

    via = (odd & (at == 0) & (row > 0), odd & (at == PLANE - 1) & (row < size - 1))
    passes_up = odd & (at == UP) & (row < size - PLANE)
    passes_down = odd & (at == DOWN) & (row >= PLANE)
    relay = (other(DOWN), other(UP + 1 - PLANE))
    roles = (
        (via[0], relay[0], other(UP - PLANE)),
        (via[1], relay[1], other(DOWN + 1)),
        (passes_up, other(PLANE - 1 - UP), other(PLANE - UP)),
        (passes_down, other(-DOWN), other(-DOWN - 1)),
    )

    def slot(d):
        return 2 * d if d < pairs else 2 * (dloc - 1 - d) + 1

    def direction(p):
        return p // 2 if p % 2 == 0 else dloc - 1 - p // 2

    small = [
        pltpu.make_async_copy(src, dst, small_sem.at[i])
        for i, (src, dst) in enumerate(
            (
                (table_h, table_v),
                (cells_h, cells),
                (angle_h, angle),
                (weight_h, weight),
                (level_h, level),
                (mask_h, mask),
                (rate_h, rate),
            )
        )
    ]
    for copy in small:
        copy.start()
    loads = [
        pltpu.make_async_copy(
            field.at[direction(p)], cur.at[p], load_sem.at[p]
        )
        for p in range(dloc)
    ]
    for copy in loads:
        copy.start()
    table_r[...] = jnp.zeros_like(table_r)

    barrier = pltpu.get_barrier_semaphore()
    pl.semaphore_signal(barrier, inc=1, device_id=partner, device_id_type=MESH)
    for side in (0, 1):

        @pl.when(has[side])
        def _():
            pl.semaphore_signal(barrier, inc=1, device_id=peer[side], device_id_type=MESH)

    peers = 1 + has[0].astype(jnp.int32) + has[1].astype(jnp.int32)
    for role, first, second in roles:

        @pl.when(role)
        def _():
            pl.semaphore_signal(barrier, inc=1, device_id=first, device_id_type=MESH)
            pl.semaphore_signal(barrier, inc=1, device_id=second, device_id_type=MESH)

        peers = peers + 2 * role.astype(jnp.int32)
    pl.semaphore_wait(barrier, peers)

    small[0].wait()
    tables = [
        pltpu.make_async_remote_copy(
            src_ref=table_v,
            dst_ref=table_r.at[1 - side],
            send_sem=table_send.at[side],
            recv_sem=table_recv.at[1 - side],
            device_id=peer[side],
            device_id_type=MESH,
        )
        for side in (0, 1)
    ]
    for side in (0, 1):

        @pl.when(has[side])
        def _():
            tables[side].start()

    for copy in loads[0 : 2 * AHEAD]:
        copy.wait()

    def full_copy(side, p):
        return pltpu.make_async_remote_copy(
            src_ref=cur.at[p],
            dst_ref=full.at[1 - side, p],
            send_sem=full_send.at[side, p],
            recv_sem=full_recv.at[1 - side, p],
            device_id=peer[side],
            device_id_type=MESH,
        )

    def full_arrival(side, p):
        return pltpu.make_async_remote_copy(
            src_ref=cur.at[p],
            dst_ref=full.at[side, p],
            send_sem=full_send.at[side, p],
            recv_sem=full_recv.at[side, p],
            device_id=peer[side],
            device_id_type=MESH,
        )

    for side in (0, 1):

        @pl.when(has[side])
        def _():
            for p in range(2 * AHEAD):
                full_copy(side, p).start()

    for copy in small[1:]:
        copy.wait()

    sub = lax.broadcasted_iota(jnp.int32, (LANES, LANES), 0)
    lane = lax.broadcasted_iota(jnp.int32, (LANES, LANES), 1)
    one = jnp.float32(1.0)
    zero = jnp.float32(0.0)

    def build(j, carry):
        at = pl.ds(pl.multiple_of(j * LANES, LANES), LANES)
        low = jnp.broadcast_to(cells[0:1, at], (LANES, LANES))
        upp = jnp.broadcast_to(cells[1:2, at], (LANES, LANES))
        for c in range(own // LANES):
            own_hot[c * LANES : (c + 1) * LANES, at] = jnp.where(
                low == sub + c * LANES, one, zero
            ).astype(HOT)
        for c in range(up_hot.shape[0] // LANES):
            up_hot[c * LANES : (c + 1) * LANES, at] = jnp.where(
                upp == sub + c * LANES, one, zero
            ).astype(HOT)
        low_t = low.T
        upp_t = upp.T
        for c in range(own // LANES):
            here = lane + c * LANES
            back_hot[at, c * LANES : (c + 1) * LANES] = (
                jnp.where(low_t == here, one, zero) - jnp.where(upp_t == here, one, zero)
            ).astype(HOT)
        return carry

    lax.fori_loop(0, fblk, build, 0)

    blocks = lax.broadcasted_iota(jnp.int32, (fblk, LANES), 0)
    slot_weight = jnp.where(blocks < live_s[0], weight[...], zero)
    along = jnp.cos(angle[...]) * slot_weight
    across = jnp.sin(angle[...]) * slot_weight
    sign = (1 - 2 * spec).astype(F32)
    along = along * sign
    across = across * sign
    for p in range(dloc):
        theta = (direction(p) + 0.5) * (2.0 * math.pi / NDIR)
        vel[p] = along * math.cos(theta) + across * math.sin(theta)

    freq = lax.broadcasted_iota(jnp.int32, (nfreq, LANES), 0)
    group = jnp.zeros((nfreq, LANES), F32)
    for f in range(nfreq):
        group = jnp.where(freq == f, speed_s[f], group)
    for c in range(own // LANES):
        lev = level[0:1, c * LANES : (c + 1) * LANES]
        area = jnp.exp2(-lev.astype(F32))
        scale[:, c * LANES : (c + 1) * LANES] = group * area
    bend = mask[...].astype(F32) * rate[...]
    turn[0:1, :] = jnp.maximum(bend, 0.0)
    turn[1:2, :] = jnp.minimum(bend, 0.0)

    for side in (0, 1):

        @pl.when(jnp.logical_not(has[side]))
        def _():
            def clear(i, carry):
                def inner(j, c):
                    got[i, side, j] = jnp.zeros(got.shape[3:], F32)
                    return c

                return lax.fori_loop(0, pairs, inner, carry)

            lax.fori_loop(0, ITERS, clear, 0)

    for side in (0, 1):

        @pl.when(has[side])
        def _():
            pltpu.make_async_remote_copy(
                src_ref=table_v,
                dst_ref=table_r.at[side],
                send_sem=table_send.at[side],
                recv_sem=table_recv.at[side],
                device_id=peer[side],
                device_id_type=MESH,
            ).wait_recv()

    for side in (0, 1):
        taken = table_r[side, 0]
        for k in range(hb):
            picks[side * hb + k] = jnp.broadcast_to(
                taken[1 - side : 2 - side, k : k + 1], (8, LANES)
            )

    mine = table_v[0]
    for side in (0, 1):
        for k in range(hb):
            picks[(2 + side) * hb + k] = jnp.broadcast_to(
                mine[side : side + 1, k : k + 1], (8, LANES)
            )

    def pick(value, which):
        wanted = jnp.broadcast_to(picks[which, 0:1, :], (nfreq, LANES))
        chosen = value[:, 0:LANES]
        for c in range(1, own // LANES):
            chosen = jnp.where(wanted == c, value[:, c * LANES : (c + 1) * LANES], chosen)
        return chosen

    def halo_copy(step, side, pair):
        return pltpu.make_async_remote_copy(
            src_ref=sent.at[step, side, pair],
            dst_ref=got.at[step, 1 - side, pair],
            send_sem=send_sem.at[step, side, pair],
            recv_sem=recv_sem.at[step, 1 - side, pair],
            device_id=peer[side],
            device_id_type=MESH,
        )

    def via_copy(step, side, pair):
        return pltpu.make_async_remote_copy(
            src_ref=sent.at[step, side, pair],
            dst_ref=passing.at[step, pair],
            send_sem=send_sem.at[step, side, pair],
            recv_sem=pass_recv.at[step, pair],
            device_id=relay[side],
            device_id_type=MESH,
        )

    def pass_copy(step, side, pair):
        return pltpu.make_async_remote_copy(
            src_ref=passing.at[step, pair],
            dst_ref=got.at[step, 1 - side, pair],
            send_sem=pass_send.at[step, pair],
            recv_sem=recv_sem.at[step, 1 - side, pair],
            device_id=other(-DOWN - 1) if side == 0 else other(PLANE - UP),
            device_id_type=MESH,
        )

    def pass_on(step, first):
        for side, role in ((0, passes_down), (1, passes_up)):

            @pl.when(role)
            def _():
                def one(pair, carry):
                    pltpu.make_async_remote_copy(
                        src_ref=passing.at[step, pair],
                        dst_ref=passing.at[step, pair],
                        send_sem=pass_send.at[step, pair],
                        recv_sem=pass_recv.at[step, pair],
                        device_id=other(1),
                        device_id_type=MESH,
                    ).wait_recv()
                    pass_copy(step, side, pair).start()
                    return carry

                lax.fori_loop(first, pairs, one, 0)

    def halo_arrival(step, side, pair):
        return pltpu.make_async_remote_copy(
            src_ref=sent.at[step, side, pair],
            dst_ref=got.at[step, side, pair],
            send_sem=send_sem.at[step, side, pair],
            recv_sem=recv_sem.at[step, side, pair],
            device_id=peer[side],
            device_id_type=MESH,
        )

    def send_pair(step, pair):
        for side in (0, 1):
            for e in (0, 1):
                value = cur[2 * pair + e]
                for k in range(hb):
                    sent[step, side, pair, e, k] = pick(value, side * hb + k)

            @pl.when(has[side] & jnp.logical_not(via[side]))
            def _():
                halo_copy(step, side, pair).start()

            @pl.when(via[side])
            def _():
                via_copy(step, side, pair).start()

    home = {}
    for begin, count in CHUNKS:
        for p in range(2 * begin, 2 * (begin + count)):
            home[p] = (4 * begin * ROWS + (p - 2 * begin) * ROWS, 2 * count * ROWS)

    def put(p, at, value):
        first, span = home[p]
        high, low = split(value)
        ext[first : first + nfreq, at] = high
        ext[first + span : first + span + nfreq, at] = low

    def split_own(p):
        put(p, slice(0, own), cur[p])

    for copy in loads[2 * AHEAD :]:
        copy.wait()
    for pair in range(AHEAD, pairs):
        send_pair(0, pair)
    for p in range(dloc):
        split_own(p)
    pass_on(0, AHEAD)
    for side in (0, 1):

        @pl.when(has[side])
        def _():
            for p in range(2 * AHEAD):
                full_arrival(side, p).wait_recv()
                value = full[side, p]
                for k in range(hb):
                    got[0, side, p // 2, p % 2, k] = pick(value, (2 + side) * hb + k)
            for p in range(2 * AHEAD):
                full_copy(side, p).wait_send()

    def turn_slot(step, p):
        d = direction(p)
        here = moved[p]
        before = moved[slot(d - 1)] if d > 0 else edge_got[step, 1]
        after = moved[slot(d + 1)] if d < dloc - 1 else edge_got[step, 0]
        cur[p] = here - turn[0:1, :] * (here - before) - turn[1:2, :] * (after - here)
        split_own(p)

    def edge_copy(step):
        return pltpu.make_async_remote_copy(
            src_ref=edge_sent.at[step],
            dst_ref=edge_got.at[step],
            send_sem=edge_send.at[step],
            recv_sem=edge_recv.at[step],
            device_id=partner,
            device_id_type=MESH,
        )

    def finish_pair(step, pair):
        turn_slot(step, 2 * pair)
        turn_slot(step, 2 * pair + 1)

        @pl.when(step < ITERS - 1)
        def _():
            send_pair(step + 1, pair)

        @pl.when(step == ITERS - 1)
        def _():
            for p in (2 * pair, 2 * pair + 1):
                out[direction(p)] = cur[p]

    def compute(step, chunk):
        begin, count = CHUNKS[chunk]
        span = 2 * count * ROWS
        rows = slice(4 * begin * ROWS, 4 * begin * ROWS + 2 * span)
        for pair in range(begin, begin + count):
            for side in (0, 1):
                awaited = has[side] if pair >= AHEAD else has[side] & (step > 0)

                @pl.when(awaited)
                def _():
                    halo_arrival(step, side, pair).wait_recv()

            for side in (0, 1):
                for e in (0, 1):
                    for k in range(hb):
                        first = own + (side * hb + k) * LANES
                        put(2 * pair + e, slice(first, first + LANES), got[step, side, pair, e, k])
        width = 2 * LANES
        for n in range(faces // width):
            at = slice(n * width, (n + 1) * width)
            low = jnp.dot(ext[rows, 0:own], own_hot[:, at], preferred_element_type=F32)
            upp = jnp.dot(ext[rows, :], up_hot[:, at], preferred_element_type=F32)
            low = low[0:span] + low[span : 2 * span]
            upp = upp[0:span] + upp[span : 2 * span]
            for i in range(2 * count):
                p = 2 * begin + i
                there = slice(i * ROWS, (i + 1) * ROWS)
                for h in range(2):
                    inner = slice(h * LANES, (h + 1) * LANES)
                    u = jnp.broadcast_to(
                        vel[p, 2 * n + h : 2 * n + h + 1, :], (ROWS, LANES)
                    )
                    flow = u * jnp.where(u > 0.0, low[there, inner], upp[there, inner])
                    high, rest = split(flow)
                    outer = slice(n * width + h * LANES, n * width + (h + 1) * LANES)
                    flux[there, outer] = high
                    flux[slice(span + i * ROWS, span + (i + 1) * ROWS), outer] = rest
        total = jnp.dot(flux[0 : 2 * span, :], back_hot[...], preferred_element_type=F32)
        total = total[0:span] + total[span : 2 * span]
        for i in range(2 * count):
            p = 2 * begin + i
            moved[p] = cur[p] - scale[...] * total[i * ROWS : i * ROWS + nfreq]

    def one_step(step, carry):
        @pl.when(step > 0)
        def _():
            pass_on(step, 0)

        done = 1
        for chunk, (begin, count) in enumerate(CHUNKS):
            compute(step, chunk)
            if chunk == 0:
                edge_sent[step] = moved[0:2]
                edge_copy(step).start()
            if chunk == EDGE_AT:
                edge_copy(step).wait_recv()
                finish_pair(step, 0)
            last = begin + count == pairs
            ready = pairs if last else begin + count - 1
            for pair in range(done, ready):
                finish_pair(step, pair)
            done = max(done, ready)
        return carry

    lax.fori_loop(0, ITERS, one_step, 0)

    for step in range(ITERS):
        edge_copy(step).wait_send()
    for side, role in ((0, passes_down), (1, passes_up)):

        @pl.when(role)
        def _():
            for step in range(ITERS):
                for pair in range(AHEAD if step == 0 else 0, pairs):
                    pass_copy(step, side, pair).wait_send()

    for side in (0, 1):

        @pl.when(has[side])
        def _():
            tables[side].wait_send()
            for step in range(ITERS):
                for pair in range(AHEAD if step == 0 else 0, pairs):
                    halo_copy(step, side, pair).wait_send()


def on_device(
    field,
    group_speed,
    face_angle,
    face_speed,
    face_cells,
    face_live,
    halo_blocks,
    cell_level,
    polar_mask,
    turn_rate,
):
    dloc, nfreq, own = field.shape
    faces = face_angle.shape[0]
    fblk = faces // LANES
    hb = halo_blocks.shape[2]
    ext = own + 2 * hb * LANES
    pairs = dloc // 2
    any_spec = pl.BlockSpec(memory_space=pl.ANY)
    smem_spec = pl.BlockSpec(memory_space=pltpu.SMEM)
    halo = (ITERS, 2, pairs, 2, hb, nfreq, LANES)
    span = 2 * max(count for _, count in CHUNKS) * ROWS
    return pl.pallas_call(
        kernel,
        out_shape=pltpu.VMEM(field.shape, field.dtype),
        in_specs=[
            any_spec,
            smem_spec,
            any_spec,
            any_spec,
            any_spec,
            smem_spec,
            any_spec,
            any_spec,
            any_spec,
            any_spec,
        ],
        out_specs=pl.BlockSpec(memory_space=pltpu.VMEM),
        scratch_shapes=[
            pltpu.VMEM((dloc, nfreq, own), F32),
            pltpu.VMEM((dloc, nfreq, own), F32),
            pltpu.VMEM(halo, F32),
            pltpu.VMEM(halo, F32),
            pltpu.VMEM((ITERS, 2, nfreq, own), F32),
            pltpu.VMEM((ITERS, 2, nfreq, own), F32),
            pltpu.VMEM((2 * dloc * ROWS, ext), BF16),
            pltpu.VMEM((2 * span, faces), BF16),
            pltpu.VMEM((own, faces), HOT),
            pltpu.VMEM((ext, faces), HOT),
            pltpu.VMEM((faces, own), HOT),
            pltpu.VMEM((dloc, fblk, LANES), F32),
            pltpu.VMEM((nfreq, own), F32),
            pltpu.VMEM((2, own), F32),
            pltpu.VMEM((fblk, LANES), F32),
            pltpu.VMEM((fblk, LANES), F32),
            pltpu.VMEM((2, faces), jnp.int32),
            pltpu.VMEM((1, own), jnp.int32),
            pltpu.VMEM((1, own), jnp.int32),
            pltpu.VMEM((1, own), F32),
            pltpu.VMEM((1, 2, hb), jnp.int32),
            pltpu.VMEM((2, 1, 2, hb), jnp.int32),
            pltpu.VMEM((4 * hb, 8, LANES), jnp.int32),
            pltpu.VMEM((2, 2 * AHEAD, nfreq, own), F32),
            pltpu.VMEM((ITERS, pairs, 2, hb, nfreq, LANES), F32),
            pltpu.SemaphoreType.DMA((dloc,)),
            pltpu.SemaphoreType.DMA((7,)),
            pltpu.SemaphoreType.DMA((2,)),
            pltpu.SemaphoreType.DMA((2,)),
            pltpu.SemaphoreType.DMA((2, 2 * AHEAD)),
            pltpu.SemaphoreType.DMA((2, 2 * AHEAD)),
            pltpu.SemaphoreType.DMA((ITERS, pairs)),
            pltpu.SemaphoreType.DMA((ITERS, pairs)),
            pltpu.SemaphoreType.DMA((ITERS, 2, pairs)),
            pltpu.SemaphoreType.DMA((ITERS, 2, pairs)),
            pltpu.SemaphoreType.DMA((ITERS,)),
            pltpu.SemaphoreType.DMA((ITERS,)),
        ],
        compiler_params=pltpu.CompilerParams(
            collective_id=0, has_side_effects=True, vmem_limit_bytes=60 * 1024 * 1024
        ),
    )(
        field,
        group_speed,
        face_angle.reshape(fblk, LANES),
        face_speed.reshape(fblk, LANES),
        face_cells,
        face_live,
        halo_blocks,
        cell_level.reshape(1, own),
        polar_mask.reshape(1, own),
        turn_rate.reshape(1, own),
    )


def solution(mesh):
    return jax.shard_map(
        on_device,
        mesh=mesh,
        in_specs=(
            P("spec", None, "rows"),
            P(),
            P("rows"),
            P("rows"),
            P(None, "rows"),
            P("rows"),
            P("rows", None, None),
            P("rows"),
            P("rows"),
            P("rows"),
        ),
        out_specs=P("spec", None, "rows"),
        check_vma=False,
    )
```
